32 devices in a mesh: seq: 8 (over z, y), tp: 4 (over x, core).
Axes of the slice: x: 2, y: 2, z: 4, core: 2. Of those that a mesh axis runs over, the one named last changes fastest.
Arguments:
- tokens: bfloat16 [8192, 2048], P('seq', 'tp'), may hold values from -8 to 8
- col_order: int32 [8192], P('seq'), may hold values from 0 to 8191, as said below
- in_gain: float32 [2, 2048], replicated, may hold values from 0.5 to 1.5
- w_in: bfloat16 [2, 2048, 2, 2048], P(None, None, None, 'tp'), may hold values from -0.125 to 0.125
- w_bc: bfloat16 [2, 2048, 256], replicated, may hold values from -0.0625 to 0.0625
- w_dt: bfloat16 [2, 2048, 32], P(None, None, 'tp'), may hold values from -2 to 2
- conv_x: float32 [2, 4, 2048], P(None, None, 'tp'), may hold values from -3 to 3
- conv_bc: float32 [2, 4, 256], replicated, may hold values from -3 to 3
- dt_bias: float32 [2, 32], P(None, 'tp'), may hold values from -1 to 0.5
- a_log: float32 [2, 32], P(None, 'tp'), may hold values from -16 to -2, as said below
- d_skip: float32 [2, 32], P(None, 'tp'), may hold values from 0.5 to 2
- out_gain: float32 [2, 2048], P(None, 'tp'), may hold values from 0.5 to 1.5
- w_out: bfloat16 [2, 2048, 2048], P(None, 'tp'), may hold values from -0.125 to 0.125
Outputs:
- mixed_out: bfloat16 [8192, 2048], P('seq', 'tp')
The draws below stay inside these ranges and needn't reach their ends.
Inputs may be any that keep to these rules, and one draw needn't show every extreme that they name: `col_order`: A permutation of the 8192 positions of a frame of 16 rows and 512 columns stored row by row: the column order visits the columns one after another in a drawn order, each from top to bottom or from bottom to top as drawn. So every aligned block of 1024 positions takes exactly 128 row-order positions from each aligned block of 1024 row-order positions. Each head's decay rate exp(a_log) is either between about one in fifty and one in seventeen a step or between 0.3 / 8192 and 2 / 8192 a step.
All inputs are finite; a program needn't handle non-finite values.
Results may differ from the reference program's by a relative error of at most 0.024.
Values may be sent and summed in bfloat16 or wider, within the bound.
A program may use at most 128 MiB of HBM per device.

```python
import math
import jax
import jax.numpy as jnp
from jax import lax

D = 2048
HEADS = 32
HEAD_DIM = 64
STATE = 128
CONV = 4
STRETCH = 128
WIDTH_CELLS = 512
INNER = 2048
FRAME_ROWS = 16
TOKENS = 8192
N_TP = 4


def shared_direction(key):
    raw = jax.random.normal(jax.random.fold_in(key, 31), (D,), dtype=jnp.float32)
    return raw / jnp.sqrt(jnp.sum(raw * raw))


def draw_tokens(key, part):
    direction = shared_direction(key)
    noise_key, level_key = jax.random.split(jax.random.fold_in(key, 17), 2)
    noise = jnp.clip(jax.random.normal(noise_key, (TOKENS, D), dtype=jnp.float32), -6.0, 6.0)
    levels = jax.random.uniform(level_key, (FRAME_ROWS,), minval=-3.0, maxval=3.0)
    along = jnp.repeat(levels, WIDTH_CELLS, total_repeat_length=TOKENS)
    return (noise + along[:, None] * direction[None, :]).astype(jnp.bfloat16)


def draw_w_dt(key, part):
    direction = shared_direction(key)
    base_key, amp_key = jax.random.split(jax.random.fold_in(key, 19), 2)
    base = jnp.clip(jax.random.normal(base_key, (2, D, HEADS), dtype=jnp.float32), -4.0, 4.0) / math.sqrt(D)
    amplitude = jax.random.uniform(amp_key, (2, HEADS), minval=0.5, maxval=1.5)
    return (base + direction[None, :, None] * amplitude[:, None, :]).astype(jnp.bfloat16)


def draw_a_log(key, part):
    base = jax.random.fold_in(key, 7)
    pick_key, fast_key, slow_key = jax.random.split(base, 3)
    share = 0.5
    fast = jax.random.uniform(pick_key, (2, HEADS)) < share
    fast_rate = jnp.exp(jax.random.uniform(fast_key, (2, HEADS), minval=math.log(1.0 / 50.0), maxval=math.log(1.0 / 17.0)))
    slow_rate = jnp.exp(jax.random.uniform(slow_key, (2, HEADS), minval=math.log(0.3), maxval=math.log(2.0))) / TOKENS
    return jnp.log(jnp.where(fast, fast_rate, slow_rate)).astype(jnp.float32)


def draw_col_order(key, part):
    base = jax.random.fold_in(key, 13)
    perm_key, turn_key = jax.random.split(base, 2)
    columns = jax.random.permutation(perm_key, WIDTH_CELLS).astype(jnp.int32)
    downward = jax.random.randint(turn_key, (WIDTH_CELLS,), 0, 2).astype(jnp.int32)
    position = jnp.arange(TOKENS, dtype=jnp.int32)
    visit = position // FRAME_ROWS
    along = position % FRAME_ROWS
    row_index = jnp.where(downward[visit] == 1, along, FRAME_ROWS - 1 - along)
    return (row_index * WIDTH_CELLS + columns[visit]).astype(jnp.int32)


def steps_of(own_key, shape, shards, least, high):
    factor_of, own = 1.0, jax.random.fold_in(own_key, 6)
    for dim, blocks in shards:
        draws = jnp.exp(jax.random.uniform(jax.random.fold_in(own, dim), (blocks,), jnp.float32, least / len(shards), high / len(shards)))
        factor_of = factor_of * jnp.repeat(draws, shape[dim] // blocks).reshape([-1 if axis == dim else 1 for axis in range(len(shape))])
    return factor_of


def normal_values(key, dims, scale, bound, cuts=(), kind=jnp.bfloat16):
    gain = steps_of(key, dims, cuts, -0.22, 0.18) if cuts else 1.0
    drawn = jax.random.normal(key, dims, jnp.float32) * scale * gain
    return jnp.minimum(jnp.maximum(drawn, -bound), bound).astype(kind)


def setup_inputs(seed: int = 0) -> dict:
    keys = jax.random.split(jax.random.key(seed), 14)
    return {
        "tokens": draw_tokens(jax.random.fold_in(keys[13], 71), 0),
        "col_order": draw_col_order(jax.random.fold_in(keys[13], 71), 0),
        "in_gain": jnp.clip(1.0 + 0.1 * jax.random.normal(keys[2], (2, D), jnp.float32), 0.5, 1.5),
        "w_in": normal_values(keys[3], (2, D, 2, INNER), D ** -0.5, 0.125, ((3, 4),)),
        "w_bc": normal_values(keys[4], (2, D, 2 * STATE), (4 * D) ** -0.5, 0.0625),
        "w_dt": draw_w_dt(jax.random.fold_in(keys[13], 71), 0),
        "conv_x": normal_values(keys[6], (2, CONV, INNER), 0.5, 3.0, ((2, 4),), jnp.float32),
        "conv_bc": normal_values(keys[7], (2, CONV, 2 * STATE), 0.5, 3.0, (), jnp.float32),
        "dt_bias": jnp.clip(-1.0 + 1.5 * jax.random.uniform(keys[8], (2, HEADS), jnp.float32) ** steps_of(keys[8], (2, HEADS), ((1, 4),), -0.2, 0.2), -1.0, 0.5),
        "a_log": draw_a_log(jax.random.fold_in(keys[13], 71), 0),
        "d_skip": jnp.clip(0.5 + 1.5 * jax.random.uniform(keys[10], (2, HEADS), jnp.float32) ** steps_of(keys[10], (2, HEADS), ((1, 4),), -0.2, 0.2), 0.5, 2.0),
        "out_gain": jnp.clip(1.0 + 0.1 * jax.random.normal(keys[11], (2, INNER), jnp.float32), 0.5, 1.5),
        "w_out": normal_values(keys[12], (2, INNER, D), INNER ** -0.5, 0.125, ((1, 4),)),
    }


highest = lax.Precision.HIGHEST
epsilon = 1e-05

def causal_mix(signal, taps):
    length = signal.shape[0]
    padded = jnp.concatenate([jnp.zeros((CONV - 1, signal.shape[1]), jnp.float32), signal.astype(jnp.float32)], axis=0)
    mixed = jnp.zeros((length, signal.shape[1]), jnp.float32)
    for offset in range(CONV):
        mixed = mixed + taps[offset] * padded[offset:offset + length]
    return mixed

def block_step(state, pieces):
    decay_log, b_rows, c_rows, feed = pieces
    cumul = jnp.cumsum(decay_log, axis=0)
    cumul_t = cumul.T
    lower = jnp.arange(STRETCH)[:, None] >= jnp.arange(STRETCH)[None, :]
    spread = jnp.where(lower[None], cumul_t[:, :, None] - cumul_t[:, None, :], -jnp.inf)
    weights = jnp.exp(spread)
    intersection = jnp.dot(c_rows, b_rows.T, precision=highest)
    inside = jnp.einsum('hqk,khp->qhp', intersection[None] * weights, feed, precision=highest)
    carried = jnp.einsum('qn,hpn->qhp', c_rows, state, precision=highest) * jnp.exp(cumul)[:, :, None]
    to_end = jnp.exp(cumul_t[:, -1:] - cumul_t)
    fresh = jnp.einsum('hk,kn,khp->hpn', to_end, b_rows, feed, precision=highest)
    new_state = jnp.exp(cumul[-1])[:, None, None] * state + fresh
    return (new_state, inside + carried)

def mix_layer(stream, which, in_gain, w_in, w_bc, w_dt, conv_x, conv_bc, dt_bias, a_log, d_skip, out_gain, w_out):
    widen = stream.astype(jnp.float32)
    scale = lax.rsqrt(lax.optimization_barrier(jnp.mean(widen * widen, axis=-1, keepdims=True)) + epsilon)
    normed = (widen * scale * in_gain[which]).astype(jnp.bfloat16)
    projected = jnp.dot(normed, w_in[which].reshape(D, 2 * INNER), preferred_element_type=jnp.float32)
    pre_x = projected[:, :INNER].astype(jnp.bfloat16)
    gate_z = projected[:, INNER:].astype(jnp.bfloat16)
    pre_bc = jnp.dot(normed, w_bc[which], preferred_element_type=jnp.float32).astype(jnp.bfloat16)
    dt_raw = jnp.dot(normed, w_dt[which], preferred_element_type=jnp.float32)
    conv_out = jax.nn.silu(causal_mix(pre_x, conv_x[which]))
    bc_out = jax.nn.silu(causal_mix(pre_bc, conv_bc[which]))
    step_size = jax.nn.softplus(dt_raw + dt_bias[which])
    decay_log = -step_size * jnp.exp(a_log[which])
    heads_in = conv_out.reshape(TOKENS, HEADS, HEAD_DIM)
    feed = heads_in * step_size[:, :, None]
    blocks = TOKENS // STRETCH
    pieces = (decay_log.reshape(blocks, STRETCH, HEADS), bc_out[:, :STATE].reshape(blocks, STRETCH, STATE), bc_out[:, STATE:].reshape(blocks, STRETCH, STATE), feed.reshape(blocks, STRETCH, HEADS, HEAD_DIM))
    start_state = jnp.zeros((HEADS, HEAD_DIM, STATE), jnp.float32)
    final_state, outputs = lax.scan(block_step, start_state, pieces)
    ssd = outputs.reshape(TOKENS, HEADS, HEAD_DIM) + d_skip[which][None, :, None] * heads_in
    gated = ssd * jax.nn.silu(gate_z.astype(jnp.float32).reshape(TOKENS, HEADS, HEAD_DIM))
    norm_scale = lax.rsqrt(lax.optimization_barrier(jnp.mean(gated * gated, axis=-1, keepdims=True)) + epsilon)
    mixed_heads = (gated * norm_scale * out_gain[which].reshape(HEADS, HEAD_DIM)).reshape(TOKENS, INNER).astype(jnp.bfloat16)
    group = INNER // N_TP
    total = jnp.zeros((TOKENS, D), jnp.float32)
    for member in range(N_TP):
        partial_sum = jnp.dot(mixed_heads[:, member * group:(member + 1) * group], w_out[which][member * group:(member + 1) * group], preferred_element_type=jnp.float32)
        rounded = lax.optimization_barrier(partial_sum.astype(jnp.bfloat16))
        total = total + rounded.astype(jnp.float32)
    return (widen + total).astype(jnp.bfloat16)

def reference(tokens, col_order, in_gain, w_in, w_bc, w_dt, conv_x, conv_bc, dt_bias, a_log, d_skip, out_gain, w_out):
    params = (in_gain, w_in, w_bc, w_dt, conv_x, conv_bc, dt_bias, a_log, d_skip, out_gain, w_out)
    row_result = mix_layer(tokens, 0, *params)
    column_rows = row_result[col_order.astype(jnp.int32)]
    return mix_layer(column_rows, 1, *params)
```

```python
import functools

import jax
import jax.numpy as jnp
from jax import lax
from jax.experimental import pallas as pl
from jax.experimental.pallas import tpu as pltpu
from jax.sharding import PartitionSpec as P

HEAD_DIM = 64
STATE = 128
STRETCH = 128
LANES = 128
HALO = 16
ROWS = 256

epsilon = 1e-05
f32 = jnp.float32
bf16 = jnp.bfloat16
MESH = pl.DeviceIdType.MESH


def iota(shape, axis):
    return lax.broadcasted_iota(jnp.int32, shape, axis)


def spreader_of(heads, inner):
    row = iota((LANES, inner), 0)
    channel = iota((LANES, inner), 1)
    chosen = (row % heads == channel // HEAD_DIM) & (row < 3 * heads)
    return jnp.where(chosen, 1.0, 0.0).astype(bf16)


def pack_pieces(values, heads):
    values = jnp.where(iota(values.shape, 1) < heads, values, 0.0)
    high = values.astype(bf16).astype(f32)
    rest = values - high
    middle = rest.astype(bf16).astype(f32)
    low = rest - middle
    packed = high + pltpu.roll(middle, heads, 1) + pltpu.roll(low, 2 * heads, 1)
    return packed.astype(bf16)


def expand(values, heads, spreader):
    return jnp.dot(pack_pieces(values, heads), spreader, preferred_element_type=f32)


def running_sum(tri, logs, heads):
    parts = jnp.dot(tri, pack_pieces(logs, heads), preferred_element_type=f32)
    total = parts + pltpu.roll(parts, LANES - heads, 1) + pltpu.roll(parts, LANES - 2 * heads, 1)
    return jnp.where(iota(total.shape, 1) < heads, total, 0.0)


def log_of(tail):
    wide = tail.astype(f32)
    return wide[0:1] + wide[1:2] + wide[2:3]


def log_rows(log):
    total = jnp.broadcast_to(log, (HALO, log.shape[1]))
    high = total.astype(bf16).astype(f32)
    middle = (total - high).astype(bf16).astype(f32)
    low = (total - high) - middle
    line = iota(total.shape, 0)
    return jnp.where(line == 0, high, jnp.where(line == 1, middle, low)).astype(bf16)


def exchange_plan(own, count):
    partners, uppers = [], []
    size = 2
    while size <= count:
        place = own % size
        base = own - place
        partners.append(base + (1 - place if size == 2 else size - 2 - place + 2 * (place % 2)))
        uppers.append(place // (size // 2) == 1)
        size *= 2
    return partners, uppers


def rows_of(k, size):
    return pl.ds(pl.multiple_of(k * size, size), size)


def layer_kernel(
    layer, count, members, with_orders,
    stream_ref, order_ref, in_gain_ref, w_in_ref, w_bc_ref, w_dt_ref, conv_x_ref, conv_bc_ref,
    small_ref, out_gain_ref, w_out_ref,
    out_ref, orders_out_ref,
    full_ref, halo_ref, orders_ref, raw_ref, w_ref, wo_ref, ext_ref, y_ref, z_ref, feed_ref,
    b_ref, c_ref, cum_ref, states_ref, sofar_exp_ref, state_ref, sofar_ref,
    end_ref, send_ref, got_ref, total_ref, prefix_ref,
    partial_ref, near_ref, sum_ref, far_ref,
    load_sem, self_sem, ag_send, ag_recv, halo_send, halo_recv, order_send, order_recv,
    ex_send, ex_recv, near_send, near_recv, far_send, far_recv,
):
    seq = lax.axis_index("seq")
    own = lax.axis_index("tp")
    chip, core = own // 2, own % 2
    near_id = chip * 2 + 1 - core
    across_id = (1 - chip) * 2 + core
    diagonal_id = (1 - chip) * 2 + 1 - core
    sibling = (seq, near_id)
    across = (seq, across_id)
    length, width = stream_ref.shape
    inner = y_ref.shape[1]
    mixed = inner + 2 * STATE
    heads = inner // HEAD_DIM
    chunks = length // ROWS
    per = ROWS // STRETCH
    blocks = length // STRETCH
    partners, uppers = exchange_plan(seq, count)
    following = (seq + 1) % count
    before = (seq + count - 1) % count

    greeted = [sibling, across]
    greeted += [(before, t) for t in range(members)]
    greeted += [(partner, own) for partner in partners]
    if with_orders:
        greeted += [((seq + d) % count, own) for d in range(1, count)]
    barrier = pltpu.get_barrier_semaphore()
    for device in greeted:
        pl.semaphore_signal(barrier, inc=1, device_id=device, device_id_type=MESH)

    loads = [
        pltpu.make_async_copy(w_in_ref.at[layer], raw_ref, load_sem.at[0]),
        pltpu.make_async_copy(
            w_bc_ref.at[layer], w_ref.at[:, inner:mixed], load_sem.at[1]
        ),
        pltpu.make_async_copy(w_out_ref.at[layer], wo_ref, load_sem.at[2]),
        pltpu.make_async_copy(stream_ref, full_ref.at[own], self_sem),
    ]
    for copy in loads:
        copy.start()

    pl.semaphore_wait(barrier, len(greeted))

    def remote(src, dst, send, recv, device):
        return pltpu.make_async_remote_copy(
            src_ref=src, dst_ref=dst, send_sem=send, recv_sem=recv,
            device_id=device, device_id_type=MESH,
        )

    def halo_copy(t):
        return remote(
            stream_ref.at[pl.ds(length - HALO, HALO)], halo_ref.at[own],
            halo_send.at[t], halo_recv.at[own], (following, t),
        )

    def halo_arrival(t):
        return remote(
            stream_ref.at[pl.ds(length - HALO, HALO)], halo_ref.at[t],
            halo_send.at[t], halo_recv.at[t], (following, t),
        )

    def across_copy(k):
        rows = rows_of(k, ROWS)
        return remote(
            stream_ref.at[rows], full_ref.at[own, rows], ag_send.at[0, k], ag_recv.at[0, k], across
        )

    def near_copy(k):
        rows = rows_of(k, ROWS)
        return remote(
            stream_ref.at[rows], full_ref.at[own, rows], ag_send.at[1, k], ag_recv.at[1, k], sibling
        )

    def forward_copy(k):
        rows = rows_of(k, ROWS)
        piece = full_ref.at[across_id, rows]
        return remote(piece, piece, ag_send.at[2, k], ag_recv.at[2, k], sibling)

    def order_copy(d):
        return remote(
            order_ref, orders_ref.at[seq], order_send.at[d - 1], order_recv.at[d - 1],
            ((seq + d) % count, own),
        )

    for t in range(members):
        halo_copy(t).start()
    for k in range(chunks):
        across_copy(k).start()
        near_copy(k).start()
    if with_orders:
        for d in range(1, count):
            order_copy(d).start()

    row = iota((2 * LANES, 2 * LANES), 0)
    col = iota((2 * LANES, 2 * LANES), 1)
    apart = jnp.where(col == 2 * (row % LANES) + row // LANES, 1.0, 0.0).astype(bf16)
    depth = w_ref.shape[0]
    dt = w_dt_ref[layer].astype(f32)
    dt = jnp.concatenate([dt, jnp.zeros((LANES - heads, depth), f32)], axis=0)
    w_ref[:, mixed + inner :] = dt.T.astype(bf16)
    loads[0].wait()

    def split_halves(i, _):
        rows = rows_of(i, LANES)
        both = raw_ref[rows].reshape(2 * LANES, inner)
        halves = jnp.dot(apart, both, preferred_element_type=f32).astype(bf16)
        w_ref[rows, 0:inner] = halves[:LANES]
        w_ref[rows, mixed : mixed + inner] = halves[LANES:]
        return 0

    lax.fori_loop(0, depth // LANES, split_halves, 0)
    loads[1].wait()
    loads[3].wait()

    gain = in_gain_ref[layer : layer + 1, :]

    def normed(v):
        wide = v.astype(f32)
        scale = lax.rsqrt(jnp.mean(wide * wide, axis=-1, keepdims=True) + epsilon)
        return (wide * scale * gain).astype(bf16)

    for t in range(members):
        halo_arrival(t).wait_recv()
    ahead = jnp.concatenate([halo_ref[t] for t in range(members)], axis=1)
    ahead = jnp.dot(normed(ahead), w_ref[:, :mixed], preferred_element_type=f32)
    ahead = ahead[HALO - 8 :, :].astype(bf16).astype(f32)
    ext_ref[0:8, :] = jnp.where(seq > 0, ahead, 0.0)
    state_ref[...] = jnp.zeros_like(state_ref)
    sofar_ref[...] = jnp.zeros_like(sofar_ref)

    spreader = spreader_of(heads, inner)
    line = iota((STRETCH, STRETCH), 0)
    lane = iota((STRETCH, STRETCH), 1)
    lower = line >= lane
    tri = jnp.where(lower, 1.0, 0.0).astype(bf16)
    small = small_ref[layer]
    bias, rate = small[0:1], small[1:2]
    skip = expand(jnp.broadcast_to(small[2:3], (8, LANES)), heads, spreader)[0:1]
    taps_x = conv_x_ref[layer]
    taps_bc = conv_bc_ref[layer]
    taps = jnp.concatenate([taps_x, taps_bc], axis=1)
    tap_count = taps.shape[0]

    def project(k, _):
        rows = rows_of(k, ROWS)
        remote(
            full_ref.at[across_id, rows], full_ref.at[across_id, rows],
            ag_send.at[0, k], ag_recv.at[0, k], across,
        ).wait_recv()
        forward_copy(k).start()
        remote(
            full_ref.at[near_id, rows], full_ref.at[near_id, rows],
            ag_send.at[1, k], ag_recv.at[1, k], sibling,
        ).wait_recv()
        remote(
            full_ref.at[diagonal_id, rows], full_ref.at[diagonal_id, rows],
            ag_send.at[2, k], ag_recv.at[2, k], sibling,
        ).wait_recv()
        tokens = jnp.concatenate([full_ref[t, rows, :] for t in range(members)], axis=1)
        projected = jnp.dot(normed(tokens), w_ref[...], preferred_element_type=f32)
        ext_ref[8 : 8 + ROWS, :] = projected[:, :mixed].astype(bf16).astype(f32)
        conv = jnp.zeros((ROWS, mixed), f32)
        for tap in range(tap_count):
            first = 9 - tap_count + tap
            conv = conv + taps[tap : tap + 1, :] * ext_ref[first : first + ROWS, :]
        conv = conv * jax.nn.sigmoid(conv)
        ext_ref[0:8, :] = ext_ref[ROWS : ROWS + 8, :]
        z_ref[rows, :] = projected[:, mixed : mixed + inner].astype(bf16)
        raw = projected[:, mixed + inner :] + bias
        step = jnp.maximum(raw, 0.0) + jnp.log1p(jnp.exp(-jnp.abs(raw)))
        logs = -step * rate
        x = conv[:, :inner]
        b_all = conv[:, inner : inner + STATE]
        b_ref[rows, :] = b_all.astype(bf16)
        c_ref[rows, :] = conv[:, inner + STATE :].astype(bf16)
        feed = x * expand(step, heads, spreader)
        feed_ref[rows, :] = feed.astype(bf16)
        y_ref[rows, :] = skip * x
        state = state_ref[...]
        sofar = sofar_ref[...]
        for block in range(per):
            part = slice(block * STRETCH, (block + 1) * STRETCH)
            index = k * per + block
            cum = running_sum(tri, logs[part], heads)
            last = cum[STRETCH - 1 : STRETCH, :]
            factors = expand(
                jnp.concatenate(
                    [jnp.exp(last - cum), jnp.exp(jnp.broadcast_to(last, (8, LANES))), jnp.exp(sofar)],
                    axis=0,
                ),
                heads, spreader,
            )
            fresh = jnp.dot(
                b_all[part].T.astype(bf16),
                (feed[part] * factors[:STRETCH]).astype(bf16),
                preferred_element_type=f32,
            )
            states_ref[index] = state
            sofar_exp_ref[index] = factors[STRETCH + 8 :]
            state = state * factors[STRETCH : STRETCH + 1] + fresh
            cum_ref[rows_of(index, STRETCH), :] = cum
            sofar = sofar + last
        state_ref[...] = state
        sofar_ref[...] = sofar
        return 0

    lax.fori_loop(0, chunks, project, 0)
    end_ref[0:STATE, :] = state_ref[...].astype(bf16)
    end_ref[STATE:, :] = log_rows(expand(sofar_ref[...], heads, spreader)[0:1])

    left = iota((STRETCH, 2 * HEAD_DIM), 1) < HEAD_DIM

    def within(block, _):
        rows = rows_of(block, STRETCH)
        cum = cum_ref[rows, :]
        cum_t = cum.T
        feed = feed_ref[rows, :]
        meet = lax.dot_general(
            c_ref[rows, :], b_ref[rows, :], (((1,), (1,)), ((), ())), preferred_element_type=f32
        )
        for pair in range(heads // 2):
            lanes = slice(pair * 2 * HEAD_DIM, (pair + 1) * 2 * HEAD_DIM)
            weights = []
            for h in (2 * pair, 2 * pair + 1):
                spread = jnp.where(lower, cum[:, h : h + 1] - cum_t[h : h + 1, :], -jnp.inf)
                weights.append((meet * jnp.exp(spread)).astype(bf16))
            fed = feed[:, lanes]
            nought = jnp.zeros_like(fed)
            stacked = jnp.concatenate(
                [jnp.where(left, fed, nought), jnp.where(left, nought, fed)], axis=0
            )
            inside = jnp.dot(
                jnp.concatenate(weights, axis=1), stacked, preferred_element_type=f32
            )
            y_ref[rows, lanes] = y_ref[rows, lanes] + inside
        return 0

    steps = len(partners)
    total_ref[...] = end_ref[:STATE, :].astype(f32)
    prefix_ref[...] = jnp.zeros_like(prefix_ref)
    total_log = log_of(end_ref[STATE:, :])
    prefix_log = jnp.zeros_like(total_log)
    sent = []
    done = 0
    for step, (partner, upper) in enumerate(zip(partners, uppers)):
        if step:
            send_ref[step - 1, :STATE, :] = total_ref[...].astype(bf16)
            send_ref[step - 1, STATE:, :] = log_rows(total_log)
        copy = remote(
            send_ref.at[step - 1] if step else end_ref, got_ref.at[step],
            ex_send.at[step], ex_recv.at[step], (partner, own),
        )
        copy.start()
        sent.append(copy)
        upto = blocks * (step + 1) // steps
        lax.fori_loop(done, upto, within, 0)
        done = upto
        copy.wait_recv()
        theirs = got_ref[step, :STATE, :].astype(f32)
        their_log = log_of(got_ref[step, STATE:, :])
        prefix = prefix_ref[...]
        prefix_ref[...] = jnp.where(upper, theirs * jnp.exp(prefix_log) + prefix, prefix)
        prefix_log = jnp.where(upper, prefix_log + their_log, prefix_log)
        if step + 1 < steps:
            mine = total_ref[...]
            first = jnp.where(upper, theirs, mine)
            then = jnp.where(upper, mine, theirs)
            total_ref[...] = first * jnp.exp(jnp.where(upper, total_log, their_log)) + then
            total_log = total_log + their_log
    if done < blocks:
        lax.fori_loop(done, blocks, within, 0)

    loads[2].wait()
    out_gain = out_gain_ref[layer : layer + 1, :]
    pair = 2 * HEAD_DIM
    one = iota((2 * pair, pair), 0) % pair // HEAD_DIM
    two = iota((2 * pair, pair), 1) // HEAD_DIM
    averager = jnp.where(one == two, 1.0 / HEAD_DIM, 0.0).astype(bf16)

    def columns(block):
        return pl.ds(pl.multiple_of(block * width, LANES), width)

    def near_part(side, k):
        rows = rows_of(k, ROWS)
        block = diagonal_id if side == 0 else near_id
        return remote(
            partial_ref.at[rows, columns(block)], near_ref.at[side, rows],
            near_send.at[side, k], near_recv.at[side, k], sibling,
        )

    def far_part(k):
        rows = rows_of(k, ROWS)
        return remote(
            sum_ref.at[rows], far_ref.at[rows], far_send.at[k], far_recv.at[k], across
        )

    def send_far(k):
        rows = rows_of(k, ROWS)
        near_part(0, k).wait_recv()
        sum_ref[rows, :] = (
            partial_ref[rows, columns(across_id)].astype(f32) + near_ref[0, rows, :].astype(f32)
        ).astype(bf16)
        far_part(k).start()

    def output(k, _):
        rows = rows_of(k, ROWS)
        grown = expand(jnp.exp(cum_ref[rows, :]), heads, spreader)
        carried = []
        for block in range(per):
            index = k * per + block
            state = states_ref[index] + prefix_ref[...] * sofar_exp_ref[index][0:1]
            carried.append(
                jnp.dot(
                    c_ref[rows_of(index, STRETCH), :], state.astype(bf16),
                    preferred_element_type=f32,
                )
            )
        gate = z_ref[rows, :].astype(f32)
        ssd = y_ref[rows, :] + jnp.concatenate(carried, axis=0) * grown
        gated = ssd * (gate * jax.nn.sigmoid(gate))
        square = gated * gated
        high = square.astype(bf16)
        low = (square - high.astype(f32)).astype(bf16)
        pieces = []
        for p in range(inner // pair):
            lanes = slice(p * pair, (p + 1) * pair)
            both = jnp.concatenate([high[:, lanes], low[:, lanes]], axis=1)
            mean = jnp.dot(both, averager, preferred_element_type=f32)
            pieces.append(
                (gated[:, lanes] * lax.rsqrt(mean + epsilon) * out_gain[:, lanes]).astype(bf16)
            )
        mixed_heads = jnp.concatenate(pieces, axis=1)
        partial_ref[rows, :] = jnp.dot(
            mixed_heads, wo_ref[...], preferred_element_type=f32
        ).astype(bf16)
        near_part(0, k).start()
        near_part(1, k).start()

        @pl.when(k > 0)
        def _():
            send_far(k - 1)

        return 0

    lax.fori_loop(0, chunks, output, 0)
    send_far(chunks - 1)

    def finish(k, _):
        rows = rows_of(k, ROWS)
        near_part(1, k).wait_recv()
        far_part(k).wait_recv()
        out_ref[rows, :] = (
            stream_ref[rows, :].astype(f32)
            + partial_ref[rows, columns(own)].astype(f32)
            + near_ref[1, rows, :].astype(f32)
            + far_ref[rows, :].astype(f32)
        ).astype(bf16)
        return 0

    lax.fori_loop(0, chunks, finish, 0)

    if with_orders:
        orders_ref[seq] = order_ref[...]
        for d in range(1, count):
            order_copy(d).wait_recv()
            order_copy(d).wait_send()
        orders_out_ref[...] = orders_ref[...]
    else:
        orders_out_ref[...] = jnp.zeros_like(orders_out_ref)
    for t in range(members):
        halo_copy(t).wait_send()

    def drain(k, _):
        across_copy(k).wait_send()
        near_copy(k).wait_send()
        forward_copy(k).wait_send()
        near_part(0, k).wait_send()
        near_part(1, k).wait_send()
        far_part(k).wait_send()
        return 0

    lax.fori_loop(0, chunks, drain, 0)
    for copy in sent:
        copy.wait_send()


def run_layer(layer, stream, order, params, with_orders):
    in_gain, w_in, w_bc, w_dt, conv_x, conv_bc, small, out_gain, w_out = params
    count, members = lax.axis_size("seq"), lax.axis_size("tp")
    steps = count.bit_length() - 1
    length, width = stream.shape
    inner = w_out.shape[1]
    heads = inner // HEAD_DIM
    mixed = inner + 2 * STATE
    depth = w_in.shape[1]
    chunks = length // ROWS
    blocks = length // STRETCH
    peers = max(count - 1, 1)
    vmem = pl.BlockSpec(memory_space=pltpu.VMEM)
    hbm = pl.BlockSpec(memory_space=pl.ANY)
    dma = pltpu.SemaphoreType.DMA
    return pl.pallas_call(
        functools.partial(layer_kernel, layer, count, members, with_orders),
        in_specs=[vmem, vmem, vmem, hbm, hbm, vmem, vmem, vmem, vmem, vmem, hbm],
        out_specs=[vmem, vmem],
        out_shape=[
            jax.ShapeDtypeStruct(stream.shape, bf16),
            jax.ShapeDtypeStruct((count if with_orders else 1, 1, length), jnp.int32),
        ],
        scratch_shapes=[
            pltpu.VMEM((members, length, width), bf16),
            pltpu.VMEM((members, HALO, width), bf16),
            pltpu.VMEM((count, 1, length), jnp.int32),
            pltpu.VMEM((depth, 2, inner), bf16),
            pltpu.VMEM((depth, mixed + inner + LANES), bf16),
            pltpu.VMEM((inner, depth), bf16),
            pltpu.VMEM((ROWS + 8, mixed), f32),
            pltpu.VMEM((length, inner), f32),
            pltpu.VMEM((length, inner), bf16),
            pltpu.VMEM((length, inner), bf16),
            pltpu.VMEM((length, STATE), bf16),
            pltpu.VMEM((length, STATE), bf16),
            pltpu.VMEM((length, LANES), f32),
            pltpu.VMEM((blocks, STATE, inner), f32),
            pltpu.VMEM((blocks, 8, inner), f32),
            pltpu.VMEM((STATE, inner), f32),
            pltpu.VMEM((8, LANES), f32),
            pltpu.VMEM((STATE + HALO, inner), bf16),
            pltpu.VMEM((max(steps - 1, 1), STATE + HALO, inner), bf16),
            pltpu.VMEM((steps, STATE + HALO, inner), bf16),
            pltpu.VMEM((STATE, inner), f32),
            pltpu.VMEM((STATE, inner), f32),
            pltpu.VMEM((length, depth), bf16),
            pltpu.VMEM((2, length, width), bf16),
            pltpu.VMEM((length, width), bf16),
            pltpu.VMEM((length, width), bf16),
            dma((3,)), dma, dma((3, chunks)), dma((3, chunks)),
            dma((members,)), dma((members,)), dma((peers,)), dma((peers,)),
            dma((steps,)), dma((steps,)), dma((2, chunks)), dma((2, chunks)),
            dma((chunks,)), dma((chunks,)),
        ],
        compiler_params=pltpu.CompilerParams(
            collective_id=layer, has_side_effects=True, vmem_limit_bytes=60 * 1024 * 1024
        ),
        name="mixer_layer_" + str(layer),
    )(stream, order, in_gain, w_in, w_bc, w_dt, conv_x, conv_bc, small, out_gain, w_out)


def plan_kernel(source_ref, local_ref, mine_ref, hand_ref, place_ref):
    own = lax.axis_index("seq")
    count, length = source_ref.shape
    share = length // count
    line = lax.broadcasted_iota(jnp.int32, (length, length), 0)
    lane = lax.broadcasted_iota(jnp.int32, (length, length), 1)
    upto = (line <= lane).astype(bf16)
    device = lax.broadcasted_iota(jnp.int32, (count, length), 0)

    def slots(member):
        ones = jnp.where(member, 1.0, 0.0)
        counted = jnp.dot(ones.astype(bf16), upto, preferred_element_type=f32)
        return jnp.where(member, counted.astype(jnp.int32) - 1, -1)

    slot = slots(source_ref[...] == own)
    short = lax.broadcasted_iota(jnp.int32, (share, length), 0)
    wide = lax.broadcasted_iota(jnp.int32, (share, length), 1)
    for d in range(count):
        chosen = slot[d : d + 1, :] == short
        local = jnp.where(chosen, local_ref[d : d + 1, :], 0).astype(f32)
        wanted = jnp.sum(local, axis=1, keepdims=True).astype(jnp.int32)
        hand_ref[d * share : (d + 1) * share, :] = jnp.where(wanted == wide, 1.0, 0.0).astype(bf16)
    from_each = mine_ref[...] == device
    arrived = jnp.where(from_each, slots(from_each) + share * device, 0).astype(f32)
    target = jnp.sum(arrived, axis=0, keepdims=True).astype(jnp.int32)
    place_ref[...] = jnp.where(line == target, 1.0, 0.0).astype(bf16)


def reorder_plans(col_order, orders):
    length = col_order.shape[0]
    vmem = pl.BlockSpec(memory_space=pltpu.VMEM)
    plan = jax.ShapeDtypeStruct((length, length), bf16)
    return pl.pallas_call(
        plan_kernel,
        in_specs=[vmem] * 3,
        out_specs=[vmem] * 2,
        out_shape=[plan, plan],
        compiler_params=pltpu.CompilerParams(vmem_limit_bytes=40 * 1024 * 1024),
        name="reorder_plans",
    )(orders // length, orders % length, (col_order // length)[None])


def pick(plan, rows):
    return jnp.dot(plan, rows, preferred_element_type=f32).astype(bf16)


def reorder_rows(stream, plans):
    hand, place = plans
    arrived = lax.all_to_all(pick(hand, stream), "seq", split_axis=0, concat_axis=0, tiled=True)
    return lax.dot_general(
        place, arrived, (((0,), (0,)), ((), ())), preferred_element_type=f32
    ).astype(bf16)


def body(
    tokens, col_order, in_gain, w_in, w_bc, w_dt, conv_x, conv_bc,
    dt_bias, a_log, d_skip, out_gain, w_out,
):
    small = jnp.stack([dt_bias, jnp.exp(a_log), d_skip], axis=1)
    small = jnp.pad(small, ((0, 0), (0, 0), (0, LANES - small.shape[2])))
    params = (
        in_gain, w_in, w_bc, jnp.swapaxes(w_dt, 1, 2), conv_x, conv_bc, small, out_gain, w_out
    )
    order = col_order[None]
    row_result, orders = run_layer(0, tokens, order, params, True)
    plans = reorder_plans(col_order, orders[:, 0])
    own_rows = reorder_rows(row_result, plans)
    return run_layer(1, own_rows, order, params, False)[0]


def solution(mesh):
    placed = (
        P("seq", "tp"),
        P("seq"),
        P(),
        P(None, None, None, "tp"),
        P(),
        P(None, None, "tp"),
        P(None, None, "tp"),
        P(),
        P(None, "tp"),
        P(None, "tp"),
        P(None, "tp"),
        P(None, "tp"),
        P(None, "tp", None),
    )
    return jax.shard_map(
        body, mesh=mesh, in_specs=placed, out_specs=P("seq", "tp"), check_vma=False
    )
```

```python
import functools

import jax
import jax.numpy as jnp
from jax import lax
from jax.experimental import pallas as pl
from jax.experimental.pallas import tpu as pltpu
from jax.sharding import PartitionSpec as P

HEAD_DIM = 64
STATE = 128
STRETCH = 128
LANES = 128
HALO = 16
ROWS = 256
COLUMNS = 128

epsilon = 1e-05
f32 = jnp.float32
bf16 = jnp.bfloat16
MESH = pl.DeviceIdType.MESH


def iota(shape, axis):
    return lax.broadcasted_iota(jnp.int32, shape, axis)


def spreader_of(heads, inner):
    row = iota((LANES, inner), 0)
    channel = iota((LANES, inner), 1)
    chosen = (row % heads == channel // HEAD_DIM) & (row < 3 * heads)
    return jnp.where(chosen, 1.0, 0.0).astype(bf16)


def pack_pieces(values, heads):
    values = jnp.where(iota(values.shape, 1) < heads, values, 0.0)
    high = values.astype(bf16).astype(f32)
    rest = values - high
    middle = rest.astype(bf16).astype(f32)
    low = rest - middle
    packed = high + pltpu.roll(middle, heads, 1) + pltpu.roll(low, 2 * heads, 1)
    return packed.astype(bf16)


def expand(values, heads, spreader):
    return jnp.dot(pack_pieces(values, heads), spreader, preferred_element_type=f32)


def running_sum(tri, logs, heads):
    parts = jnp.dot(tri, pack_pieces(logs, heads), preferred_element_type=f32)
    total = parts + pltpu.roll(parts, LANES - heads, 1) + pltpu.roll(parts, LANES - 2 * heads, 1)
    return jnp.where(iota(total.shape, 1) < heads, total, 0.0)


def log_of(tail):
    wide = tail.astype(f32)
    return wide[0:1] + wide[1:2] + wide[2:3]


def log_rows(log):
    total = jnp.broadcast_to(log, (HALO, log.shape[1]))
    high = total.astype(bf16).astype(f32)
    middle = (total - high).astype(bf16).astype(f32)
    low = (total - high) - middle
    line = iota(total.shape, 0)
    return jnp.where(line == 0, high, jnp.where(line == 1, middle, low)).astype(bf16)


def exchange_plan(own, count):
    partners, uppers = [], []
    size = 2
    while size <= count:
        place = own % size
        base = own - place
        partners.append(base + (1 - place if size == 2 else size - 2 - place + 2 * (place % 2)))
        uppers.append(place // (size // 2) == 1)
        size *= 2
    return partners, uppers


def rows_of(k, size):
    return pl.ds(pl.multiple_of(k * size, size), size)


def layer_kernel(
    layer, count, members, reorder,
    stream_ref, order_ref, in_gain_ref, w_in_ref, w_bc_ref, w_dt_ref, conv_x_ref, conv_bc_ref,
    small_ref, out_gain_ref, w_out_ref,
    out_ref,
    full_ref, halo_ref, orders_ref, raw_ref, w_ref, wo_ref, ext_ref, y_ref, z_ref, feed_ref,
    b_ref, c_ref, cum_ref, states_ref, sofar_exp_ref, state_ref, sofar_ref,
    end_ref, send_ref, got_ref, total_ref, prefix_ref,
    partial_ref, near_ref, sum_ref, far_ref,
    mixed_ref, hand_ref, place_ref, leaving_ref, arrived_ref,
    load_sem, self_sem, ag_send, ag_recv, halo_send, halo_recv, order_send, order_recv,
    ex_send, ex_recv, near_send, near_recv, far_send, far_recv,
    move_send, move_recv,
):
    seq = lax.axis_index("seq")
    own = lax.axis_index("tp")
    chip, core = own // 2, own % 2
    near_id = chip * 2 + 1 - core
    across_id = (1 - chip) * 2 + core
    diagonal_id = (1 - chip) * 2 + 1 - core
    sibling = (seq, near_id)
    across = (seq, across_id)
    length, width = stream_ref.shape
    inner = y_ref.shape[1]
    mixed = inner + 2 * STATE
    heads = inner // HEAD_DIM
    chunks = length // ROWS
    per = ROWS // STRETCH
    blocks = length // STRETCH
    partners, uppers = exchange_plan(seq, count)
    following = (seq + 1) % count
    before = (seq + count - 1) % count

    greeted = [sibling, across]
    greeted += [(before, t) for t in range(members)]
    greeted += [(partner, own) for partner in partners]
    if reorder:
        greeted += [((seq + d) % count, own) for d in range(1, count)]
    barrier = pltpu.get_barrier_semaphore()
    for device in greeted:
        pl.semaphore_signal(barrier, inc=1, device_id=device, device_id_type=MESH)

    loads = [
        pltpu.make_async_copy(w_in_ref.at[layer], raw_ref, load_sem.at[0]),
        pltpu.make_async_copy(
            w_bc_ref.at[layer], w_ref.at[:, inner:mixed], load_sem.at[1]
        ),
        pltpu.make_async_copy(stream_ref, full_ref.at[own], self_sem),
    ]
    if reorder:
        pieces = width // COLUMNS
        for j in range(pieces):
            for t in range(members):
                first = t * width + j * COLUMNS
                loads.append(
                    pltpu.make_async_copy(
                        w_out_ref.at[layer, :, first : first + COLUMNS],
                        wo_ref.at[:, (j * members + t) * COLUMNS : (j * members + t + 1) * COLUMNS],
                        load_sem.at[2 + j * members + t],
                    )
                )
    else:
        loads.append(pltpu.make_async_copy(w_out_ref.at[layer], wo_ref, load_sem.at[2]))
    for copy in loads:
        copy.start()

    pl.semaphore_wait(barrier, len(greeted))

    def remote(src, dst, send, recv, device):
        return pltpu.make_async_remote_copy(
            src_ref=src, dst_ref=dst, send_sem=send, recv_sem=recv,
            device_id=device, device_id_type=MESH,
        )

    def halo_copy(t):
        return remote(
            stream_ref.at[pl.ds(length - HALO, HALO)], halo_ref.at[own],
            halo_send.at[t], halo_recv.at[own], (following, t),
        )

    def halo_arrival(t):
        return remote(
            stream_ref.at[pl.ds(length - HALO, HALO)], halo_ref.at[t],
            halo_send.at[t], halo_recv.at[t], (following, t),
        )

    def across_copy(k):
        rows = rows_of(k, ROWS)
        return remote(
            stream_ref.at[rows], full_ref.at[own, rows], ag_send.at[0, k], ag_recv.at[0, k], across
        )

    def near_copy(k):
        rows = rows_of(k, ROWS)
        return remote(
            stream_ref.at[rows], full_ref.at[own, rows], ag_send.at[1, k], ag_recv.at[1, k], sibling
        )

    def forward_copy(k):
        rows = rows_of(k, ROWS)
        piece = full_ref.at[across_id, rows]
        return remote(piece, piece, ag_send.at[2, k], ag_recv.at[2, k], sibling)

    def order_copy(d):
        return remote(
            order_ref, orders_ref.at[seq], order_send.at[d - 1], order_recv.at[d - 1],
            ((seq + d) % count, own),
        )

    for t in range(members):
        halo_copy(t).start()
    for k in range(chunks):
        across_copy(k).start()
        near_copy(k).start()
    if reorder:
        for d in range(1, count):
            order_copy(d).start()

    row = iota((2 * LANES, 2 * LANES), 0)
    col = iota((2 * LANES, 2 * LANES), 1)
    apart = jnp.where(col == 2 * (row % LANES) + row // LANES, 1.0, 0.0).astype(bf16)
    depth = w_ref.shape[0]
    dt = w_dt_ref[layer].astype(f32)
    dt = jnp.concatenate([dt, jnp.zeros((LANES - heads, depth), f32)], axis=0)
    w_ref[:, mixed + inner :] = dt.T.astype(bf16)
    loads[0].wait()

    def split_halves(i, _):
        rows = rows_of(i, LANES)
        both = raw_ref[rows].reshape(2 * LANES, inner)
        halves = jnp.dot(apart, both, preferred_element_type=f32).astype(bf16)
        w_ref[rows, 0:inner] = halves[:LANES]
        w_ref[rows, mixed : mixed + inner] = halves[LANES:]
        return 0

    lax.fori_loop(0, depth // LANES, split_halves, 0)
    loads[1].wait()
    loads[2].wait()

    gain = in_gain_ref[layer : layer + 1, :]

    def normed(v):
        wide = v.astype(f32)
        scale = lax.rsqrt(jnp.mean(wide * wide, axis=-1, keepdims=True) + epsilon)
        return (wide * scale * gain).astype(bf16)

    for t in range(members):
        halo_arrival(t).wait_recv()
    ahead = jnp.concatenate([halo_ref[t] for t in range(members)], axis=1)
    ahead = jnp.dot(normed(ahead), w_ref[:, :mixed], preferred_element_type=f32)
    ahead = ahead[HALO - 8 :, :].astype(bf16).astype(f32)
    ext_ref[0:8, :] = jnp.where(seq > 0, ahead, 0.0)
    state_ref[...] = jnp.zeros_like(state_ref)
    sofar_ref[...] = jnp.zeros_like(sofar_ref)

    spreader = spreader_of(heads, inner)
    line = iota((STRETCH, STRETCH), 0)
    lane = iota((STRETCH, STRETCH), 1)
    lower = line >= lane
    tri = jnp.where(lower, 1.0, 0.0).astype(bf16)
    small = small_ref[layer]
    bias, rate = small[0:1], small[1:2]
    skip = expand(jnp.broadcast_to(small[2:3], (8, LANES)), heads, spreader)[0:1]
    taps_x = conv_x_ref[layer]
    taps_bc = conv_bc_ref[layer]
    taps = jnp.concatenate([taps_x, taps_bc], axis=1)
    tap_count = taps.shape[0]

    def project(k, _):
        rows = rows_of(k, ROWS)
        remote(
            full_ref.at[across_id, rows], full_ref.at[across_id, rows],
            ag_send.at[0, k], ag_recv.at[0, k], across,
        ).wait_recv()
        forward_copy(k).start()
        remote(
            full_ref.at[near_id, rows], full_ref.at[near_id, rows],
            ag_send.at[1, k], ag_recv.at[1, k], sibling,
        ).wait_recv()
        remote(
            full_ref.at[diagonal_id, rows], full_ref.at[diagonal_id, rows],
            ag_send.at[2, k], ag_recv.at[2, k], sibling,
        ).wait_recv()
        tokens = jnp.concatenate([full_ref[t, rows, :] for t in range(members)], axis=1)
        projected = jnp.dot(normed(tokens), w_ref[...], preferred_element_type=f32)
        ext_ref[8 : 8 + ROWS, :] = projected[:, :mixed].astype(bf16).astype(f32)
        conv = jnp.zeros((ROWS, mixed), f32)
        for tap in range(tap_count):
            first = 9 - tap_count + tap
            conv = conv + taps[tap : tap + 1, :] * ext_ref[first : first + ROWS, :]
        conv = conv * jax.nn.sigmoid(conv)
        ext_ref[0:8, :] = ext_ref[ROWS : ROWS + 8, :]
        z_ref[rows, :] = projected[:, mixed : mixed + inner].astype(bf16)
        raw = projected[:, mixed + inner :] + bias
        step = jnp.maximum(raw, 0.0) + jnp.log1p(jnp.exp(-jnp.abs(raw)))
        logs = -step * rate
        x = conv[:, :inner]
        b_all = conv[:, inner : inner + STATE]
        b_ref[rows, :] = b_all.astype(bf16)
        c_ref[rows, :] = conv[:, inner + STATE :].astype(bf16)
        feed = x * expand(step, heads, spreader)
        feed_ref[rows, :] = feed.astype(bf16)
        y_ref[rows, :] = skip * x
        state = state_ref[...]
        sofar = sofar_ref[...]
        for block in range(per):
            part = slice(block * STRETCH, (block + 1) * STRETCH)
            index = k * per + block
            cum = running_sum(tri, logs[part], heads)
            last = cum[STRETCH - 1 : STRETCH, :]
            factors = expand(
                jnp.concatenate(
                    [jnp.exp(last - cum), jnp.exp(jnp.broadcast_to(last, (8, LANES))), jnp.exp(sofar)],
                    axis=0,
                ),
                heads, spreader,
            )
            fresh = jnp.dot(
                b_all[part].T.astype(bf16),
                (feed[part] * factors[:STRETCH]).astype(bf16),
                preferred_element_type=f32,
            )
            states_ref[index] = state
            sofar_exp_ref[index] = factors[STRETCH + 8 :]
            state = state * factors[STRETCH : STRETCH + 1] + fresh
            cum_ref[rows_of(index, STRETCH), :] = cum
            sofar = sofar + last
        state_ref[...] = state
        sofar_ref[...] = sofar
        return 0

    lax.fori_loop(0, chunks, project, 0)
    end_ref[0:STATE, :] = state_ref[...].astype(bf16)
    end_ref[STATE:, :] = log_rows(expand(sofar_ref[...], heads, spreader)[0:1])

    left = iota((STRETCH, 2 * HEAD_DIM), 1) < HEAD_DIM

    def within(block, _):
        rows = rows_of(block, STRETCH)
        cum = cum_ref[rows, :]
        cum_t = cum.T
        feed = feed_ref[rows, :]
        meet = lax.dot_general(
            c_ref[rows, :], b_ref[rows, :], (((1,), (1,)), ((), ())), preferred_element_type=f32
        )
        for pair in range(heads // 2):
            lanes = slice(pair * 2 * HEAD_DIM, (pair + 1) * 2 * HEAD_DIM)
            weights = []
            for h in (2 * pair, 2 * pair + 1):
                spread = jnp.where(lower, cum[:, h : h + 1] - cum_t[h : h + 1, :], -jnp.inf)
                weights.append((meet * jnp.exp(spread)).astype(bf16))
            fed = feed[:, lanes]
            nought = jnp.zeros_like(fed)
            stacked = jnp.concatenate(
                [jnp.where(left, fed, nought), jnp.where(left, nought, fed)], axis=0
            )
            inside = jnp.dot(
                jnp.concatenate(weights, axis=1), stacked, preferred_element_type=f32
            )
            y_ref[rows, lanes] = y_ref[rows, lanes] + inside
        return 0

    steps = len(partners)
    total_ref[...] = end_ref[:STATE, :].astype(f32)
    prefix_ref[...] = jnp.zeros_like(prefix_ref)
    total_log = log_of(end_ref[STATE:, :])
    prefix_log = jnp.zeros_like(total_log)
    sent = []
    done = 0
    for step, (partner, upper) in enumerate(zip(partners, uppers)):
        if step:
            send_ref[step - 1, :STATE, :] = total_ref[...].astype(bf16)
            send_ref[step - 1, STATE:, :] = log_rows(total_log)
        copy = remote(
            send_ref.at[step - 1] if step else end_ref, got_ref.at[step],
            ex_send.at[step], ex_recv.at[step], (partner, own),
        )
        copy.start()
        sent.append(copy)
        upto = blocks * (step + 1) // steps
        lax.fori_loop(done, upto, within, 0)
        done = upto
        copy.wait_recv()
        theirs = got_ref[step, :STATE, :].astype(f32)
        their_log = log_of(got_ref[step, STATE:, :])
        prefix = prefix_ref[...]
        prefix_ref[...] = jnp.where(upper, theirs * jnp.exp(prefix_log) + prefix, prefix)
        prefix_log = jnp.where(upper, prefix_log + their_log, prefix_log)
        if step + 1 < steps:
            mine = total_ref[...]
            first = jnp.where(upper, theirs, mine)
            then = jnp.where(upper, mine, theirs)
            total_ref[...] = first * jnp.exp(jnp.where(upper, total_log, their_log)) + then
            total_log = total_log + their_log
    if done < blocks:
        lax.fori_loop(done, blocks, within, 0)

    for copy in loads[3:]:
        copy.wait()
    out_gain = out_gain_ref[layer : layer + 1, :]
    pair = 2 * HEAD_DIM
    one = iota((2 * pair, pair), 0) % pair // HEAD_DIM
    two = iota((2 * pair, pair), 1) // HEAD_DIM
    averager = jnp.where(one == two, 1.0 / HEAD_DIM, 0.0).astype(bf16)

    def mixed_of(k):
        rows = rows_of(k, ROWS)
        grown = expand(jnp.exp(cum_ref[rows, :]), heads, spreader)
        carried = []
        for block in range(per):
            index = k * per + block
            state = states_ref[index] + prefix_ref[...] * sofar_exp_ref[index][0:1]
            carried.append(
                jnp.dot(
                    c_ref[rows_of(index, STRETCH), :], state.astype(bf16),
                    preferred_element_type=f32,
                )
            )
        gate = z_ref[rows, :].astype(f32)
        ssd = y_ref[rows, :] + jnp.concatenate(carried, axis=0) * grown
        gated = ssd * (gate * jax.nn.sigmoid(gate))
        square = gated * gated
        high = square.astype(bf16)
        low = (square - high.astype(f32)).astype(bf16)
        pieces = []
        for p in range(inner // pair):
            lanes = slice(p * pair, (p + 1) * pair)
            both = jnp.concatenate([high[:, lanes], low[:, lanes]], axis=1)
            mean = jnp.dot(both, averager, preferred_element_type=f32)
            pieces.append(
                (gated[:, lanes] * lax.rsqrt(mean + epsilon) * out_gain[:, lanes]).astype(bf16)
            )
        return jnp.concatenate(pieces, axis=1)

    size, wide = (length, COLUMNS) if reorder else (ROWS, width)
    parts = (length // size) * (width // wide)

    def columns(k, block):
        place = (k * members + block) if reorder else block
        return pl.ds(pl.multiple_of(place * wide, LANES), wide)

    def rows_in(k):
        return pl.ds(0, length) if reorder else rows_of(k, ROWS)

    def near_part(side, k):
        block = diagonal_id if side == 0 else near_id
        return remote(
            partial_ref.at[rows_in(k), columns(k, block)], near_ref.at[side, k],
            near_send.at[side, k], near_recv.at[side, k], sibling,
        )

    def far_part(k):
        return remote(sum_ref.at[k], far_ref.at[k], far_send.at[k], far_recv.at[k], across)

    def send_far(k):
        near_part(0, k).wait_recv()
        sum_ref[k] = (
            partial_ref[rows_in(k), columns(k, across_id)].astype(f32)
            + near_ref[0, k].astype(f32)
        ).astype(bf16)
        far_part(k).start()

    def summed(k, stream):
        near_part(1, k).wait_recv()
        far_part(k).wait_recv()
        return (
            stream.astype(f32)
            + partial_ref[rows_in(k), columns(k, own)].astype(f32)
            + near_ref[1, k].astype(f32)
            + far_ref[k].astype(f32)
        ).astype(bf16)

    def send_near(k):
        near_part(0, k).start()
        near_part(1, k).start()

        @pl.when(k > 0)
        def _():
            send_far(k - 1)

    if reorder:

        def mix(k, _):
            mixed_ref[rows_of(k, ROWS), :] = mixed_of(k)
            return 0

        lax.fori_loop(0, chunks, mix, 0)

        def output(j, _):
            lanes = pl.ds(pl.multiple_of(j * members * wide, LANES), members * wide)

            def product(k, _):
                rows = rows_of(k, ROWS)
                partial_ref[rows, lanes] = jnp.dot(
                    mixed_ref[rows, :], wo_ref[:, lanes], preferred_element_type=f32
                ).astype(bf16)
                return 0

            lax.fori_loop(0, chunks, product, 0)
            send_near(j)
            return 0

        lax.fori_loop(0, parts, output, 0)
        send_far(parts - 1)

        share = length // count
        shift = length.bit_length() - 1
        for d in range(1, count):
            order_copy(d).wait_recv()
        orders_ref[seq] = order_ref[...]
        orders = jnp.concatenate([orders_ref[d] for d in range(count)], axis=0)

        def count_up(r, _):
            first = iota((LANES, length), 0) + r * LANES
            place_ref[rows_of(r, LANES), :] = jnp.where(
                first <= iota((LANES, length), 1), 1.0, 0.0
            ).astype(bf16)
            return 0

        lax.fori_loop(0, length // LANES, count_up, 0)
        device = iota((count, length), 0)
        wanted_here = jnp.right_shift(orders, shift) == seq
        from_each = jnp.right_shift(order_ref[...], shift) == device
        ones = jnp.concatenate(
            [jnp.where(wanted_here, 1.0, 0.0), jnp.where(from_each, 1.0, 0.0)], axis=0
        ).astype(bf16)
        counted = jnp.dot(ones, place_ref[...], preferred_element_type=f32).astype(jnp.int32) - 1
        slot = jnp.where(wanted_here, counted[:count], -1)
        local = jnp.bitwise_and(orders, length - 1)
        short = iota((share, length), 0)
        long = iota((share, length), 1)
        for d in range(count):
            chosen = slot[d : d + 1, :] == short
            found = jnp.where(chosen, local[d : d + 1, :], 0).astype(f32)
            wanted = jnp.sum(found, axis=1, keepdims=True).astype(jnp.int32)
            hand_ref[d * share : (d + 1) * share, :] = jnp.where(
                wanted == long, 1.0, 0.0
            ).astype(bf16)
        target = jnp.where(from_each, counted[count:] + share * device, 0).astype(f32)
        target = jnp.sum(target, axis=0, keepdims=True)
        target = jnp.broadcast_to(target, (LANES, length)).T.astype(jnp.int32)
        for c in range(length // LANES):
            place_ref[:, c * LANES : (c + 1) * LANES] = jnp.where(
                target == iota((length, LANES), 1) + c * LANES, 1.0, 0.0
            ).astype(bf16)

        def move_copy(j, d):
            other = (seq + d) % count
            return remote(
                leaving_ref.at[j, rows_of(other, share)], arrived_ref.at[j, rows_of(seq, share)],
                move_send.at[j, d - 1], move_recv.at[j, d - 1], (other, own),
            )

        def move_arrival(j, d):
            other = (seq + count - d) % count
            return remote(
                leaving_ref.at[j, rows_of(other, share)], arrived_ref.at[j, rows_of(other, share)],
                move_send.at[j, d - 1], move_recv.at[j, d - 1], ((seq + d) % count, own),
            )

        def hand_over(j):
            lanes = slice(j * wide, (j + 1) * wide)
            held = summed(j, stream_ref[:, lanes])
            leaving_ref[j] = jnp.dot(
                hand_ref[...], held, preferred_element_type=f32
            ).astype(bf16)

            def send(d, _):
                move_copy(j, d).start()
                return 0

            lax.fori_loop(1, count, send, 0)
            arrived_ref[j, rows_of(seq, share), :] = leaving_ref[j, rows_of(seq, share), :]

        def put(j):
            lanes = slice(j * wide, (j + 1) * wide)

            def arrive(d, _):
                move_arrival(j, d).wait_recv()
                return 0

            lax.fori_loop(1, count, arrive, 0)
            out_ref[:, lanes] = jnp.dot(
                place_ref[...], arrived_ref[j], preferred_element_type=f32
            ).astype(bf16)

        for j in range(parts):
            hand_over(j)
            if j:
                put(j - 1)
        put(parts - 1)

        def moved(d, _):
            for j in range(parts):
                move_copy(j, d).wait_send()
            return 0

        lax.fori_loop(1, count, moved, 0)
        for d in range(1, count):
            order_copy(d).wait_send()
    else:

        def output(k, _):
            partial_ref[rows_of(k, ROWS), :] = jnp.dot(
                mixed_of(k), wo_ref[...], preferred_element_type=f32
            ).astype(bf16)
            send_near(k)
            return 0

        lax.fori_loop(0, parts, output, 0)
        send_far(parts - 1)

        def finish(k, _):
            rows = rows_of(k, ROWS)
            out_ref[rows, :] = summed(k, stream_ref[rows, :])
            return 0

        lax.fori_loop(0, parts, finish, 0)

    for t in range(members):
        halo_copy(t).wait_send()

    def drain(k, _):
        across_copy(k).wait_send()
        near_copy(k).wait_send()
        forward_copy(k).wait_send()
        return 0

    lax.fori_loop(0, chunks, drain, 0)

    def drain_sums(k, _):
        near_part(0, k).wait_send()
        near_part(1, k).wait_send()
        far_part(k).wait_send()
        return 0

    lax.fori_loop(0, parts, drain_sums, 0)
    for copy in sent:
        copy.wait_send()


def run_layer(layer, stream, order, params, reorder):
    in_gain, w_in, w_bc, w_dt, conv_x, conv_bc, small, out_gain, w_out = params
    count, members = lax.axis_size("seq"), lax.axis_size("tp")
    steps = count.bit_length() - 1
    length, width = stream.shape
    inner = w_out.shape[1]
    heads = inner // HEAD_DIM
    mixed = inner + 2 * STATE
    depth = w_in.shape[1]
    chunks = length // ROWS
    blocks = length // STRETCH
    peers = max(count - 1, 1)
    size, wide = (length, COLUMNS) if reorder else (ROWS, width)
    parts = (length // size) * (width // wide)
    plan = (length, length) if reorder else (16, LANES)
    moving = (parts, length, wide) if reorder else (1, 16, LANES)
    vmem = pl.BlockSpec(memory_space=pltpu.VMEM)
    hbm = pl.BlockSpec(memory_space=pl.ANY)
    dma = pltpu.SemaphoreType.DMA
    return pl.pallas_call(
        functools.partial(layer_kernel, layer, count, members, reorder),
        in_specs=[vmem, vmem, vmem, hbm, hbm, vmem, vmem, vmem, vmem, vmem, hbm],
        out_specs=vmem,
        out_shape=jax.ShapeDtypeStruct(stream.shape, bf16),
        scratch_shapes=[
            pltpu.VMEM((members, length, width), bf16),
            pltpu.VMEM((members, HALO, width), bf16),
            pltpu.VMEM((count, 1, length), jnp.int32),
            pltpu.VMEM((depth, 2, inner), bf16),
            pltpu.VMEM((depth, mixed + inner + LANES), bf16),
            pltpu.VMEM((inner, depth), bf16),
            pltpu.VMEM((ROWS + 8, mixed), f32),
            pltpu.VMEM((length, inner), f32),
            pltpu.VMEM((length, inner), bf16),
            pltpu.VMEM((length, inner), bf16),
            pltpu.VMEM((length, STATE), bf16),
            pltpu.VMEM((length, STATE), bf16),
            pltpu.VMEM((length, LANES), f32),
            pltpu.VMEM((blocks, STATE, inner), f32),
            pltpu.VMEM((blocks, 8, inner), f32),
            pltpu.VMEM((STATE, inner), f32),
            pltpu.VMEM((8, LANES), f32),
            pltpu.VMEM((STATE + HALO, inner), bf16),
            pltpu.VMEM((max(steps - 1, 1), STATE + HALO, inner), bf16),
            pltpu.VMEM((steps, STATE + HALO, inner), bf16),
            pltpu.VMEM((STATE, inner), f32),
            pltpu.VMEM((STATE, inner), f32),
            pltpu.VMEM((length, depth), bf16),
            pltpu.VMEM((2, parts, size, wide), bf16),
            pltpu.VMEM((parts, size, wide), bf16),
            pltpu.VMEM((parts, size, wide), bf16),
            pltpu.VMEM((length, inner) if reorder else (16, LANES), bf16),
            pltpu.VMEM(plan, bf16), pltpu.VMEM(plan, bf16),
            pltpu.VMEM(moving, bf16), pltpu.VMEM(moving, bf16),
            dma((2 + (parts * members if reorder else 1),)), dma, dma((3, chunks)), dma((3, chunks)),
            dma((members,)), dma((members,)), dma((peers,)), dma((peers,)),
            dma((steps,)), dma((steps,)), dma((2, parts)), dma((2, parts)),
            dma((parts,)), dma((parts,)), dma((parts, peers)), dma((parts, peers)),
        ],
        compiler_params=pltpu.CompilerParams(
            collective_id=layer, has_side_effects=True, vmem_limit_bytes=60 * 1024 * 1024
        ),
        name="mixer_layer_" + str(layer),
    )(stream, order, in_gain, w_in, w_bc, w_dt, conv_x, conv_bc, small, out_gain, w_out)


def body(
    tokens, col_order, in_gain, w_in, w_bc, w_dt, conv_x, conv_bc,
    dt_bias, a_log, d_skip, out_gain, w_out,
):
    small = jnp.stack([dt_bias, jnp.exp(a_log), d_skip], axis=1)
    small = jnp.pad(small, ((0, 0), (0, 0), (0, LANES - small.shape[2])))
    params = (
        in_gain, w_in, w_bc, jnp.swapaxes(w_dt, 1, 2), conv_x, conv_bc, small, out_gain, w_out
    )
    order = col_order[None]
    own_rows = run_layer(0, tokens, order, params, True)
    return run_layer(1, own_rows, order, params, False)


def solution(mesh):
    placed = (
        P("seq", "tp"),
        P("seq"),
        P(),
        P(None, None, None, "tp"),
        P(),
        P(None, None, "tp"),
        P(None, None, "tp"),
        P(),
        P(None, "tp"),
        P(None, "tp"),
        P(None, "tp"),
        P(None, "tp"),
        P(None, "tp", None),
    )
    return jax.shard_map(
        body, mesh=mesh, in_specs=placed, out_specs=P("seq", "tp"), check_vma=False
    )
```

```python
import functools

import jax
import jax.numpy as jnp
from jax import lax
from jax.experimental import pallas as pl
from jax.experimental.pallas import tpu as pltpu
from jax.sharding import PartitionSpec as P

HEAD_DIM = 64
STATE = 128
STRETCH = 128
LANES = 128
HALO = 16
ROWS = 256
COLUMNS = 128

epsilon = 1e-05
f32 = jnp.float32
bf16 = jnp.bfloat16
MESH = pl.DeviceIdType.MESH


def iota(shape, axis):
    return lax.broadcasted_iota(jnp.int32, shape, axis)


def spreader_of(heads, inner):
    row = iota((LANES, inner), 0)
    channel = iota((LANES, inner), 1)
    chosen = (row % heads == channel // HEAD_DIM) & (row < 3 * heads)
    return jnp.where(chosen, 1.0, 0.0).astype(bf16)


def pack_pieces(values, heads):
    values = jnp.where(iota(values.shape, 1) < heads, values, 0.0)
    high = values.astype(bf16).astype(f32)
    rest = values - high
    middle = rest.astype(bf16).astype(f32)
    low = rest - middle
    packed = high + pltpu.roll(middle, heads, 1) + pltpu.roll(low, 2 * heads, 1)
    return packed.astype(bf16)


def expand(values, heads, spreader):
    return jnp.dot(pack_pieces(values, heads), spreader, preferred_element_type=f32)


def running_sum(tri, logs, heads):
    parts = jnp.dot(tri, pack_pieces(logs, heads), preferred_element_type=f32)
    total = parts + pltpu.roll(parts, LANES - heads, 1) + pltpu.roll(parts, LANES - 2 * heads, 1)
    return jnp.where(iota(total.shape, 1) < heads, total, 0.0)


def rows_of(k, size):
    return pl.ds(pl.multiple_of(k * size, size), size)


def lanes_of(k, size):
    return pl.ds(pl.multiple_of(k * size, LANES), size)


def pad_row(row):
    return jnp.concatenate([row, jnp.zeros((1, LANES - row.shape[1]), f32)], axis=1)


def layers_kernel(
    count, members,
    stream_ref, order_ref, in_gain_ref, w_in_ref, w_bc_ref, w_dt_ref, conv_x_ref, conv_bc_ref,
    bias_ref, a_log_ref, d_skip_ref, out_gain_ref, w_out_ref,
    out_ref,
    full_ref, tail_ref, halo_ref, orders_ref, raw_ref, raw_bc_ref, w_ref, wz_ref, wo_col_ref, wo_ref,
    ext_ref, y_ref, z_ref, feed_ref, b_ref, c_ref, cum_ref, scale_ref, states_ref, sofar_exp_ref,
    state_ref, sofar_ref,
    end_ref, log_ref, got_ref, logs_ref, give_ref, arriving_ref, prefix_ref,
    partial_ref, near_col_ref, sum_col_ref, far_col_ref, near_row_ref, sum_row_ref, far_row_ref,
    mixed_ref, hand_ref, place_ref, leaving_ref, arrived_ref,
    load_sem, wo_sem, self_sem, ag_send, ag_recv, halo_send, halo_recv, order_send, order_recv,
    end_send, end_recv, log_send, log_recv, give_send, give_recv,
    near_send, near_recv, far_send, far_recv, move_send, move_recv,
):
    seq = lax.axis_index("seq")
    own = lax.axis_index("tp")
    chip, core = own // 2, own % 2
    near_id = chip * 2 + 1 - core
    across_id = (1 - chip) * 2 + core
    diagonal_id = (1 - chip) * 2 + 1 - core
    sibling = (seq, near_id)
    across = (seq, across_id)
    length, width = stream_ref.shape
    depth = w_ref.shape[0]
    inner = y_ref.shape[1]
    mixed = inner + 2 * STATE
    heads = inner // HEAD_DIM
    chunks = length // ROWS
    per = ROWS // STRETCH
    blocks = length // STRETCH
    pieces = width // COLUMNS
    share = length // count
    state_rows = STATE // count
    following = (seq + 1) % count
    before = (seq + count - 1) % count

    def remote(src, dst, send, recv, device):
        return pltpu.make_async_remote_copy(
            src_ref=src, dst_ref=dst, send_sem=send, recv_sem=recv,
            device_id=device, device_id_type=MESH,
        )

    def each(first, last, act):
        def step(i, _):
            act(i)
            return 0

        lax.fori_loop(first, last, step, 0)

    greeted = [sibling, across]
    greeted += [(before, t) for t in range(members)]
    greeted += [((seq + d) % count, own) for d in range(1, count)]
    barrier = pltpu.get_barrier_semaphore()
    for device in greeted:
        pl.semaphore_signal(barrier, inc=1, device_id=device, device_id_type=MESH)

    def weight_loads(layer):
        return [
            pltpu.make_async_copy(w_in_ref.at[layer], raw_ref, load_sem.at[layer, 0]),
            pltpu.make_async_copy(w_bc_ref.at[layer], raw_bc_ref, load_sem.at[layer, 1]),
        ]

    own_lanes = lanes_of(own, COLUMNS)
    self_loads, wo_loads = [], []
    for j in range(pieces):
        self_loads.append(
            pltpu.make_async_copy(
                stream_ref.at[:, j * COLUMNS : (j + 1) * COLUMNS],
                full_ref.at[j, :, own_lanes], self_sem.at[j],
            )
        )
        for t in range(members):
            first = t * width + j * COLUMNS
            place = j * members + t
            wo_loads.append(
                pltpu.make_async_copy(
                    w_out_ref.at[0, :, first : first + COLUMNS],
                    wo_col_ref.at[:, place * COLUMNS : (place + 1) * COLUMNS],
                    wo_sem.at[place],
                )
            )
    wo_loads.append(pltpu.make_async_copy(w_out_ref.at[1], wo_ref, wo_sem.at[pieces * members]))
    for copy in weight_loads(0) + self_loads + wo_loads:
        copy.start()

    pl.semaphore_wait(barrier, len(greeted))

    def piece_of(j, k, t):
        return full_ref.at[j, rows_of(k, ROWS), lanes_of(t, COLUMNS)]

    def gather_copy(layer, kind, j, k, owner):
        src = piece_of(j, k, owner)
        if layer == 0 and kind < 2:
            src = stream_ref.at[rows_of(k, ROWS), lanes_of(j, COLUMNS)]
        return remote(
            src, piece_of(j, k, owner), ag_send.at[layer, kind, j, k],
            ag_recv.at[layer, kind, j, k], across if kind == 0 else sibling,
        )

    def send_piece(layer, j, k):
        gather_copy(layer, 0, j, k, own).start()
        gather_copy(layer, 1, j, k, own).start()

    def forward_piece(layer, j, k):
        gather_copy(layer, 0, j, k, across_id).wait_recv()
        gather_copy(layer, 2, j, k, across_id).start()

    def rest_of_piece(layer, j, k):
        gather_copy(layer, 1, j, k, near_id).wait_recv()
        gather_copy(layer, 2, j, k, diagonal_id).wait_recv()

    def gathered(layer):
        def drain(k):
            for j in range(pieces):
                gather_copy(layer, 0, j, k, own).wait_send()
                gather_copy(layer, 1, j, k, own).wait_send()
                gather_copy(layer, 2, j, k, across_id).wait_send()

        each(0, chunks, drain)

    def tail_of(layer):
        return tail_ref if layer else stream_ref.at[pl.ds(length - HALO, HALO)]

    def halo_copy(layer, t, source):
        return remote(
            tail_of(layer), halo_ref.at[layer, source],
            halo_send.at[layer, t], halo_recv.at[layer, source], (following, t),
        )

    def order_copy(d):
        return remote(
            order_ref, orders_ref.at[seq], order_send.at[d - 1], order_recv.at[d - 1],
            ((seq + d) % count, own),
        )

    for t in range(members):
        halo_copy(0, t, own).start()

    def send_rows(k):
        for j in range(pieces):
            send_piece(0, j, k)

    each(0, chunks, send_rows)
    each(1, count, lambda d: order_copy(d).start())

    row = iota((2 * LANES, 2 * LANES), 0)
    col = iota((2 * LANES, 2 * LANES), 1)
    apart = jnp.where(col == 2 * (row % LANES) + row // LANES, 1.0, 0.0).astype(bf16)

    def prepare(layer, j):
        def block(t):
            i = t * pieces + j
            rows = rows_of(i, LANES)
            to = rows_of(j * members + t, LANES)
            gain = in_gain_ref[layer : layer + 1, lanes_of(i, LANES)]
            gain = jnp.broadcast_to(gain, (LANES, LANES)).T
            both = raw_ref[rows].reshape(2 * LANES, inner)
            halves = jnp.dot(apart, both, preferred_element_type=f32)
            for p in range(inner // LANES):
                lanes = slice(p * LANES, (p + 1) * LANES)
                w_ref[to, lanes] = (halves[:LANES, lanes] * gain).astype(bf16)
                wz_ref[to, lanes] = (halves[LANES:, lanes] * gain).astype(bf16)
            for p in range(2 * STATE // LANES):
                lanes = slice(p * LANES, (p + 1) * LANES)
                w_ref[to, inner + p * LANES : inner + (p + 1) * LANES] = (
                    raw_bc_ref[rows, lanes].astype(f32) * gain
                ).astype(bf16)
            dt = w_dt_ref[layer, :, lanes_of(i, LANES)].astype(f32)
            dt = jnp.concatenate([dt, jnp.zeros((LANES - heads, LANES), f32)], axis=0)
            w_ref[to, mixed:] = (dt.T * gain).astype(bf16)

        each(0, members, block)

    spreader = spreader_of(heads, inner)
    line = iota((STRETCH, STRETCH), 0)
    lane = iota((STRETCH, STRETCH), 1)
    lower = line >= lane
    tri = jnp.where(lower, 1.0, 0.0).astype(bf16)
    left = iota((STRETCH, 2 * HEAD_DIM), 1) < HEAD_DIM

    def scale_of(v):
        wide = v.astype(f32)
        return lax.rsqrt(jnp.mean(wide * wide, axis=-1, keepdims=True) + epsilon)

    def scan(layer, arrive):
        for t in range(members):
            halo_copy(layer, t, t).wait_recv()
        ahead = jnp.concatenate(
            [
                halo_ref[layer, t, :, j * COLUMNS : (j + 1) * COLUMNS]
                for j in range(pieces) for t in range(members)
            ],
            axis=1,
        )
        ahead = jnp.dot(ahead, w_ref[:, :mixed], preferred_element_type=f32) * scale_of(ahead)
        ahead = ahead[HALO - 8 :, :].astype(bf16).astype(f32)
        ext_ref[0:8, :] = jnp.where(seq > 0, ahead, 0.0)
        state_ref[...] = jnp.zeros_like(state_ref)
        sofar_ref[...] = jnp.zeros_like(sofar_ref)
        bias = pad_row(bias_ref[layer : layer + 1, :])
        rate = pad_row(jnp.exp(a_log_ref[layer : layer + 1, :]))
        skip = pad_row(d_skip_ref[layer : layer + 1, :])
        skip = expand(jnp.broadcast_to(skip, (8, LANES)), heads, spreader)[0:1]
        taps = jnp.concatenate([conv_x_ref[layer], conv_bc_ref[layer]], axis=1)
        tap_count = taps.shape[0]

        def project(k):
            rows = rows_of(k, ROWS)
            arrive(k)
            tokens = jnp.concatenate([full_ref[j, rows, :] for j in range(pieces)], axis=1)
            scale = scale_of(tokens)
            scale_ref[rows, :] = jnp.broadcast_to(scale, (ROWS, LANES))
            projected = jnp.dot(tokens, w_ref[...], preferred_element_type=f32) * scale
            ext_ref[8 : 8 + ROWS, :] = projected[:, :mixed].astype(bf16).astype(f32)
            conv = jnp.zeros((ROWS, mixed), f32)
            for tap in range(tap_count):
                first = 9 - tap_count + tap
                conv = conv + taps[tap : tap + 1, :] * ext_ref[first : first + ROWS, :]
            conv = conv * jax.nn.sigmoid(conv)
            ext_ref[0:8, :] = ext_ref[ROWS : ROWS + 8, :]
            raw = projected[:, mixed:] + bias
            step = jnp.maximum(raw, 0.0) + jnp.log1p(jnp.exp(-jnp.abs(raw)))
            logs = -step * rate
            x = conv[:, :inner]
            b_all = conv[:, inner : inner + STATE]
            b_ref[rows, :] = b_all.astype(bf16)
            c_ref[rows, :] = conv[:, inner + STATE :].astype(bf16)
            feed = x * expand(step, heads, spreader)
            feed_ref[rows, :] = feed.astype(bf16)
            y_ref[rows, :] = skip * x
            state = state_ref[...]
            sofar = sofar_ref[...]
            for block in range(per):
                part = slice(block * STRETCH, (block + 1) * STRETCH)
                index = k * per + block
                cum = running_sum(tri, logs[part], heads)
                last = cum[STRETCH - 1 : STRETCH, :]
                factors = expand(
                    jnp.concatenate(
                        [
                            jnp.exp(last - cum),
                            jnp.exp(jnp.broadcast_to(last, (8, LANES))),
                            jnp.exp(sofar),
                        ],
                        axis=0,
                    ),
                    heads, spreader,
                )
                fresh = jnp.dot(
                    b_all[part].T.astype(bf16),
                    (feed[part] * factors[:STRETCH]).astype(bf16),
                    preferred_element_type=f32,
                )
                states_ref[index] = state
                sofar_exp_ref[index] = factors[STRETCH + 8 :]
                state = state * factors[STRETCH : STRETCH + 1] + fresh
                cum_ref[rows_of(index, STRETCH), :] = cum
                sofar = sofar + last
            state_ref[...] = state
            sofar_ref[...] = sofar

        each(0, chunks, project)

    def within(k):
        rows = rows_of(k, ROWS)
        tokens = jnp.concatenate([full_ref[j, rows, :] for j in range(pieces)], axis=1)
        gate = jnp.dot(tokens, wz_ref[...], preferred_element_type=f32)
        z_ref[rows, :] = (gate * scale_ref[rows, 0:1]).astype(bf16)

        def block(b):
            rows = rows_of(k * per + b, STRETCH)
            cum = cum_ref[rows, :]
            cum_t = cum.T
            feed = feed_ref[rows, :]
            meet = lax.dot_general(
                c_ref[rows, :], b_ref[rows, :], (((1,), (1,)), ((), ())),
                preferred_element_type=f32,
            )
            for pair in range(heads // 2):
                lanes = slice(pair * 2 * HEAD_DIM, (pair + 1) * 2 * HEAD_DIM)
                weights = []
                for h in (2 * pair, 2 * pair + 1):
                    spread = jnp.where(lower, cum[:, h : h + 1] - cum_t[h : h + 1, :], -jnp.inf)
                    weights.append((meet * jnp.exp(spread)).astype(bf16))
                fed = feed[:, lanes]
                nought = jnp.zeros_like(fed)
                stacked = jnp.concatenate(
                    [jnp.where(left, fed, nought), jnp.where(left, nought, fed)], axis=0
                )
                inside = jnp.dot(
                    jnp.concatenate(weights, axis=1), stacked, preferred_element_type=f32
                )
                y_ref[rows, lanes] = y_ref[rows, lanes] + inside

        each(0, per, block)

    def exchange(layer):
        def end_copy(d, place):
            other = (seq + d) % count
            return remote(
                end_ref.at[layer, other], got_ref.at[layer, place],
                end_send.at[layer, d - 1], end_recv.at[layer, d - 1], (other, own),
            )

        def log_copy(d, place):
            return remote(
                log_ref.at[layer], logs_ref.at[layer, place],
                log_send.at[layer, d - 1], log_recv.at[layer, d - 1], ((seq + d) % count, own),
            )

        def give_copy(d, place):
            other = (seq + d) % count
            return remote(
                give_ref.at[layer, other], arriving_ref.at[layer, place],
                give_send.at[layer, d - 1], give_recv.at[layer, d - 1], (other, own),
            )

        def sender(d):
            return (seq + count - d) % count

        state = state_ref[...]
        for d in range(count):
            end_ref[layer, d] = state[d * state_rows : (d + 1) * state_rows].astype(bf16)
        log_ref[layer] = sofar_ref[...]

        def send(d):
            log_copy(d, seq).start()
            end_copy(d, seq).start()

        each(1, count, send)
        each(0, chunks // 2, within)

        def receive(d):
            log_copy(d, sender(d)).wait_recv()
            end_copy(d, sender(d)).wait_recv()

        each(1, count, receive)
        got_ref[layer, seq] = end_ref[layer, seq]
        logs_ref[layer, seq] = log_ref[layer]
        logs = jnp.concatenate([logs_ref[layer, d, 0:1] for d in range(count)], axis=0)
        factors = expand(jnp.exp(logs), heads, spreader)
        prefix = jnp.zeros((state_rows, inner), f32)
        for d in range(count):
            give_ref[layer, d] = prefix.astype(bf16)
            if d + 1 < count:
                prefix = prefix * factors[d : d + 1] + got_ref[layer, d].astype(f32)
        each(1, count, lambda d: give_copy(d, seq).start())
        each(chunks // 2, chunks, within)
        each(1, count, lambda d: give_copy(d, sender(d)).wait_recv())
        arriving_ref[layer, seq] = give_ref[layer, seq]
        prefix_ref[...] = jnp.concatenate(
            [arriving_ref[layer, d].astype(f32) for d in range(count)], axis=0
        )

        def drain(d):
            log_copy(d, seq).wait_send()
            end_copy(d, seq).wait_send()
            give_copy(d, seq).wait_send()

        each(1, count, drain)

    pair = 2 * HEAD_DIM
    one = iota((2 * pair, pair), 0) % pair // HEAD_DIM
    two = iota((2 * pair, pair), 1) // HEAD_DIM
    averager = jnp.where(one == two, 1.0 / HEAD_DIM, 0.0).astype(bf16)

    def mixed_of(layer, k):
        rows = rows_of(k, ROWS)
        grown = expand(jnp.exp(cum_ref[rows, :]), heads, spreader)
        carried = []
        for block in range(per):
            index = k * per + block
            state = states_ref[index] + prefix_ref[...] * sofar_exp_ref[index][0:1]
            carried.append(
                jnp.dot(
                    c_ref[rows_of(index, STRETCH), :], state.astype(bf16),
                    preferred_element_type=f32,
                )
            )
        gate = z_ref[rows, :].astype(f32)
        ssd = y_ref[rows, :] + jnp.concatenate(carried, axis=0) * grown
        gated = ssd * (gate * jax.nn.sigmoid(gate))
        square = gated * gated
        high = square.astype(bf16)
        low = (square - high.astype(f32)).astype(bf16)
        results = []
        for p in range(inner // pair):
            lanes = slice(p * pair, (p + 1) * pair)
            both = jnp.concatenate([high[:, lanes], low[:, lanes]], axis=1)
            mean = jnp.dot(both, averager, preferred_element_type=f32)
            scaled = gated[:, lanes] * lax.rsqrt(mean + epsilon)
            results.append((scaled * out_gain_ref[layer : layer + 1, lanes]).astype(bf16))
        return jnp.concatenate(results, axis=1)

    sums = (
        (near_col_ref, sum_col_ref, far_col_ref, pieces),
        (near_row_ref, sum_row_ref, far_row_ref, chunks),
    )

    def part_of(layer, k, block):
        if layer == 0:
            return pl.ds(0, length), lanes_of(k * members + block, COLUMNS)
        return rows_of(k, ROWS), lanes_of(block, width)

    def near_part(layer, side, k):
        block = diagonal_id if side == 0 else near_id
        rows, lanes = part_of(layer, k, block)
        return remote(
            partial_ref.at[rows, lanes], sums[layer][0].at[side, k],
            near_send.at[layer, side, k], near_recv.at[layer, side, k], sibling,
        )

    def far_part(layer, k):
        return remote(
            sums[layer][1].at[k], sums[layer][2].at[k],
            far_send.at[layer, k], far_recv.at[layer, k], across,
        )

    def send_far(layer, k):
        near_ref, sum_ref = sums[layer][:2]
        near_part(layer, 0, k).wait_recv()
        rows, lanes = part_of(layer, k, across_id)
        sum_ref[k] = (
            partial_ref[rows, lanes].astype(f32) + near_ref[0, k].astype(f32)
        ).astype(bf16)
        far_part(layer, k).start()

    def send_near(layer, k):
        near_part(layer, 0, k).start()
        near_part(layer, 1, k).start()

        @pl.when(k > 0)
        def _():
            send_far(layer, k - 1)

    def summed(layer, k, stream):
        near_ref, far_ref = sums[layer][0], sums[layer][2]
        near_part(layer, 1, k).wait_recv()
        far_part(layer, k).wait_recv()
        rows, lanes = part_of(layer, k, own)
        return (
            stream.astype(f32)
            + partial_ref[rows, lanes].astype(f32)
            + near_ref[1, k].astype(f32)
            + far_ref[k].astype(f32)
        ).astype(bf16)

    def drain_sums(layer):
        def drain(k):
            near_part(layer, 0, k).wait_send()
            near_part(layer, 1, k).wait_send()
            far_part(layer, k).wait_send()

        each(0, sums[layer][3], drain)

    def plan():
        shift = length.bit_length() - 1
        each(1, count, lambda d: order_copy(d).wait_recv())
        orders_ref[seq] = order_ref[...]
        orders = jnp.concatenate([orders_ref[d] for d in range(count)], axis=0)

        def count_up(r):
            first = iota((LANES, length), 0) + r * LANES
            place_ref[rows_of(r, LANES), :] = jnp.where(
                first <= iota((LANES, length), 1), 1.0, 0.0
            ).astype(bf16)

        each(0, length // LANES, count_up)
        device = iota((count, length), 0)
        wanted_here = jnp.right_shift(orders, shift) == seq
        from_each = jnp.right_shift(order_ref[...], shift) == device
        ones = jnp.concatenate(
            [jnp.where(wanted_here, 1.0, 0.0), jnp.where(from_each, 1.0, 0.0)], axis=0
        ).astype(bf16)
        counted = jnp.dot(ones, place_ref[...], preferred_element_type=f32).astype(jnp.int32) - 1
        slot = jnp.where(wanted_here, counted[:count], -1)
        local = jnp.bitwise_and(orders, length - 1)
        short = iota((share, length), 0)
        long = iota((share, length), 1)
        for d in range(count):
            chosen = slot[d : d + 1, :] == short
            found = jnp.where(chosen, local[d : d + 1, :], 0).astype(f32)
            wanted = jnp.sum(found, axis=1, keepdims=True).astype(jnp.int32)
            hand_ref[d * share : (d + 1) * share, :] = jnp.where(
                wanted == long, 1.0, 0.0
            ).astype(bf16)
        target = jnp.where(from_each, counted[count:] + share * device, 0).astype(f32)
        target = jnp.sum(target, axis=0, keepdims=True)
        target = jnp.broadcast_to(target, (LANES, length)).T.astype(jnp.int32)
        for c in range(length // LANES):
            place_ref[:, c * LANES : (c + 1) * LANES] = jnp.where(
                target == iota((length, LANES), 1) + c * LANES, 1.0, 0.0
            ).astype(bf16)

    def move_copy(j, d):
        other = (seq + d) % count
        return remote(
            leaving_ref.at[j, rows_of(other, share)], arrived_ref.at[j, rows_of(seq, share)],
            move_send.at[j, d - 1], move_recv.at[j, d - 1], (other, own),
        )

    def move_arrival(j, d):
        other = (seq + count - d) % count
        return remote(
            leaving_ref.at[j, rows_of(other, share)], arrived_ref.at[j, rows_of(other, share)],
            move_send.at[j, d - 1], move_recv.at[j, d - 1], ((seq + d) % count, own),
        )

    def hand_over(j):
        held = summed(0, j, stream_ref[:, j * COLUMNS : (j + 1) * COLUMNS])
        leaving_ref[j] = jnp.dot(hand_ref[...], held, preferred_element_type=f32).astype(bf16)
        each(1, count, lambda d: move_copy(j, d).start())
        arrived_ref[j, rows_of(seq, share), :] = leaving_ref[j, rows_of(seq, share), :]

    def put(j):
        lanes = slice(j * COLUMNS, (j + 1) * COLUMNS)
        each(1, count, lambda d: move_arrival(j, d).wait_recv())
        rows = jnp.dot(place_ref[...], arrived_ref[j], preferred_element_type=f32).astype(bf16)
        out_ref[:, lanes] = rows
        full_ref[j, :, own_lanes] = rows
        tail_ref[:, lanes] = rows[length - HALO :]
        each(0, chunks, lambda k: send_piece(1, j, k))

    for copy in weight_loads(0):
        copy.wait()
    for j in range(pieces):
        prepare(0, j)
    for copy in weight_loads(1):
        copy.start()
    for copy in self_loads:
        copy.wait()

    def arrive_first(k):
        for j in range(pieces):
            forward_piece(0, j, k)
        for j in range(pieces):
            rest_of_piece(0, j, k)

    scan(0, arrive_first)
    exchange(0)
    gathered(0)
    for copy in wo_loads:
        copy.wait()

    def mix(k):
        mixed_ref[rows_of(k, ROWS), :] = mixed_of(0, k)

    each(0, chunks, mix)

    def output_columns(j):
        lanes = lanes_of(j, members * COLUMNS)

        def product(k):
            rows = rows_of(k, ROWS)
            partial_ref[rows, lanes] = jnp.dot(
                mixed_ref[rows, :], wo_col_ref[:, lanes], preferred_element_type=f32
            ).astype(bf16)

        each(0, chunks, product)
        send_near(0, j)

    each(0, pieces, output_columns)
    send_far(0, pieces - 1)
    plan()
    for copy in weight_loads(1):
        copy.wait()

    for j in range(pieces):
        hand_over(j)
        if j:
            put(j - 1)
        prepare(1, j)
    put(pieces - 1)
    for t in range(members):
        halo_copy(1, t, own).start()
    drain_sums(0)

    for j in range(pieces - 1):
        each(0, chunks, lambda k: forward_piece(1, j, k))

    def arrive_second(k):
        forward_piece(1, pieces - 1, k)
        for j in range(pieces):
            rest_of_piece(1, j, k)

    scan(1, arrive_second)
    exchange(1)

    def output_rows(k):
        partial_ref[rows_of(k, ROWS), :] = jnp.dot(
            mixed_of(1, k), wo_ref[...], preferred_element_type=f32
        ).astype(bf16)
        send_near(1, k)

    each(0, chunks, output_rows)
    send_far(1, chunks - 1)

    def finish(k):
        rows = rows_of(k, ROWS)
        out_ref[rows, :] = summed(1, k, out_ref[rows, :])

    each(0, chunks, finish)
    gathered(1)
    drain_sums(1)
    for layer in range(2):
        for t in range(members):
            halo_copy(layer, t, own).wait_send()

    def moved(d):
        order_copy(d).wait_send()
        for j in range(pieces):
            move_copy(j, d).wait_send()

    each(1, count, moved)


def body(
    tokens, col_order, in_gain, w_in, w_bc, w_dt, conv_x, conv_bc,
    dt_bias, a_log, d_skip, out_gain, w_out,
):
    count, members = lax.axis_size("seq"), lax.axis_size("tp")
    length, width = tokens.shape
    inner = w_out.shape[1]
    heads = inner // HEAD_DIM
    mixed = inner + 2 * STATE
    depth = w_in.shape[1]
    chunks = length // ROWS
    blocks = length // STRETCH
    pieces = width // COLUMNS
    peers = count - 1
    state_rows = STATE // count
    vmem = pl.BlockSpec(memory_space=pltpu.VMEM)
    hbm = pl.BlockSpec(memory_space=pl.ANY)
    dma = pltpu.SemaphoreType.DMA
    return pl.pallas_call(
        functools.partial(layers_kernel, count, members),
        in_specs=[vmem, vmem, vmem, hbm, hbm] + [vmem] * 7 + [hbm],
        out_specs=vmem,
        out_shape=jax.ShapeDtypeStruct(tokens.shape, bf16),
        scratch_shapes=[
            pltpu.VMEM((pieces, length, members * COLUMNS), bf16),
            pltpu.VMEM((HALO, width), bf16),
            pltpu.VMEM((2, members, HALO, width), bf16),
            pltpu.VMEM((count, 1, length), jnp.int32),
            pltpu.VMEM((depth, 2, inner), bf16),
            pltpu.VMEM((depth, 2 * STATE), bf16),
            pltpu.VMEM((depth, mixed + LANES), bf16),
            pltpu.VMEM((depth, inner), bf16),
            pltpu.VMEM((inner, depth), bf16),
            pltpu.VMEM((inner, depth), bf16),
            pltpu.VMEM((ROWS + 8, mixed), f32),
            pltpu.VMEM((length, inner), f32),
            pltpu.VMEM((length, inner), bf16),
            pltpu.VMEM((length, inner), bf16),
            pltpu.VMEM((length, STATE), bf16),
            pltpu.VMEM((length, STATE), bf16),
            pltpu.VMEM((length, LANES), f32),
            pltpu.VMEM((length, LANES), f32),
            pltpu.VMEM((blocks, STATE, inner), f32),
            pltpu.VMEM((blocks, 8, inner), f32),
            pltpu.VMEM((STATE, inner), f32),
            pltpu.VMEM((8, LANES), f32),
            pltpu.VMEM((2, count, state_rows, inner), bf16),
            pltpu.VMEM((2, 8, LANES), f32),
            pltpu.VMEM((2, count, state_rows, inner), bf16),
            pltpu.VMEM((2, count, 8, LANES), f32),
            pltpu.VMEM((2, count, state_rows, inner), bf16),
            pltpu.VMEM((2, count, state_rows, inner), bf16),
            pltpu.VMEM((STATE, inner), f32),
            pltpu.VMEM((length, depth), bf16),
            pltpu.VMEM((2, pieces, length, COLUMNS), bf16),
            pltpu.VMEM((pieces, length, COLUMNS), bf16),
            pltpu.VMEM((pieces, length, COLUMNS), bf16),
            pltpu.VMEM((2, chunks, ROWS, width), bf16),
            pltpu.VMEM((chunks, ROWS, width), bf16),
            pltpu.VMEM((chunks, ROWS, width), bf16),
            pltpu.VMEM((length, inner), bf16),
            pltpu.VMEM((length, length), bf16),
            pltpu.VMEM((length, length), bf16),
            pltpu.VMEM((pieces, length, COLUMNS), bf16),
            pltpu.VMEM((pieces, length, COLUMNS), bf16),
            dma((2, 2)), dma((pieces * members + 1,)), dma((pieces,)),
            dma((2, 3, pieces, chunks)), dma((2, 3, pieces, chunks)),
            dma((2, members)), dma((2, members)), dma((peers,)), dma((peers,)),
            dma((2, peers)), dma((2, peers)), dma((2, peers)), dma((2, peers)),
            dma((2, peers)), dma((2, peers)),
            dma((2, 2, max(pieces, chunks))), dma((2, 2, max(pieces, chunks))),
            dma((2, max(pieces, chunks))), dma((2, max(pieces, chunks))),
            dma((pieces, peers)), dma((pieces, peers)),
        ],
        compiler_params=pltpu.CompilerParams(
            collective_id=0, has_side_effects=True, vmem_limit_bytes=63 * 1024 * 1024
        ),
        name="mixer_layers",
    )(
        tokens, col_order[None], in_gain, w_in, w_bc, jnp.swapaxes(w_dt, 1, 2), conv_x, conv_bc,
        dt_bias, a_log, d_skip, out_gain, w_out,
    )


def solution(mesh):
    placed = (
        P("seq", "tp"),
        P("seq"),
        P(),
        P(None, None, None, "tp"),
        P(),
        P(None, None, "tp"),
        P(None, None, "tp"),
        P(),
        P(None, "tp"),
        P(None, "tp"),
        P(None, "tp"),
        P(None, "tp"),
        P(None, "tp", None),
    )
    return jax.shard_map(
        body, mesh=mesh, in_specs=placed, out_specs=P("seq", "tp"), check_vma=False
    )
```

```python
import functools

import jax
import jax.numpy as jnp
from jax import lax
from jax.experimental import pallas as pl
from jax.experimental.pallas import tpu as pltpu
from jax.sharding import PartitionSpec as P

HEAD_DIM = 64
STATE = 128
STRETCH = 128
LANES = 128
HALO = 16
ROWS = 256
COLUMNS = 128

epsilon = 1e-05
f32 = jnp.float32
bf16 = jnp.bfloat16
MESH = pl.DeviceIdType.MESH


def iota(shape, axis):
    return lax.broadcasted_iota(jnp.int32, shape, axis)


def spreader_of(heads, inner):
    row = iota((LANES, inner), 0)
    channel = iota((LANES, inner), 1)
    chosen = (row % heads == channel // HEAD_DIM) & (row < 3 * heads)
    return jnp.where(chosen, 1.0, 0.0).astype(bf16)


def pack_pieces(values, heads):
    values = jnp.where(iota(values.shape, 1) < heads, values, 0.0)
    high = values.astype(bf16).astype(f32)
    rest = values - high
    middle = rest.astype(bf16).astype(f32)
    low = rest - middle
    packed = high + pltpu.roll(middle, heads, 1) + pltpu.roll(low, 2 * heads, 1)
    return packed.astype(bf16)


def expand(values, heads, spreader):
    return jnp.dot(pack_pieces(values, heads), spreader, preferred_element_type=f32)


def running_sum(tri, logs, heads):
    parts = jnp.dot(tri, pack_pieces(logs, heads), preferred_element_type=f32)
    total = parts + pltpu.roll(parts, LANES - heads, 1) + pltpu.roll(parts, LANES - 2 * heads, 1)
    return jnp.where(iota(total.shape, 1) < heads, total, 0.0)


def rows_of(k, size):
    return pl.ds(pl.multiple_of(k * size, size), size)


def lanes_of(k, size):
    return pl.ds(pl.multiple_of(k * size, LANES), size)


def pad_row(row):
    return jnp.concatenate([row, jnp.zeros((1, LANES - row.shape[1]), f32)], axis=1)


def layers_kernel(
    count, members,
    stream_ref, order_ref, in_gain_ref, w_in_ref, w_bc_ref, w_dt_ref, conv_x_ref, conv_bc_ref,
    bias_ref, a_log_ref, d_skip_ref, out_gain_ref, w_out_ref,
    out_ref,
    full_ref, tail_ref, halo_ref, orders_ref, raw_ref, raw_bc_ref, w_ref, wz_ref, wo_col_ref, wo_ref,
    ext_ref, y_ref, z_ref, feed_ref, b_ref, c_ref, cum_ref, scale_ref, states_ref, sofar_exp_ref,
    state_ref, sofar_ref,
    end_ref, log_ref, got_ref, logs_ref, give_ref, arriving_ref, prefix_ref,
    partial_ref, near_col_ref, sum_col_ref, far_col_ref, near_row_ref, sum_row_ref, far_row_ref,
    mixed_ref, hand_ref, place_ref, leaving_ref, arrived_ref, held_ref, acc_ref,
    load_sem, wo_sem, self_sem, ag_send, ag_recv, halo_send, halo_recv, order_send, order_recv,
    end_send, end_recv, log_send, log_recv, give_send, give_recv,
    near_send, near_recv, far_send, far_recv, move_send, move_recv,
):
    seq = lax.axis_index("seq")
    own = lax.axis_index("tp")
    chip, core = own // 2, own % 2
    near_id = chip * 2 + 1 - core
    across_id = (1 - chip) * 2 + core
    diagonal_id = (1 - chip) * 2 + 1 - core
    sibling = (seq, near_id)
    across = (seq, across_id)
    length, width = stream_ref.shape
    depth = w_ref.shape[0]
    inner = y_ref.shape[1]
    mixed = inner + 2 * STATE
    heads = inner // HEAD_DIM
    chunks = length // ROWS
    per = ROWS // STRETCH
    blocks = length // STRETCH
    pieces = width // COLUMNS
    share = length // count
    state_rows = STATE // count
    following = (seq + 1) % count
    before = (seq + count - 1) % count

    def remote(src, dst, send, recv, device):
        return pltpu.make_async_remote_copy(
            src_ref=src, dst_ref=dst, send_sem=send, recv_sem=recv,
            device_id=device, device_id_type=MESH,
        )

    def each(first, last, act):
        def step(i, _):
            act(i)
            return 0

        lax.fori_loop(first, last, step, 0)

    greeted = [sibling, across]
    greeted += [(before, t) for t in range(members)]
    greeted += [((seq + d) % count, own) for d in range(1, count)]
    barrier = pltpu.get_barrier_semaphore()
    for device in greeted:
        pl.semaphore_signal(barrier, inc=1, device_id=device, device_id_type=MESH)

    def weight_loads(layer):
        return [
            pltpu.make_async_copy(w_in_ref.at[layer], raw_ref, load_sem.at[layer, 0]),
            pltpu.make_async_copy(w_bc_ref.at[layer], raw_bc_ref, load_sem.at[layer, 1]),
        ]

    own_lanes = lanes_of(own, COLUMNS)
    self_loads, wo_loads = [], []
    for j in range(pieces):
        self_loads.append(
            pltpu.make_async_copy(
                stream_ref.at[:, j * COLUMNS : (j + 1) * COLUMNS],
                full_ref.at[j, :, own_lanes], self_sem.at[j],
            )
        )
        for t in range(members):
            first = t * width + j * COLUMNS
            place = j * members + t
            wo_loads.append(
                pltpu.make_async_copy(
                    w_out_ref.at[0, :, first : first + COLUMNS],
                    wo_col_ref.at[:, place * COLUMNS : (place + 1) * COLUMNS],
                    wo_sem.at[place],
                )
            )
    wo_loads.append(pltpu.make_async_copy(w_out_ref.at[1], wo_ref, wo_sem.at[pieces * members]))
    for copy in weight_loads(0) + self_loads + wo_loads:
        copy.start()

    pl.semaphore_wait(barrier, len(greeted))

    last_piece = pieces - 1

    def block_of(layer, i, owner):
        lanes = lanes_of(owner, COLUMNS)
        if layer == 0:
            return full_ref.at[:, rows_of(i, ROWS), lanes], i
        if isinstance(i, int):
            return full_ref.at[i, :, lanes], chunks + i
        return full_ref.at[last_piece, rows_of(i[0], ROWS), lanes], chunks + last_piece + i[0]

    def gather_copy(layer, kind, i, owner):
        block, slot = block_of(layer, i, owner)
        return remote(
            block, block, ag_send.at[kind, slot], ag_recv.at[kind, slot],
            across if kind == 0 else sibling,
        )

    def send_rows(k):
        rows = rows_of(k, ROWS)
        for kind, device in ((0, across), (1, sibling)):
            for j in range(pieces):
                remote(
                    stream_ref.at[rows, lanes_of(j, COLUMNS)], full_ref.at[j, rows, own_lanes],
                    ag_send.at[kind, k], ag_recv.at[kind, k], device,
                ).start()

    def send_block(layer, i):
        gather_copy(layer, 0, i, own).start()
        gather_copy(layer, 1, i, own).start()

    def forward_block(layer, i):
        gather_copy(layer, 0, i, across_id).wait_recv()
        gather_copy(layer, 2, i, across_id).start()

    def rest_of_block(layer, i):
        gather_copy(layer, 1, i, near_id).wait_recv()
        gather_copy(layer, 2, i, diagonal_id).wait_recv()

    def drain_block(layer, i):
        gather_copy(layer, 0, i, own).wait_send()
        gather_copy(layer, 1, i, own).wait_send()
        gather_copy(layer, 2, i, across_id).wait_send()

    def halo_copy(layer, t, source):
        tail = tail_ref if layer else stream_ref.at[pl.ds(length - HALO, HALO)]
        return remote(
            tail, halo_ref.at[layer, source],
            halo_send.at[layer, t], halo_recv.at[layer, source], (following, t),
        )

    def halo_piece(j, t):
        lanes = lanes_of(j, COLUMNS)
        return remote(
            tail_ref.at[:, lanes], halo_ref.at[1, own, :, lanes],
            halo_send.at[1, t], halo_recv.at[1, own], (following, t),
        )

    def order_copy(d):
        return remote(
            order_ref, orders_ref.at[seq], order_send, order_recv, ((seq + d) % count, own)
        )

    def all_orders():
        others = orders_ref.at[pl.ds(0, count - 1)]
        return remote(others, others, order_send, order_recv, (following, own))

    for t in range(members):
        halo_copy(0, t, own).start()

    each(0, chunks, send_rows)
    each(1, count, lambda d: order_copy(d).start())

    row = iota((2 * LANES, 2 * LANES), 0)
    col = iota((2 * LANES, 2 * LANES), 1)
    apart = jnp.where(col == 2 * (row % LANES) + row // LANES, 1.0, 0.0).astype(bf16)

    def prepare(layer, j):
        def block(t):
            i = t * pieces + j
            rows = rows_of(i, LANES)
            to = rows_of(j * members + t, LANES)
            gain = in_gain_ref[layer : layer + 1, lanes_of(i, LANES)]
            gain = jnp.broadcast_to(gain, (LANES, LANES)).T
            both = raw_ref[rows].reshape(2 * LANES, inner)
            halves = jnp.dot(apart, both, preferred_element_type=f32)
            for p in range(inner // LANES):
                lanes = slice(p * LANES, (p + 1) * LANES)
                w_ref[to, lanes] = (halves[:LANES, lanes] * gain).astype(bf16)
                wz_ref[to, lanes] = (halves[LANES:, lanes] * gain).astype(bf16)
            for p in range(2 * STATE // LANES):
                lanes = slice(p * LANES, (p + 1) * LANES)
                w_ref[to, inner + p * LANES : inner + (p + 1) * LANES] = (
                    raw_bc_ref[rows, lanes].astype(f32) * gain
                ).astype(bf16)
            dt = w_dt_ref[layer, :, lanes_of(i, LANES)].astype(f32)
            dt = jnp.concatenate([dt, jnp.zeros((LANES - heads, LANES), f32)], axis=0)
            w_ref[to, mixed:] = (dt.T * gain).astype(bf16)

        each(0, members, block)

    spreader = spreader_of(heads, inner)
    line = iota((STRETCH, STRETCH), 0)
    lane = iota((STRETCH, STRETCH), 1)
    lower = line >= lane
    tri = jnp.where(lower, 1.0, 0.0).astype(bf16)
    left = iota((STRETCH, 2 * HEAD_DIM), 1) < HEAD_DIM

    def scale_of(v):
        wide = v.astype(f32)
        return lax.rsqrt(jnp.mean(wide * wide, axis=-1, keepdims=True) + epsilon)

    def scan(layer, arrive):
        for t in range(members):
            halo_copy(layer, t, t).wait_recv()
        ahead = jnp.concatenate(
            [
                halo_ref[layer, t, :, j * COLUMNS : (j + 1) * COLUMNS]
                for j in range(pieces) for t in range(members)
            ],
            axis=1,
        )
        ahead = jnp.dot(ahead, w_ref[:, :mixed], preferred_element_type=f32) * scale_of(ahead)
        ahead = ahead[HALO - 8 :, :].astype(bf16).astype(f32)
        ext_ref[0:8, :] = jnp.where(seq > 0, ahead, 0.0)
        state_ref[...] = jnp.zeros_like(state_ref)
        sofar_ref[...] = jnp.zeros_like(sofar_ref)
        bias = pad_row(bias_ref[layer : layer + 1, :])
        rate = pad_row(jnp.exp(a_log_ref[layer : layer + 1, :]))
        skip = pad_row(d_skip_ref[layer : layer + 1, :])
        skip = expand(jnp.broadcast_to(skip, (8, LANES)), heads, spreader)[0:1]
        taps = jnp.concatenate([conv_x_ref[layer], conv_bc_ref[layer]], axis=1)
        tap_count = taps.shape[0]

        def project(k):
            rows = rows_of(k, ROWS)
            arrive(k)
            tokens = jnp.concatenate([full_ref[j, rows, :] for j in range(pieces)], axis=1)
            scale = scale_of(tokens)
            scale_ref[rows, :] = jnp.broadcast_to(scale, (ROWS, LANES))
            if layer == 0:
                projected = jnp.dot(tokens, w_ref[...], preferred_element_type=f32)
            else:
                projected = acc_ref[rows, :] + jnp.dot(
                    full_ref[last_piece, rows, :], w_ref[last_piece * width :, :],
                    preferred_element_type=f32,
                )
            projected = projected * scale
            ext_ref[8 : 8 + ROWS, :] = projected[:, :mixed].astype(bf16).astype(f32)
            conv = jnp.zeros((ROWS, mixed), f32)
            for tap in range(tap_count):
                first = 9 - tap_count + tap
                conv = conv + taps[tap : tap + 1, :] * ext_ref[first : first + ROWS, :]
            conv = conv * jax.nn.sigmoid(conv)
            ext_ref[0:8, :] = ext_ref[ROWS : ROWS + 8, :]
            raw = projected[:, mixed:] + bias
            step = jnp.maximum(raw, 0.0) + jnp.log1p(jnp.exp(-jnp.abs(raw)))
            logs = -step * rate
            x = conv[:, :inner]
            b_all = conv[:, inner : inner + STATE]
            b_ref[rows, :] = b_all.astype(bf16)
            c_ref[rows, :] = conv[:, inner + STATE :].astype(bf16)
            feed = x * expand(step, heads, spreader)
            feed_ref[rows, :] = feed.astype(bf16)
            y_ref[rows, :] = skip * x
            state = state_ref[...]
            sofar = sofar_ref[...]
            for block in range(per):
                part = slice(block * STRETCH, (block + 1) * STRETCH)
                index = k * per + block
                cum = running_sum(tri, logs[part], heads)
                last = cum[STRETCH - 1 : STRETCH, :]
                factors = expand(
                    jnp.concatenate(
                        [
                            jnp.exp(last - cum),
                            jnp.exp(jnp.broadcast_to(last, (8, LANES))),
                            jnp.exp(sofar),
                        ],
                        axis=0,
                    ),
                    heads, spreader,
                )
                fresh = jnp.dot(
                    b_all[part].T.astype(bf16),
                    (feed[part] * factors[:STRETCH]).astype(bf16),
                    preferred_element_type=f32,
                )
                states_ref[index] = state
                sofar_exp_ref[index] = factors[STRETCH + 8 :]
                state = state * factors[STRETCH : STRETCH + 1] + fresh
                cum_ref[rows_of(index, STRETCH), :] = cum
                sofar = sofar + last
            state_ref[...] = state
            sofar_ref[...] = sofar

        each(0, chunks, project)

    def within(k):
        rows = rows_of(k, ROWS)
        tokens = jnp.concatenate([full_ref[j, rows, :] for j in range(pieces)], axis=1)
        gate = jnp.dot(tokens, wz_ref[...], preferred_element_type=f32)
        z_ref[rows, :] = (gate * scale_ref[rows, 0:1]).astype(bf16)

        def block(b):
            rows = rows_of(k * per + b, STRETCH)
            cum = cum_ref[rows, :]
            cum_t = cum.T
            feed = feed_ref[rows, :]
            meet = lax.dot_general(
                c_ref[rows, :], b_ref[rows, :], (((1,), (1,)), ((), ())),
                preferred_element_type=f32,
            )
            for pair in range(heads // 2):
                lanes = slice(pair * 2 * HEAD_DIM, (pair + 1) * 2 * HEAD_DIM)
                weights = []
                for h in (2 * pair, 2 * pair + 1):
                    spread = jnp.where(lower, cum[:, h : h + 1] - cum_t[h : h + 1, :], -jnp.inf)
                    weights.append((meet * jnp.exp(spread)).astype(bf16))
                fed = feed[:, lanes]
                nought = jnp.zeros_like(fed)
                stacked = jnp.concatenate(
                    [jnp.where(left, fed, nought), jnp.where(left, nought, fed)], axis=0
                )
                inside = jnp.dot(
                    jnp.concatenate(weights, axis=1), stacked, preferred_element_type=f32
                )
                y_ref[rows, lanes] = y_ref[rows, lanes] + inside

        each(0, per, block)

    def exchange(layer):
        def end_copy(d):
            other = (seq + d) % count
            return remote(
                end_ref.at[layer, other], got_ref.at[layer, seq],
                end_send.at[layer], end_recv.at[layer], (other, own),
            )

        def log_copy(d):
            return remote(
                log_ref.at[layer], logs_ref.at[layer, seq],
                log_send.at[layer], log_recv.at[layer], ((seq + d) % count, own),
            )

        def give_copy(d):
            other = (seq + d) % count
            return remote(
                give_ref.at[layer, other], arriving_ref.at[layer, seq],
                give_send.at[layer], give_recv.at[layer], (other, own),
            )

        others = pl.ds(0, count - 1)

        def all_of(ref, send, recv):
            block = ref.at[layer, others]
            return remote(block, block, send.at[layer], recv.at[layer], (following, own))

        all_ends = all_of(got_ref, end_send, end_recv)
        all_logs = all_of(logs_ref, log_send, log_recv)
        all_given = all_of(arriving_ref, give_send, give_recv)

        state = state_ref[...]
        for d in range(count):
            end_ref[layer, d] = state[d * state_rows : (d + 1) * state_rows].astype(bf16)
        log_ref[layer] = sofar_ref[...]

        def send(d):
            log_copy(d).start()
            end_copy(d).start()

        each(1, count, send)
        each(0, chunks // 2, within)
        all_logs.wait_recv()
        all_ends.wait_recv()
        got_ref[layer, seq] = end_ref[layer, seq]
        logs_ref[layer, seq] = log_ref[layer]
        logs = jnp.concatenate([logs_ref[layer, d, 0:1] for d in range(count)], axis=0)
        factors = expand(jnp.exp(logs), heads, spreader)
        prefix = jnp.zeros((state_rows, inner), f32)
        for d in range(count):
            give_ref[layer, d] = prefix.astype(bf16)
            if d + 1 < count:
                prefix = prefix * factors[d : d + 1] + got_ref[layer, d].astype(f32)
        each(1, count, lambda d: give_copy(d).start())
        each(chunks // 2, chunks, within)
        all_given.wait_recv()
        arriving_ref[layer, seq] = give_ref[layer, seq]
        prefix_ref[...] = jnp.concatenate(
            [arriving_ref[layer, d].astype(f32) for d in range(count)], axis=0
        )

        all_logs.wait_send()
        all_ends.wait_send()
        all_given.wait_send()

    pair = 2 * HEAD_DIM
    one = iota((2 * pair, pair), 0) % pair // HEAD_DIM
    two = iota((2 * pair, pair), 1) // HEAD_DIM
    averager = jnp.where(one == two, 1.0 / HEAD_DIM, 0.0).astype(bf16)

    def mixed_of(layer, k):
        rows = rows_of(k, ROWS)
        grown = expand(jnp.exp(cum_ref[rows, :]), heads, spreader)
        carried = []
        for block in range(per):
            index = k * per + block
            state = states_ref[index] + prefix_ref[...] * sofar_exp_ref[index][0:1]
            carried.append(
                jnp.dot(
                    c_ref[rows_of(index, STRETCH), :], state.astype(bf16),
                    preferred_element_type=f32,
                )
            )
        gate = z_ref[rows, :].astype(f32)
        ssd = y_ref[rows, :] + jnp.concatenate(carried, axis=0) * grown
        gated = ssd * (gate * jax.nn.sigmoid(gate))
        square = gated * gated
        high = square.astype(bf16)
        low = (square - high.astype(f32)).astype(bf16)
        results = []
        for p in range(inner // pair):
            lanes = slice(p * pair, (p + 1) * pair)
            both = jnp.concatenate([high[:, lanes], low[:, lanes]], axis=1)
            mean = jnp.dot(both, averager, preferred_element_type=f32)
            scaled = gated[:, lanes] * lax.rsqrt(mean + epsilon)
            results.append((scaled * out_gain_ref[layer : layer + 1, lanes]).astype(bf16))
        return jnp.concatenate(results, axis=1)

    def part_of(layer, i):
        if layer == 1:
            rows = rows_of(i, ROWS)
            blocks_of = [ref.at[rows] for ref in (sum_row_ref, far_row_ref)]
            nears = [near_row_ref.at[side, rows] for side in range(2)]
            return rows, lambda t: lanes_of(t, width), nears, blocks_of, i
        if isinstance(i, int):
            rows, j, slot = pl.ds(0, length), i, chunks + i - 1
        else:
            rows, j, slot = rows_of(i[0], ROWS), 0, i[0]
        blocks_of = [ref.at[j, rows] for ref in (sum_col_ref, far_col_ref)]
        nears = [near_col_ref.at[side, j, rows] for side in range(2)]
        return rows, lambda t: lanes_of(j * members + t, COLUMNS), nears, blocks_of, slot

    def near_part(layer, side, i):
        rows, lanes, nears, _, slot = part_of(layer, i)
        block = diagonal_id if side == 0 else near_id
        return remote(
            partial_ref.at[rows, lanes(block)], nears[side],
            near_send.at[layer, side, slot], near_recv.at[layer, side, slot], sibling,
        )

    def far_part(layer, i):
        _, _, _, (summing, far), slot = part_of(layer, i)
        return remote(summing, far, far_send.at[layer, slot], far_recv.at[layer, slot], across)

    def send_near(layer, i):
        near_part(layer, 0, i).start()
        near_part(layer, 1, i).start()

    def send_far(layer, i):
        rows, lanes, nears, (summing, _), _ = part_of(layer, i)
        near_part(layer, 0, i).wait_recv()
        summing[...] = (
            partial_ref[rows, lanes(across_id)].astype(f32) + nears[0][...].astype(f32)
        ).astype(bf16)
        far_part(layer, i).start()

    def summed(layer, i, stream):
        rows, lanes, nears, (_, far), _ = part_of(layer, i)
        near_part(layer, 1, i).wait_recv()
        far_part(layer, i).wait_recv()
        return (
            stream.astype(f32)
            + partial_ref[rows, lanes(own)].astype(f32)
            + nears[1][...].astype(f32)
            + far[...].astype(f32)
        ).astype(bf16)

    def drain_part(layer, i):
        near_part(layer, 0, i).wait_send()
        near_part(layer, 1, i).wait_send()
        far_part(layer, i).wait_send()

    def plan():
        shift = length.bit_length() - 1
        all_orders().wait_recv()
        orders_ref[seq] = order_ref[...]
        orders = jnp.concatenate([orders_ref[d] for d in range(count)], axis=0)

        def count_up(r):
            first = iota((LANES, length), 0) + r * LANES
            place_ref[rows_of(r, LANES), :] = jnp.where(
                first <= iota((LANES, length), 1), 1.0, 0.0
            ).astype(bf16)

        each(0, length // LANES, count_up)
        device = iota((count, length), 0)
        wanted_here = jnp.right_shift(orders, shift) == seq
        from_each = jnp.right_shift(order_ref[...], shift) == device
        ones = jnp.concatenate(
            [jnp.where(wanted_here, 1.0, 0.0), jnp.where(from_each, 1.0, 0.0)], axis=0
        ).astype(bf16)
        counted = jnp.dot(ones, place_ref[...], preferred_element_type=f32).astype(jnp.int32) - 1
        slot = jnp.where(wanted_here, counted[:count], -1)
        local = jnp.bitwise_and(orders, length - 1)
        short = iota((share, length), 0)
        long = iota((share, length), 1)
        for d in range(count):
            chosen = slot[d : d + 1, :] == short
            found = jnp.where(chosen, local[d : d + 1, :], 0).astype(f32)
            wanted = jnp.sum(found, axis=1, keepdims=True).astype(jnp.int32)
            hand_ref[d * share : (d + 1) * share, :] = jnp.where(
                wanted == long, 1.0, 0.0
            ).astype(bf16)
        target = jnp.where(from_each, counted[count:] + share * device, 0).astype(f32)
        target = jnp.sum(target, axis=0, keepdims=True)
        target = jnp.broadcast_to(target, (LANES, length)).T.astype(jnp.int32)
        for c in range(length // LANES):
            place_ref[:, c * LANES : (c + 1) * LANES] = jnp.where(
                target == iota((length, LANES), 1) + c * LANES, 1.0, 0.0
            ).astype(bf16)

    def move_copy(j, d):
        other = (seq + d) % count
        return remote(
            leaving_ref.at[j, rows_of(other, share)], arrived_ref.at[j, rows_of(seq, share)],
            move_send.at[j], move_recv.at[j], (other, own),
        )

    def all_moves(j):
        others = arrived_ref.at[j, pl.ds(0, length - share)]
        return remote(others, others, move_send.at[j], move_recv.at[j], (following, own))

    def hand_over(j):
        if j:
            held = summed(0, j, stream_ref[:, j * COLUMNS : (j + 1) * COLUMNS])
        else:

            def first(k):
                rows = rows_of(k, ROWS)
                held_ref[rows, :] = summed(0, (k,), stream_ref[rows, :COLUMNS])

            each(0, chunks, first)
            held = held_ref[...]
        leaving_ref[j] = jnp.dot(hand_ref[...], held, preferred_element_type=f32).astype(bf16)
        each(1, count, lambda d: move_copy(j, d).start())
        arrived_ref[j, rows_of(seq, share), :] = leaving_ref[j, rows_of(seq, share), :]

    def put(j):
        lanes = slice(j * COLUMNS, (j + 1) * COLUMNS)
        all_moves(j).wait_recv()
        rows = jnp.dot(place_ref[...], arrived_ref[j], preferred_element_type=f32).astype(bf16)
        tail_ref[:, lanes] = rows[length - HALO :]
        full_ref[j, :, own_lanes] = rows
        for t in range(members):
            halo_piece(j, t).start()
        if j < last_piece:
            send_block(1, j)
        else:
            each(0, chunks, lambda k: send_block(1, (k,)))
        out_ref[:, lanes] = rows

    def accumulate(j):
        part = slice(j * width, (j + 1) * width)

        def product(k):
            rows = rows_of(k, ROWS)
            result = jnp.dot(
                full_ref[j, rows, :], w_ref[part, :], preferred_element_type=f32
            )
            acc_ref[rows, :] = result if j == 0 else acc_ref[rows, :] + result

        each(0, chunks, product)

    for copy in weight_loads(0):
        copy.wait()
    for j in range(pieces):
        prepare(0, j)
    for copy in weight_loads(1):
        copy.start()
    for copy in self_loads:
        copy.wait()

    def arrive_first(k):
        forward_block(0, k)
        rest_of_block(0, k)

    scan(0, arrive_first)
    exchange(0)
    each(0, chunks, lambda k: drain_block(0, k))
    for copy in wo_loads:
        copy.wait()

    def product_of(k, j):
        rows, lanes = rows_of(k, ROWS), lanes_of(j, members * COLUMNS)
        partial_ref[rows, lanes] = jnp.dot(
            mixed_ref[rows, :], wo_col_ref[:, lanes], preferred_element_type=f32
        ).astype(bf16)

    def mix(k):
        mixed_ref[rows_of(k, ROWS), :] = mixed_of(0, k)
        product_of(k, 0)
        send_near(0, (k,))

        @pl.when(k > 0)
        def _():
            send_far(0, (k - 1,))

    each(0, chunks, mix)
    for j in range(1, pieces):
        each(0, chunks, lambda k: product_of(k, j))
        send_near(0, j)
        send_far(0, j - 1 if j > 1 else (chunks - 1,))
    send_far(0, pieces - 1)
    plan()
    for copy in weight_loads(1):
        copy.wait()

    for j in range(pieces):
        hand_over(j)
        if j:
            put(j - 1)
        prepare(1, j)
    put(pieces - 1)
    each(0, chunks, lambda k: drain_part(0, (k,)))
    for j in range(1, pieces):
        drain_part(0, j)

    for j in range(last_piece):
        forward_block(1, j)
        rest_of_block(1, j)
        accumulate(j)
    forward_block(1, (0,))

    def arrive_second(k):
        @pl.when(k + 1 < chunks)
        def _():
            forward_block(1, (k + 1,))

        rest_of_block(1, (k,))

    scan(1, arrive_second)
    exchange(1)

    def output_rows(k):
        partial_ref[rows_of(k, ROWS), :] = jnp.dot(
            mixed_of(1, k), wo_ref[...], preferred_element_type=f32
        ).astype(bf16)
        send_near(1, k)

        @pl.when(k > 0)
        def _():
            send_far(1, k - 1)

    each(0, chunks, output_rows)
    send_far(1, chunks - 1)

    def finish(k):
        rows = rows_of(k, ROWS)
        out_ref[rows, :] = summed(1, k, out_ref[rows, :])

    each(0, chunks, finish)
    for j in range(last_piece):
        drain_block(1, j)

    def drain_last(k):
        drain_block(1, (k,))
        drain_part(1, k)

    each(0, chunks, drain_last)
    for layer in range(2):
        for t in range(members):
            halo_copy(layer, t, own).wait_send()
    all_orders().wait_send()
    for j in range(pieces):
        all_moves(j).wait_send()


def body(
    tokens, col_order, in_gain, w_in, w_bc, w_dt, conv_x, conv_bc,
    dt_bias, a_log, d_skip, out_gain, w_out,
):
    count, members = lax.axis_size("seq"), lax.axis_size("tp")
    length, width = tokens.shape
    inner = w_out.shape[1]
    heads = inner // HEAD_DIM
    mixed = inner + 2 * STATE
    depth = w_in.shape[1]
    chunks = length // ROWS
    blocks = length // STRETCH
    pieces = width // COLUMNS
    state_rows = STATE // count
    vmem = pl.BlockSpec(memory_space=pltpu.VMEM)
    hbm = pl.BlockSpec(memory_space=pl.ANY)
    dma = pltpu.SemaphoreType.DMA
    return pl.pallas_call(
        functools.partial(layers_kernel, count, members),
        in_specs=[vmem, vmem, vmem, hbm, hbm] + [vmem] * 7 + [hbm],
        out_specs=vmem,
        out_shape=jax.ShapeDtypeStruct(tokens.shape, bf16),
        scratch_shapes=[
            pltpu.VMEM((pieces, length, members * COLUMNS), bf16),
            pltpu.VMEM((HALO, width), bf16),
            pltpu.VMEM((2, members, HALO, width), bf16),
            pltpu.VMEM((count, 1, length), jnp.int32),
            pltpu.VMEM((depth, 2, inner), bf16),
            pltpu.VMEM((depth, 2 * STATE), bf16),
            pltpu.VMEM((depth, mixed + LANES), bf16),
            pltpu.VMEM((depth, inner), bf16),
            pltpu.VMEM((inner, depth), bf16),
            pltpu.VMEM((inner, depth), bf16),
            pltpu.VMEM((ROWS + 8, mixed), f32),
            pltpu.VMEM((length, inner), f32),
            pltpu.VMEM((length, inner), bf16),
            pltpu.VMEM((length, inner), bf16),
            pltpu.VMEM((length, STATE), bf16),
            pltpu.VMEM((length, STATE), bf16),
            pltpu.VMEM((length, LANES), f32),
            pltpu.VMEM((length, LANES), f32),
            pltpu.VMEM((blocks, STATE, inner), f32),
            pltpu.VMEM((blocks, 8, inner), f32),
            pltpu.VMEM((STATE, inner), f32),
            pltpu.VMEM((8, LANES), f32),
            pltpu.VMEM((2, count, state_rows, inner), bf16),
            pltpu.VMEM((2, 8, LANES), f32),
            pltpu.VMEM((2, count, state_rows, inner), bf16),
            pltpu.VMEM((2, count, 8, LANES), f32),
            pltpu.VMEM((2, count, state_rows, inner), bf16),
            pltpu.VMEM((2, count, state_rows, inner), bf16),
            pltpu.VMEM((STATE, inner), f32),
            pltpu.VMEM((length, depth), bf16),
            pltpu.VMEM((2, pieces, length, COLUMNS), bf16),
            pltpu.VMEM((pieces, length, COLUMNS), bf16),
            pltpu.VMEM((pieces, length, COLUMNS), bf16),
            pltpu.VMEM((2, length, width), bf16),
            pltpu.VMEM((length, width), bf16),
            pltpu.VMEM((length, width), bf16),
            pltpu.VMEM((length, inner), bf16),
            pltpu.VMEM((length, length), bf16),
            pltpu.VMEM((length, length), bf16),
            pltpu.VMEM((pieces, length, COLUMNS), bf16),
            pltpu.VMEM((pieces, length, COLUMNS), bf16),
            pltpu.VMEM((length, COLUMNS), bf16),
            pltpu.VMEM((length, mixed + LANES), f32),
            dma((2, 2)), dma((pieces * members + 1,)), dma((pieces,)),
            dma((3, 2 * chunks + pieces - 1)), dma((3, 2 * chunks + pieces - 1)),
            dma((2, members)), dma((2, members)), dma, dma,
            dma((2,)), dma((2,)), dma((2,)), dma((2,)), dma((2,)), dma((2,)),
            dma((2, 2, chunks + pieces - 1)), dma((2, 2, chunks + pieces - 1)),
            dma((2, chunks + pieces - 1)), dma((2, chunks + pieces - 1)),
            dma((pieces,)), dma((pieces,)),
        ],
        compiler_params=pltpu.CompilerParams(
            collective_id=0, has_side_effects=True, vmem_limit_bytes=63 * 1024 * 1024
        ),
        name="mixer_layers",
    )(
        tokens, col_order[None], in_gain, w_in, w_bc, jnp.swapaxes(w_dt, 1, 2), conv_x, conv_bc,
        dt_bias, a_log, d_skip, out_gain, w_out,
    )


def solution(mesh):
    placed = (
        P("seq", "tp"),
        P("seq"),
        P(),
        P(None, None, None, "tp"),
        P(),
        P(None, None, "tp"),
        P(None, None, "tp"),
        P(),
        P(None, "tp"),
        P(None, "tp"),
        P(None, "tp"),
        P(None, "tp"),
        P(None, "tp", None),
    )
    return jax.shard_map(
        body, mesh=mesh, in_specs=placed, out_specs=P("seq", "tp"), check_vma=False
    )
```

```python
import functools

import jax
import jax.numpy as jnp
from jax import lax
from jax.experimental import pallas as pl
from jax.experimental.pallas import tpu as pltpu
from jax.sharding import PartitionSpec as P

HEAD_DIM = 64
STATE = 128
STRETCH = 128
LANES = 128
HALO = 16
ROWS = 256
FINE = 128
COLUMNS = 128

epsilon = 1e-05
f32 = jnp.float32
bf16 = jnp.bfloat16
MESH = pl.DeviceIdType.MESH


def iota(shape, axis):
    return lax.broadcasted_iota(jnp.int32, shape, axis)


def spreader_of(heads, inner):
    row = iota((LANES, inner), 0)
    channel = iota((LANES, inner), 1)
    chosen = (row % heads == channel // HEAD_DIM) & (row < 3 * heads)
    return jnp.where(chosen, 1.0, 0.0).astype(bf16)


def pack_pieces(values, heads):
    values = jnp.where(iota(values.shape, 1) < heads, values, 0.0)
    high = values.astype(bf16).astype(f32)
    rest = values - high
    middle = rest.astype(bf16).astype(f32)
    low = rest - middle
    packed = high + pltpu.roll(middle, heads, 1) + pltpu.roll(low, 2 * heads, 1)
    return packed.astype(bf16)


def expand(values, heads, spreader):
    return jnp.dot(pack_pieces(values, heads), spreader, preferred_element_type=f32)


def unpack_sum(pieces, heads):
    total = (
        pieces
        + pltpu.roll(pieces, LANES - heads, 1)
        + pltpu.roll(pieces, LANES - 2 * heads, 1)
    )
    return jnp.where(iota(total.shape, 1) < heads, total, 0.0)


def rows_of(k, size):
    return pl.ds(pl.multiple_of(k * size, size), size)


def lanes_of(k, size):
    return pl.ds(pl.multiple_of(k * size, LANES), size)


def pad_row(row):
    return jnp.concatenate([row, jnp.zeros((1, LANES - row.shape[1]), f32)], axis=1)


def layers_kernel(
    count, members,
    stream_ref, order_ref, in_gain_ref, w_in_ref, w_bc_ref, w_dt_ref, conv_x_ref, conv_bc_ref,
    bias_ref, a_log_ref, d_skip_ref, out_gain_ref, w_out_ref,
    out_ref,
    full_ref, tail_ref, halo_ref, orders_ref, raw_ref, raw_bc_ref, w_ref, wz_ref, wo_col_ref, wo_ref,
    ext_ref, y_ref, z_ref, feed_ref, b_ref, c_ref, cum_ref, scale_ref, states_ref, sofar_exp_ref,
    state_ref, sofar_ref,
    end_ref, log_ref, got_ref, logs_ref, give_ref, arriving_ref, prefix_ref,
    partial_ref, near_col_ref, sum_col_ref, far_col_ref, near_row_ref, sum_row_ref, far_row_ref,
    mixed_ref, hand_ref, place_ref, leaving_ref, arrived_ref, held_ref, acc_ref, own_ref,
    load_sem, wo_sem, self_sem, ag_send, ag_recv, halo_send, halo_recv, order_send, order_recv,
    end_send, end_recv, log_send, log_recv, give_send, give_recv,
    near_send, near_recv, far_send, far_recv, move_send, move_recv, out_sem,
):
    seq = lax.axis_index("seq")
    own = lax.axis_index("tp")
    chip, core = own // 2, own % 2
    near_id = chip * 2 + 1 - core
    across_id = (1 - chip) * 2 + core
    diagonal_id = (1 - chip) * 2 + 1 - core
    sibling = (seq, near_id)
    across = (seq, across_id)
    length, width = stream_ref.shape
    depth = w_ref.shape[0]
    inner = y_ref.shape[1]
    mixed = inner + 2 * STATE
    heads = inner // HEAD_DIM
    chunks = length // ROWS
    fines = length // FINE
    per = ROWS // STRETCH
    blocks = length // STRETCH
    pieces = width // COLUMNS
    share = length // count
    state_rows = STATE // count
    following = (seq + 1) % count
    before = (seq + count - 1) % count

    def remote(src, dst, send, recv, device):
        return pltpu.make_async_remote_copy(
            src_ref=src, dst_ref=dst, send_sem=send, recv_sem=recv,
            device_id=device, device_id_type=MESH,
        )

    def other_of(i):
        low = seq < count // 2
        other = jnp.where(low, count - 1 - i, i)
        return jnp.where(low, other - (other <= seq), other + (other >= seq))

    def each(first, last, act):
        def step(i, _):
            act(i)
            return 0

        lax.fori_loop(first, last, step, 0)

    greeted = [sibling, across]
    greeted += [(before, t) for t in range(members)]
    greeted += [((seq + d) % count, own) for d in range(1, count)]
    barrier = pltpu.get_barrier_semaphore()
    for device in greeted:
        pl.semaphore_signal(barrier, inc=1, device_id=device, device_id_type=MESH)

    def weight_loads(layer):
        return [
            pltpu.make_async_copy(w_in_ref.at[layer], raw_ref, load_sem.at[layer, 0]),
            pltpu.make_async_copy(w_bc_ref.at[layer], raw_bc_ref, load_sem.at[layer, 1]),
        ]

    own_lanes = lanes_of(own, COLUMNS)
    self_loads, wo_loads = [], []
    for j in range(pieces):
        self_loads.append(
            pltpu.make_async_copy(
                stream_ref.at[:, j * COLUMNS : (j + 1) * COLUMNS],
                full_ref.at[j, :, own_lanes], self_sem,
            )
        )
        for t in range(members):
            first = t * width + j * COLUMNS
            place = j * members + t
            wo_loads.append(
                pltpu.make_async_copy(
                    w_out_ref.at[0, :, first : first + COLUMNS],
                    wo_col_ref.at[:, place * COLUMNS : (place + 1) * COLUMNS],
                    wo_sem.at[0],
                )
            )
    wo_loads.append(pltpu.make_async_copy(w_out_ref.at[1], wo_ref, wo_sem.at[1]))
    for copy in weight_loads(0) + self_loads + wo_loads:
        copy.start()

    pl.semaphore_wait(barrier, len(greeted))

    last_piece = pieces - 1

    def block_of(layer, i, owner):
        lanes = lanes_of(owner, COLUMNS)
        if layer == 0:
            return full_ref.at[:, rows_of(i, FINE), lanes], i
        if isinstance(i, int):
            return full_ref.at[i, :, lanes], fines + i
        return full_ref.at[last_piece, rows_of(i[0], ROWS), lanes], fines + last_piece + i[0]

    def gather_copy(layer, kind, i, owner):
        block, slot = block_of(layer, i, owner)
        return remote(
            block, block, ag_send.at[layer, kind], ag_recv.at[kind, slot],
            across if kind == 0 else sibling,
        )

    def send_rows(k):
        rows = rows_of(k, FINE)
        for kind, device in ((0, across), (1, sibling)):
            for j in range(pieces):
                remote(
                    stream_ref.at[rows, lanes_of(j, COLUMNS)], full_ref.at[j, rows, own_lanes],
                    ag_send.at[0, kind], ag_recv.at[kind, k], device,
                ).start()

    def send_block(layer, i):
        gather_copy(layer, 0, i, own).start()
        gather_copy(layer, 1, i, own).start()

    def forward_block(layer, i):
        gather_copy(layer, 0, i, across_id).wait_recv()
        gather_copy(layer, 2, i, across_id).start()

    def rest_of_block(layer, i):
        gather_copy(layer, 1, i, near_id).wait_recv()
        gather_copy(layer, 2, i, diagonal_id).wait_recv()

    def drain_gather(layer):
        for kind, owner in ((0, own), (1, own), (2, across_id)):
            block = full_ref.at[:, :, lanes_of(owner, COLUMNS)]
            remote(block, block, ag_send.at[layer, kind], ag_recv.at[kind, 0], sibling).wait_send()

    def halo_copy(layer, t, source):
        tail = tail_ref if layer else stream_ref.at[pl.ds(length - HALO, HALO)]
        return remote(
            tail, halo_ref.at[layer, source],
            halo_send.at[layer], halo_recv.at[layer, source], (following, t),
        )

    def halo_piece(j, t):
        lanes = lanes_of(j, COLUMNS)
        return remote(
            tail_ref.at[:, lanes], halo_ref.at[1, own, :, lanes],
            halo_send.at[1], halo_recv.at[1, own], (following, t),
        )

    def order_copy(d):
        return remote(
            order_ref, orders_ref.at[seq], order_send, order_recv, (other_of(d), own)
        )

    def all_orders():
        others = orders_ref.at[pl.ds(0, count - 1)]
        return remote(others, others, order_send, order_recv, (following, own))

    for t in range(members):
        halo_copy(0, t, own).start()

    each(0, fines, send_rows)
    each(0, count - 1, lambda d: order_copy(d).start())

    row = iota((2 * LANES, 2 * LANES), 0)
    col = iota((2 * LANES, 2 * LANES), 1)
    apart = jnp.where(col == 2 * (row % LANES) + row // LANES, 1.0, 0.0).astype(bf16)

    def prepare(layer, j):
        def block(t):
            i = t * pieces + j
            rows = rows_of(i, LANES)
            to = rows_of(j * members + t, LANES)
            gain = in_gain_ref[layer : layer + 1, lanes_of(i, LANES)]
            gain = jnp.broadcast_to(gain, (LANES, LANES)).T
            both = raw_ref[rows].reshape(2 * LANES, inner)
            halves = jnp.dot(apart, both, preferred_element_type=f32)
            for p in range(inner // LANES):
                lanes = slice(p * LANES, (p + 1) * LANES)
                w_ref[to, lanes] = (halves[:LANES, lanes] * gain).astype(bf16)
                wz_ref[to, lanes] = (halves[LANES:, lanes] * gain).astype(bf16)
            for p in range(2 * STATE // LANES):
                lanes = slice(p * LANES, (p + 1) * LANES)
                w_ref[to, inner + p * LANES : inner + (p + 1) * LANES] = (
                    raw_bc_ref[rows, lanes].astype(f32) * gain
                ).astype(bf16)
            dt = w_dt_ref[layer, :, lanes_of(i, LANES)].astype(f32)
            dt = jnp.concatenate([dt, jnp.zeros((LANES - heads, LANES), f32)], axis=0)
            w_ref[to, mixed:] = (dt.T * gain).astype(bf16)

        each(0, members, block)

    spreader = spreader_of(heads, inner)
    line = iota((STRETCH, STRETCH), 0)
    lane = iota((STRETCH, STRETCH), 1)
    lower = line >= lane
    tri = jnp.where(lower, 1.0, 0.0).astype(bf16)
    left = iota((STRETCH, 2 * HEAD_DIM), 1) < HEAD_DIM

    def squares_of(v):
        wide = v.astype(f32)
        return jnp.sum(wide * wide, axis=-1, keepdims=True)

    def scale_of(v):
        return lax.rsqrt(squares_of(v) / depth + epsilon)

    def scan(layer, arrive):
        for t in range(members):
            halo_copy(layer, t, t).wait_recv()
        ahead = jnp.concatenate(
            [
                halo_ref[layer, t, :, j * COLUMNS : (j + 1) * COLUMNS]
                for j in range(pieces) for t in range(members)
            ],
            axis=1,
        )
        ahead = jnp.dot(ahead, w_ref[:, :mixed], preferred_element_type=f32) * scale_of(ahead)
        ahead = ahead[HALO - 8 :, :].astype(bf16).astype(f32)
        ext_ref[0:8, :] = jnp.where(seq > 0, ahead, 0.0)
        state_ref[...] = jnp.zeros_like(state_ref)
        sofar_ref[...] = jnp.zeros_like(sofar_ref)
        bias = pad_row(bias_ref[layer : layer + 1, :])
        rate = pad_row(jnp.exp(a_log_ref[layer : layer + 1, :]))
        skip = pad_row(d_skip_ref[layer : layer + 1, :])
        skip = expand(jnp.broadcast_to(skip, (8, LANES)), heads, spreader)[0:1]
        taps = jnp.concatenate([conv_x_ref[layer], conv_bc_ref[layer]], axis=1)
        tap_count = taps.shape[0]

        size = ROWS if layer else FINE
        parts = size // STRETCH

        def project(k):
            rows = rows_of(k, size)
            arrive(k)
            if layer == 0:
                tokens = jnp.concatenate([full_ref[j, rows, :] for j in range(pieces)], axis=1)
                scale = scale_of(tokens)
                projected = jnp.dot(tokens, w_ref[...], preferred_element_type=f32)
            else:
                tokens = full_ref[last_piece, rows, :]
                square = scale_ref[rows, 0:1] + squares_of(tokens)
                scale = lax.rsqrt(square / depth + epsilon)
                projected = acc_ref[rows, :] + jnp.dot(
                    tokens, w_ref[last_piece * width :, :], preferred_element_type=f32
                )
            scale_ref[rows, :] = jnp.broadcast_to(scale, (size, LANES))
            projected = projected * scale
            raw = projected[:, mixed:] + bias
            step = jnp.maximum(raw, 0.0) + jnp.log1p(jnp.exp(-jnp.abs(raw)))
            logs = pack_pieces(-step * rate, heads)
            sofar = sofar_ref[...]
            summed_logs = jnp.dot(
                tri,
                jnp.concatenate(
                    [logs[b * STRETCH : (b + 1) * STRETCH] for b in range(parts)], axis=1
                ),
                preferred_element_type=f32,
            )
            to_end, whole, earlier = [], [], []
            for b in range(parts):
                cum = unpack_sum(summed_logs[:, b * LANES : (b + 1) * LANES], heads)
                last = cum[STRETCH - 1 : STRETCH, :]
                cum_ref[rows_of(k * parts + b, STRETCH), :] = cum
                to_end.append(step[b * STRETCH : (b + 1) * STRETCH] * jnp.exp(last - cum))
                whole.append(jnp.exp(jnp.broadcast_to(last, (8, LANES))))
                earlier.append(jnp.exp(sofar))
                sofar = sofar + last
            sofar_ref[...] = sofar
            factors = expand(
                jnp.concatenate([step] + to_end + whole + earlier, axis=0), heads, spreader
            )
            ext_ref[8 : 8 + size, :] = projected[:, :mixed].astype(bf16).astype(f32)
            conv = jnp.zeros((size, mixed), f32)
            for tap in range(tap_count):
                first = 9 - tap_count + tap
                conv = conv + taps[tap : tap + 1, :] * ext_ref[first : first + size, :]
            conv = conv * jax.nn.sigmoid(conv)
            ext_ref[0:8, :] = ext_ref[size : size + 8, :]
            x = conv[:, :inner]
            b_all = conv[:, inner : inner + STATE]
            b_ref[rows, :] = b_all.astype(bf16)
            c_ref[rows, :] = conv[:, inner + STATE :].astype(bf16)
            feed_ref[rows, :] = (x * factors[:size]).astype(bf16)
            y_ref[rows, :] = skip * x
            ending = (x * factors[size : 2 * size]).astype(bf16)
            state = state_ref[...]
            for b in range(parts):
                part = slice(b * STRETCH, (b + 1) * STRETCH)
                index = k * parts + b
                fresh = jnp.dot(
                    b_all[part].T.astype(bf16), ending[part], preferred_element_type=f32
                )
                first = 2 * size + 8 * b
                states_ref[index] = state
                sofar_exp_ref[index] = factors[first + 8 * parts : first + 8 * parts + 8]
                state = state * factors[first : first + 1] + fresh
            state_ref[...] = state

        each(0, length // size, project)

    def within(k):
        rows = rows_of(k, ROWS)
        tokens = jnp.concatenate([full_ref[j, rows, :] for j in range(pieces)], axis=1)
        gate = jnp.dot(tokens, wz_ref[...], preferred_element_type=f32)
        z_ref[rows, :] = (gate * scale_ref[rows, 0:1]).astype(bf16)

        def block(b):
            rows = rows_of(k * per + b, STRETCH)
            cum = cum_ref[rows, :]
            cum_t = cum.T
            feed = feed_ref[rows, :]
            meet = lax.dot_general(
                c_ref[rows, :], b_ref[rows, :], (((1,), (1,)), ((), ())),
                preferred_element_type=f32,
            )
            for pair in range(heads // 2):
                lanes = slice(pair * 2 * HEAD_DIM, (pair + 1) * 2 * HEAD_DIM)
                weights = []
                for h in (2 * pair, 2 * pair + 1):
                    spread = jnp.where(lower, cum[:, h : h + 1] - cum_t[h : h + 1, :], -jnp.inf)
                    weights.append((meet * jnp.exp(spread)).astype(bf16))
                fed = feed[:, lanes]
                nought = jnp.zeros_like(fed)
                stacked = jnp.concatenate(
                    [jnp.where(left, fed, nought), jnp.where(left, nought, fed)], axis=0
                )
                inside = jnp.dot(
                    jnp.concatenate(weights, axis=1), stacked, preferred_element_type=f32
                )
                y_ref[rows, lanes] = y_ref[rows, lanes] + inside

        each(0, per, block)

    def exchange(layer):
        def end_copy(d):
            other = other_of(d)
            return remote(
                end_ref.at[layer, other], got_ref.at[layer, seq],
                end_send.at[layer], end_recv.at[layer], (other, own),
            )

        def log_copy(d):
            return remote(
                log_ref.at[layer], logs_ref.at[layer, seq],
                log_send.at[layer], log_recv.at[layer], (other_of(d), own),
            )

        def give_copy(d):
            other = other_of(d)
            return remote(
                give_ref.at[layer, other], arriving_ref.at[layer, seq],
                give_send.at[layer], give_recv.at[layer], (other, own),
            )

        others = pl.ds(0, count - 1)

        def all_of(ref, send, recv):
            block = ref.at[layer, others]
            return remote(block, block, send.at[layer], recv.at[layer], (following, own))

        all_ends = all_of(got_ref, end_send, end_recv)
        all_logs = all_of(logs_ref, log_send, log_recv)
        all_given = all_of(arriving_ref, give_send, give_recv)

        state = state_ref[...]
        for d in range(count):
            end_ref[layer, d] = state[d * state_rows : (d + 1) * state_rows].astype(bf16)
        log_ref[layer] = sofar_ref[...]

        def send(d):
            log_copy(d).start()
            end_copy(d).start()

        each(0, count - 1, send)
        each(0, chunks // 2, within)
        all_logs.wait_recv()
        all_ends.wait_recv()
        got_ref[layer, seq] = end_ref[layer, seq]
        logs_ref[layer, seq] = log_ref[layer]
        logs = jnp.concatenate([logs_ref[layer, d, 0:1] for d in range(count)], axis=0)
        factors = expand(jnp.exp(logs), heads, spreader)
        prefix = jnp.zeros((state_rows, inner), f32)
        for d in range(count):
            give_ref[layer, d] = prefix.astype(bf16)
            if d + 1 < count:
                prefix = prefix * factors[d : d + 1] + got_ref[layer, d].astype(f32)
        each(0, count - 1, lambda d: give_copy(d).start())
        each(chunks // 2, chunks, within)
        all_given.wait_recv()
        arriving_ref[layer, seq] = give_ref[layer, seq]
        prefix_ref[...] = jnp.concatenate(
            [arriving_ref[layer, d].astype(f32) for d in range(count)], axis=0
        )

        all_logs.wait_send()
        all_ends.wait_send()
        all_given.wait_send()

    pair = 2 * HEAD_DIM
    one = iota((2 * pair, pair), 0) % pair // HEAD_DIM
    two = iota((2 * pair, pair), 1) // HEAD_DIM
    averager = jnp.where(one == two, 1.0 / HEAD_DIM, 0.0).astype(bf16)

    def mixed_of(layer, k):
        rows = rows_of(k, ROWS)
        grown = expand(jnp.exp(cum_ref[rows, :]), heads, spreader)
        carried = []
        for block in range(per):
            index = k * per + block
            state = states_ref[index] + prefix_ref[...] * sofar_exp_ref[index][0:1]
            carried.append(
                jnp.dot(
                    c_ref[rows_of(index, STRETCH), :], state.astype(bf16),
                    preferred_element_type=f32,
                )
            )
        gate = z_ref[rows, :].astype(f32)
        ssd = y_ref[rows, :] + jnp.concatenate(carried, axis=0) * grown
        gated = ssd * (gate * jax.nn.sigmoid(gate))
        square = gated * gated
        high = square.astype(bf16)
        low = (square - high.astype(f32)).astype(bf16)
        results = []
        for p in range(inner // pair):
            lanes = slice(p * pair, (p + 1) * pair)
            both = jnp.concatenate([high[:, lanes], low[:, lanes]], axis=1)
            mean = jnp.dot(both, averager, preferred_element_type=f32)
            scaled = gated[:, lanes] * lax.rsqrt(mean + epsilon)
            results.append((scaled * out_gain_ref[layer : layer + 1, lanes]).astype(bf16))
        return jnp.concatenate(results, axis=1)

    def part_of(layer, i):
        if layer == 1:
            rows = rows_of(i, ROWS)
            blocks_of = [ref.at[rows] for ref in (sum_row_ref, far_row_ref)]
            nears = [near_row_ref.at[side, rows] for side in range(2)]
            return rows, lambda t: lanes_of(t, width), nears, blocks_of, i
        if isinstance(i, int):
            rows, j, slot = pl.ds(0, length), i, chunks + i - 1
        else:
            rows, j, slot = rows_of(i[0], ROWS), 0, i[0]
        blocks_of = [ref.at[j, rows] for ref in (sum_col_ref, far_col_ref)]
        nears = [near_col_ref.at[side, j, rows] for side in range(2)]
        return rows, lambda t: lanes_of(j * members + t, COLUMNS), nears, blocks_of, slot

    def near_part(layer, side, i):
        rows, lanes, nears, _, slot = part_of(layer, i)
        block = diagonal_id if side == 0 else near_id
        return remote(
            partial_ref.at[rows, lanes(block)], nears[side],
            near_send.at[layer, side], near_recv.at[layer, side, slot], sibling,
        )

    def far_part(layer, i):
        _, _, _, (summing, far), slot = part_of(layer, i)
        return remote(summing, far, far_send.at[layer], far_recv.at[layer, slot], across)

    def send_near(layer, i):
        near_part(layer, 0, i).start()
        near_part(layer, 1, i).start()

    def send_far(layer, i):
        rows, lanes, nears, (summing, _), _ = part_of(layer, i)
        near_part(layer, 0, i).wait_recv()
        summing[...] = (
            partial_ref[rows, lanes(across_id)].astype(f32) + nears[0][...].astype(f32)
        ).astype(bf16)
        far_part(layer, i).start()

    def summed(layer, i, stream):
        rows, lanes, nears, (_, far), _ = part_of(layer, i)
        near_part(layer, 1, i).wait_recv()
        far_part(layer, i).wait_recv()
        return (
            stream.astype(f32)
            + partial_ref[rows, lanes(own)].astype(f32)
            + nears[1][...].astype(f32)
            + far[...].astype(f32)
        ).astype(bf16)

    def drain_sums(layer):
        near_ref, sum_ref = ((near_col_ref, sum_col_ref), (near_row_ref, sum_row_ref))[layer]
        for side in range(2):
            block = near_ref.at[side]
            remote(
                block, block, near_send.at[layer, side], near_recv.at[layer, side, 0], sibling
            ).wait_send()
        remote(sum_ref, sum_ref, far_send.at[layer], far_recv.at[layer, 0], across).wait_send()

    def plan():
        shift = length.bit_length() - 1
        all_orders().wait_recv()
        orders_ref[seq] = order_ref[...]
        orders = jnp.concatenate([orders_ref[d] for d in range(count)], axis=0)

        def count_up(r):
            first = iota((LANES, length), 0) + r * LANES
            place_ref[rows_of(r, LANES), :] = jnp.where(
                first <= iota((LANES, length), 1), 1.0, 0.0
            ).astype(bf16)

        each(0, length // LANES, count_up)
        device = iota((count, length), 0)
        wanted_here = jnp.right_shift(orders, shift) == seq
        from_each = jnp.right_shift(order_ref[...], shift) == device
        ones = jnp.concatenate(
            [jnp.where(wanted_here, 1.0, 0.0), jnp.where(from_each, 1.0, 0.0)], axis=0
        ).astype(bf16)
        counted = jnp.dot(ones, place_ref[...], preferred_element_type=f32).astype(jnp.int32) - 1
        slot = jnp.where(wanted_here, counted[:count], -1)
        local = jnp.bitwise_and(orders, length - 1)
        short = iota((share, length), 0)
        long = iota((share, length), 1)
        for d in range(count):
            chosen = slot[d : d + 1, :] == short
            found = jnp.where(chosen, local[d : d + 1, :], 0).astype(f32)
            wanted = jnp.sum(found, axis=1, keepdims=True).astype(jnp.int32)
            hand_ref[d * share : (d + 1) * share, :] = jnp.where(
                wanted == long, 1.0, 0.0
            ).astype(bf16)
        target = jnp.where(from_each, counted[count:] + share * device, 0).astype(f32)
        target = jnp.sum(target, axis=0, keepdims=True)
        target = jnp.broadcast_to(target, (LANES, length)).T.astype(jnp.int32)
        for c in range(length // LANES):
            place_ref[:, c * LANES : (c + 1) * LANES] = jnp.where(
                target == iota((length, LANES), 1) + c * LANES, 1.0, 0.0
            ).astype(bf16)

    def move_copy(j, d):
        other = other_of(d)
        return remote(
            leaving_ref.at[j, rows_of(other, share)], arrived_ref.at[j, rows_of(seq, share)],
            move_send, move_recv.at[j], (other, own),
        )

    def all_moves(j):
        others = arrived_ref.at[j, pl.ds(0, length - share)]
        return remote(others, others, move_send, move_recv.at[j], (following, own))

    def hand_over(j):
        if j:
            held = summed(0, j, stream_ref[:, j * COLUMNS : (j + 1) * COLUMNS])
        else:

            def first(k):
                rows = rows_of(k, ROWS)
                held_ref[rows, :] = summed(0, (k,), stream_ref[rows, :COLUMNS])

            each(0, chunks, first)
            held = held_ref[...]
        leaving_ref[j] = jnp.dot(hand_ref[...], held, preferred_element_type=f32).astype(bf16)
        each(0, count - 1, lambda d: move_copy(j, d).start())
        arrived_ref[j, rows_of(seq, share), :] = leaving_ref[j, rows_of(seq, share), :]

    def put(j):
        lanes = slice(j * COLUMNS, (j + 1) * COLUMNS)
        all_moves(j).wait_recv()
        rows = jnp.dot(place_ref[...], arrived_ref[j], preferred_element_type=f32).astype(bf16)
        tail_ref[:, lanes] = rows[length - HALO :]
        full_ref[j, :, own_lanes] = rows
        for t in range(members):
            halo_piece(j, t).start()
        if j < last_piece:
            send_block(1, j)
        else:
            each(0, chunks, lambda k: send_block(1, (k,)))
        own_ref[:, lanes] = rows

    def accumulate(j):
        part = slice(j * width, (j + 1) * width)

        def product(k):
            rows = rows_of(k, ROWS)
            result = jnp.dot(
                full_ref[j, rows, :], w_ref[part, :], preferred_element_type=f32
            )
            acc_ref[rows, :] = result if j == 0 else acc_ref[rows, :] + result
            square = jnp.broadcast_to(squares_of(full_ref[j, rows, :]), (ROWS, LANES))
            scale_ref[rows, :] = square if j == 0 else scale_ref[rows, :] + square

        each(0, chunks, product)

    for copy in weight_loads(0):
        copy.wait()
    for j in range(pieces):
        prepare(0, j)
    for copy in weight_loads(1):
        copy.start()
    own_columns = full_ref.at[:, :, own_lanes]
    pltpu.make_async_copy(own_columns, own_columns, self_sem).wait()

    def arrive_first(k):
        forward_block(0, k)
        rest_of_block(0, k)

    scan(0, arrive_first)
    exchange(0)
    drain_gather(0)
    pltpu.make_async_copy(w_out_ref.at[0], wo_col_ref, wo_sem.at[0]).wait()
    pltpu.make_async_copy(w_out_ref.at[1], wo_ref, wo_sem.at[1]).wait()

    def product_of(k, j):
        rows, lanes = rows_of(k, ROWS), lanes_of(j, members * COLUMNS)
        partial_ref[rows, lanes] = jnp.dot(
            mixed_ref[rows, :], wo_col_ref[:, lanes], preferred_element_type=f32
        ).astype(bf16)

    def mix(k):
        mixed_ref[rows_of(k, ROWS), :] = mixed_of(0, k)
        product_of(k, 0)
        send_near(0, (k,))

        @pl.when(k > 0)
        def _():
            send_far(0, (k - 1,))

    each(0, chunks, mix)
    for j in range(1, pieces):
        each(0, chunks, lambda k: product_of(k, j))
        send_near(0, j)
        send_far(0, j - 1 if j > 1 else (chunks - 1,))
    send_far(0, pieces - 1)
    plan()
    for copy in weight_loads(1):
        copy.wait()

    for j in range(pieces):
        hand_over(j)
        if j:
            put(j - 1)
        prepare(1, j)
    put(pieces - 1)
    drain_sums(0)

    for j in range(last_piece):
        forward_block(1, j)
        rest_of_block(1, j)
        accumulate(j)
    forward_block(1, (0,))

    def arrive_second(k):
        @pl.when(k + 1 < chunks)
        def _():
            forward_block(1, (k + 1,))

        rest_of_block(1, (k,))

    scan(1, arrive_second)
    exchange(1)

    def output_rows(k):
        rows = rows_of(k, ROWS)
        mixed_heads = mixed_of(1, k)
        for side, block in enumerate((diagonal_id, near_id, across_id, own)):
            lanes = lanes_of(block, width)
            partial_ref[rows, lanes] = jnp.dot(
                mixed_heads, wo_ref[:, lanes], preferred_element_type=f32
            ).astype(bf16)
            if side < 2:
                near_part(1, side, k).start()
        send_far(1, k)

    each(0, chunks, output_rows)

    def out_copy(k):
        rows = rows_of(k, ROWS)
        return pltpu.make_async_copy(own_ref.at[rows], out_ref.at[rows], out_sem.at[k])

    def finish(k):
        rows = rows_of(k, ROWS)
        own_ref[rows, :] = summed(1, k, own_ref[rows, :])
        out_copy(k).start()

    each(0, chunks, finish)
    drain_gather(1)
    drain_sums(1)
    for layer in range(2):
        block = halo_ref.at[layer]
        remote(
            block, block, halo_send.at[layer], halo_recv.at[layer, 0], (following, own)
        ).wait_send()
    all_orders().wait_send()
    others = arrived_ref.at[:, pl.ds(0, length - share)]
    remote(others, others, move_send, move_recv.at[0], (following, own)).wait_send()
    each(0, chunks, lambda k: out_copy(k).wait())


def body(
    tokens, col_order, in_gain, w_in, w_bc, w_dt, conv_x, conv_bc,
    dt_bias, a_log, d_skip, out_gain, w_out,
):
    count, members = lax.axis_size("seq"), lax.axis_size("tp")
    length, width = tokens.shape
    inner = w_out.shape[1]
    heads = inner // HEAD_DIM
    mixed = inner + 2 * STATE
    depth = w_in.shape[1]
    chunks, fines = length // ROWS, length // FINE
    blocks = length // STRETCH
    pieces = width // COLUMNS
    state_rows = STATE // count
    vmem = pl.BlockSpec(memory_space=pltpu.VMEM)
    hbm = pl.BlockSpec(memory_space=pl.ANY)
    dma = pltpu.SemaphoreType.DMA
    return pl.pallas_call(
        functools.partial(layers_kernel, count, members),
        in_specs=[vmem, vmem, vmem, hbm, hbm] + [vmem] * 7 + [hbm],
        out_specs=hbm,
        out_shape=jax.ShapeDtypeStruct(tokens.shape, bf16),
        scratch_shapes=[
            pltpu.VMEM((pieces, length, members * COLUMNS), bf16),
            pltpu.VMEM((HALO, width), bf16),
            pltpu.VMEM((2, members, HALO, width), bf16),
            pltpu.VMEM((count, 1, length), jnp.int32),
            pltpu.VMEM((depth, 2, inner), bf16),
            pltpu.VMEM((depth, 2 * STATE), bf16),
            pltpu.VMEM((depth, mixed + LANES), bf16),
            pltpu.VMEM((depth, inner), bf16),
            pltpu.VMEM((inner, depth), bf16),
            pltpu.VMEM((inner, depth), bf16),
            pltpu.VMEM((ROWS + 8, mixed), f32),
            pltpu.VMEM((length, inner), f32),
            pltpu.VMEM((length, inner), bf16),
            pltpu.VMEM((length, inner), bf16),
            pltpu.VMEM((length, STATE), bf16),
            pltpu.VMEM((length, STATE), bf16),
            pltpu.VMEM((length, LANES), f32),
            pltpu.VMEM((length, LANES), f32),
            pltpu.VMEM((blocks, STATE, inner), f32),
            pltpu.VMEM((blocks, 8, inner), f32),
            pltpu.VMEM((STATE, inner), f32),
            pltpu.VMEM((8, LANES), f32),
            pltpu.VMEM((2, count, state_rows, inner), bf16),
            pltpu.VMEM((2, 8, LANES), f32),
            pltpu.VMEM((2, count, state_rows, inner), bf16),
            pltpu.VMEM((2, count, 8, LANES), f32),
            pltpu.VMEM((2, count, state_rows, inner), bf16),
            pltpu.VMEM((2, count, state_rows, inner), bf16),
            pltpu.VMEM((STATE, inner), f32),
            pltpu.VMEM((length, depth), bf16),
            pltpu.VMEM((2, pieces, length, COLUMNS), bf16),
            pltpu.VMEM((pieces, length, COLUMNS), bf16),
            pltpu.VMEM((pieces, length, COLUMNS), bf16),
            pltpu.VMEM((2, length, width), bf16),
            pltpu.VMEM((length, width), bf16),
            pltpu.VMEM((length, width), bf16),
            pltpu.VMEM((length, inner), bf16),
            pltpu.VMEM((length, length), bf16),
            pltpu.VMEM((length, length), bf16),
            pltpu.VMEM((pieces, length, COLUMNS), bf16),
            pltpu.VMEM((pieces, length, COLUMNS), bf16),
            pltpu.VMEM((length, COLUMNS), bf16),
            pltpu.VMEM((length, mixed + LANES), f32),
            pltpu.VMEM((length, width), bf16),
            dma((2, 2)), dma((2,)), dma,
            dma((2, 3)), dma((3, fines + chunks + pieces - 1)),
            dma((2,)), dma((2, members)), dma, dma,
            dma((2,)), dma((2,)), dma((2,)), dma((2,)), dma((2,)), dma((2,)),
            dma((2, 2)), dma((2, 2, chunks + pieces - 1)),
            dma((2,)), dma((2, chunks + pieces - 1)),
            dma, dma((pieces,)), dma((chunks,)),
        ],
        compiler_params=pltpu.CompilerParams(
            collective_id=0, has_side_effects=True, vmem_limit_bytes=63 * 1024 * 1024
        ),
        name="mixer_layers",
    )(
        tokens, col_order[None], in_gain, w_in, w_bc, jnp.swapaxes(w_dt, 1, 2), conv_x, conv_bc,
        dt_bias, a_log, d_skip, out_gain, w_out,
    )


def solution(mesh):
    placed = (
        P("seq", "tp"),
        P("seq"),
        P(),
        P(None, None, None, "tp"),
        P(),
        P(None, None, "tp"),
        P(None, None, "tp"),
        P(),
        P(None, "tp"),
        P(None, "tp"),
        P(None, "tp"),
        P(None, "tp"),
        P(None, "tp", None),
    )
    return jax.shard_map(
        body, mesh=mesh, in_specs=placed, out_specs=P("seq", "tp"), check_vma=False
    )
```

```python
import functools

import jax
import jax.numpy as jnp
from jax import lax
from jax.experimental import pallas as pl
from jax.experimental.pallas import tpu as pltpu
from jax.sharding import PartitionSpec as P

HEAD_DIM = 64
STATE = 128
STRETCH = 128
LANES = 128
HALO = 16
ROWS = 256
FINE = 128
COLUMNS = 128

epsilon = 1e-05
f32 = jnp.float32
bf16 = jnp.bfloat16
MESH = pl.DeviceIdType.MESH


def iota(shape, axis):
    return lax.broadcasted_iota(jnp.int32, shape, axis)


def spreader_of(heads, inner):
    row = iota((LANES, inner), 0)
    channel = iota((LANES, inner), 1)
    chosen = (row % heads == channel // HEAD_DIM) & (row < 3 * heads)
    return jnp.where(chosen, 1.0, 0.0).astype(bf16)


def pack_pieces(values, heads):
    values = jnp.where(iota(values.shape, 1) < heads, values, 0.0)
    high = values.astype(bf16).astype(f32)
    rest = values - high
    middle = rest.astype(bf16).astype(f32)
    low = rest - middle
    packed = high + pltpu.roll(middle, heads, 1) + pltpu.roll(low, 2 * heads, 1)
    return packed.astype(bf16)


def expand(values, heads, spreader):
    return jnp.dot(pack_pieces(values, heads), spreader, preferred_element_type=f32)


def unpack_sum(pieces, heads):
    total = (
        pieces
        + pltpu.roll(pieces, LANES - heads, 1)
        + pltpu.roll(pieces, LANES - 2 * heads, 1)
    )
    return jnp.where(iota(total.shape, 1) < heads, total, 0.0)


def rows_of(k, size):
    return pl.ds(pl.multiple_of(k * size, size), size)


def lanes_of(k, size):
    return pl.ds(pl.multiple_of(k * size, LANES), size)


def pad_row(row):
    return jnp.concatenate([row, jnp.zeros((1, LANES - row.shape[1]), f32)], axis=1)


def layers_kernel(
    count, members,
    stream_ref, order_ref, in_gain_ref, w_in_ref, w_bc_ref, w_dt_ref, conv_x_ref, conv_bc_ref,
    bias_ref, a_log_ref, d_skip_ref, out_gain_ref, w_out_ref,
    out_ref,
    full_ref, tail_ref, halo_ref, orders_ref, raw_ref, raw_bc_ref, w_ref, wz_ref, wo_col_ref, wo_ref,
    ext_ref, y_ref, z_ref, feed_ref, b_ref, c_ref, cum_ref, scale_ref, states_ref, sofar_exp_ref,
    state_ref, sofar_ref,
    end_ref, log_ref, got_ref, logs_ref, give_ref, arriving_ref, prefix_ref,
    partial_ref, near_col_ref, sum_col_ref, far_col_ref, near_row_ref, sum_row_ref, far_row_ref,
    mixed_ref, hand_ref, place_ref, leaving_ref, arrived_ref, held_ref, acc_ref, gate_ref, own_ref,
    load_sem, wo_sem, self_sem, ag_send, ag_recv, halo_send, halo_recv, order_send, order_recv,
    end_send, end_recv, log_send, log_recv, give_send, give_recv,
    near_send, near_recv, far_send, far_recv, move_send, move_recv, out_sem,
):
    seq = lax.axis_index("seq")
    own = lax.axis_index("tp")
    chip, core = own // 2, own % 2
    near_id = chip * 2 + 1 - core
    across_id = (1 - chip) * 2 + core
    diagonal_id = (1 - chip) * 2 + 1 - core
    sibling = (seq, near_id)
    across = (seq, across_id)
    length, width = stream_ref.shape
    depth = w_ref.shape[0]
    inner = y_ref.shape[1]
    mixed = inner + 2 * STATE
    heads = inner // HEAD_DIM
    chunks = length // ROWS
    fines = length // FINE
    per = ROWS // STRETCH
    blocks = length // STRETCH
    pieces = width // COLUMNS
    share = length // count
    state_rows = STATE // count
    following = (seq + 1) % count
    before = (seq + count - 1) % count

    def remote(src, dst, send, recv, device):
        return pltpu.make_async_remote_copy(
            src_ref=src, dst_ref=dst, send_sem=send, recv_sem=recv,
            device_id=device, device_id_type=MESH,
        )

    def other_of(i):
        low = seq < count // 2
        other = jnp.where(low, count - 1 - i, i)
        return jnp.where(low, other - (other <= seq), other + (other >= seq))

    def each(first, last, act):
        def step(i, _):
            act(i)
            return 0

        lax.fori_loop(first, last, step, 0)

    greeted = [sibling, across]
    greeted += [(before, t) for t in range(members)]
    greeted += [((seq + d) % count, own) for d in range(1, count)]
    barrier = pltpu.get_barrier_semaphore()
    for device in greeted:
        pl.semaphore_signal(barrier, inc=1, device_id=device, device_id_type=MESH)

    def weight_loads(layer):
        return [
            pltpu.make_async_copy(w_in_ref.at[layer], raw_ref, load_sem.at[layer, 0]),
            pltpu.make_async_copy(w_bc_ref.at[layer], raw_bc_ref, load_sem.at[layer, 1]),
        ]

    own_lanes = lanes_of(own, COLUMNS)
    self_loads, wo_loads = [], []
    for j in range(pieces):
        self_loads.append(
            pltpu.make_async_copy(
                stream_ref.at[:, j * COLUMNS : (j + 1) * COLUMNS],
                full_ref.at[j, :, own_lanes], self_sem,
            )
        )
        for t in range(members):
            first = t * width + j * COLUMNS
            place = j * members + t
            wo_loads.append(
                pltpu.make_async_copy(
                    w_out_ref.at[0, :, first : first + COLUMNS],
                    wo_col_ref.at[:, place * COLUMNS : (place + 1) * COLUMNS],
                    wo_sem.at[0],
                )
            )
    wo_loads.append(pltpu.make_async_copy(w_out_ref.at[1], wo_ref, wo_sem.at[1]))
    for copy in weight_loads(0) + self_loads + wo_loads:
        copy.start()

    pl.semaphore_wait(barrier, len(greeted))

    last_piece = pieces - 1
    late = pieces - 2

    def block_of(layer, i, owner):
        lanes = lanes_of(owner, COLUMNS)
        if layer == 0:
            return full_ref.at[:, rows_of(i, FINE), lanes], i
        if isinstance(i, int):
            return full_ref.at[i, :, lanes], fines + i
        return full_ref.at[last_piece, rows_of(i[0], ROWS), lanes], fines + last_piece + i[0]

    def gather_copy(layer, kind, i, owner):
        block, slot = block_of(layer, i, owner)
        return remote(
            block, block, ag_send.at[layer, kind], ag_recv.at[kind, slot],
            across if kind == 0 else sibling,
        )

    def send_rows(k):
        rows = rows_of(k, FINE)
        for kind, device in ((0, across), (1, sibling)):
            for j in range(pieces):
                remote(
                    stream_ref.at[rows, lanes_of(j, COLUMNS)], full_ref.at[j, rows, own_lanes],
                    ag_send.at[0, kind], ag_recv.at[kind, k], device,
                ).start()

    def send_block(layer, i):
        gather_copy(layer, 0, i, own).start()
        gather_copy(layer, 1, i, own).start()

    def forward_block(layer, i):
        gather_copy(layer, 0, i, across_id).wait_recv()
        gather_copy(layer, 2, i, across_id).start()

    def rest_of_block(layer, i):
        gather_copy(layer, 1, i, near_id).wait_recv()
        gather_copy(layer, 2, i, diagonal_id).wait_recv()

    def drain_gather(layer):
        for kind, owner in ((0, own), (1, own), (2, across_id)):
            block = full_ref.at[:, :, lanes_of(owner, COLUMNS)]
            remote(block, block, ag_send.at[layer, kind], ag_recv.at[kind, 0], sibling).wait_send()

    def halo_copy(layer, t, source):
        tail = tail_ref if layer else stream_ref.at[pl.ds(length - HALO, HALO)]
        return remote(
            tail, halo_ref.at[layer, source],
            halo_send.at[layer], halo_recv.at[layer, source], (following, t),
        )

    def halo_piece(j, t):
        lanes = lanes_of(j, COLUMNS)
        return remote(
            tail_ref.at[:, lanes], halo_ref.at[1, own, :, lanes],
            halo_send.at[1], halo_recv.at[1, own], (following, t),
        )

    def order_copy(d):
        return remote(
            order_ref, orders_ref.at[seq], order_send, order_recv, (other_of(d), own)
        )

    def all_orders():
        others = orders_ref.at[pl.ds(0, count - 1)]
        return remote(others, others, order_send, order_recv, (following, own))

    for t in range(members):
        halo_copy(0, t, own).start()

    each(0, fines, send_rows)
    each(0, count - 1, lambda d: order_copy(d).start())

    row = iota((2 * LANES, 2 * LANES), 0)
    col = iota((2 * LANES, 2 * LANES), 1)
    apart = jnp.where(col == 2 * (row % LANES) + row // LANES, 1.0, 0.0).astype(bf16)

    def prepare(layer, j):
        def block(t):
            i = t * pieces + j
            rows = rows_of(i, LANES)
            to = rows_of(j * members + t, LANES)
            gain = in_gain_ref[layer : layer + 1, lanes_of(i, LANES)]
            gain = jnp.broadcast_to(gain, (LANES, LANES)).T
            both = raw_ref[rows].reshape(2 * LANES, inner)
            halves = jnp.dot(apart, both, preferred_element_type=f32)
            for p in range(inner // LANES):
                lanes = slice(p * LANES, (p + 1) * LANES)
                w_ref[to, lanes] = (halves[:LANES, lanes] * gain).astype(bf16)
                wz_ref[to, lanes] = (halves[LANES:, lanes] * gain).astype(bf16)
            for p in range(2 * STATE // LANES):
                lanes = slice(p * LANES, (p + 1) * LANES)
                w_ref[to, inner + p * LANES : inner + (p + 1) * LANES] = (
                    raw_bc_ref[rows, lanes].astype(f32) * gain
                ).astype(bf16)
            dt = w_dt_ref[layer, :, lanes_of(i, LANES)].astype(f32)
            dt = jnp.concatenate([dt, jnp.zeros((LANES - heads, LANES), f32)], axis=0)
            w_ref[to, mixed:] = (dt.T * gain).astype(bf16)

        each(0, members, block)

    spreader = spreader_of(heads, inner)
    line = iota((STRETCH, STRETCH), 0)
    lane = iota((STRETCH, STRETCH), 1)
    lower = line >= lane
    tri = jnp.where(lower, 1.0, 0.0).astype(bf16)
    left = iota((STRETCH, 2 * HEAD_DIM), 1) < HEAD_DIM

    def late_tokens(rows):
        return jnp.concatenate([full_ref[j, rows, :] for j in range(late, pieces)], axis=1)

    def squares_of(v):
        wide = v.astype(f32)
        return jnp.sum(wide * wide, axis=-1, keepdims=True)

    def scale_of(v):
        return lax.rsqrt(squares_of(v) / depth + epsilon)

    def scan(layer, arrive):
        for t in range(members):
            halo_copy(layer, t, t).wait_recv()
        ahead = jnp.concatenate(
            [
                halo_ref[layer, t, :, j * COLUMNS : (j + 1) * COLUMNS]
                for j in range(pieces) for t in range(members)
            ],
            axis=1,
        )
        ahead = jnp.dot(ahead, w_ref[:, :mixed], preferred_element_type=f32) * scale_of(ahead)
        ahead = ahead[HALO - 8 :, :].astype(bf16).astype(f32)
        ext_ref[0:8, :] = jnp.where(seq > 0, ahead, 0.0)
        state_ref[...] = jnp.zeros_like(state_ref)
        sofar_ref[...] = jnp.zeros_like(sofar_ref)
        bias = pad_row(bias_ref[layer : layer + 1, :])
        rate = pad_row(jnp.exp(a_log_ref[layer : layer + 1, :]))
        skip = pad_row(d_skip_ref[layer : layer + 1, :])
        skip = expand(jnp.broadcast_to(skip, (8, LANES)), heads, spreader)[0:1]
        taps = jnp.concatenate([conv_x_ref[layer], conv_bc_ref[layer]], axis=1)
        tap_count = taps.shape[0]

        size = ROWS if layer else FINE
        parts = size // STRETCH

        def project(k):
            rows = rows_of(k, size)
            arrive(k)
            if layer == 0:
                tokens = jnp.concatenate([full_ref[j, rows, :] for j in range(pieces)], axis=1)
                scale = scale_of(tokens)
                projected = jnp.dot(tokens, w_ref[...], preferred_element_type=f32)
                gate = jnp.dot(tokens, wz_ref[...], preferred_element_type=f32)
                z_ref[rows, :] = (gate * scale).astype(bf16)
            else:
                tokens = late_tokens(rows)
                square = scale_ref[rows, 0:1] + squares_of(tokens)
                scale = lax.rsqrt(square / depth + epsilon)
                projected = acc_ref[rows, :] + jnp.dot(
                    tokens, w_ref[late * width :, :], preferred_element_type=f32
                )
                scale_ref[rows, :] = jnp.broadcast_to(scale, (size, LANES))
            projected = projected * scale
            raw = projected[:, mixed:] + bias
            step = jnp.maximum(raw, 0.0) + jnp.log1p(jnp.exp(-jnp.abs(raw)))
            logs = pack_pieces(-step * rate, heads)
            sofar = sofar_ref[...]
            summed_logs = jnp.dot(
                tri,
                jnp.concatenate(
                    [logs[b * STRETCH : (b + 1) * STRETCH] for b in range(parts)], axis=1
                ),
                preferred_element_type=f32,
            )
            to_end, whole, earlier = [], [], []
            for b in range(parts):
                cum = unpack_sum(summed_logs[:, b * LANES : (b + 1) * LANES], heads)
                last = cum[STRETCH - 1 : STRETCH, :]
                cum_ref[rows_of(k * parts + b, STRETCH), :] = cum
                to_end.append(step[b * STRETCH : (b + 1) * STRETCH] * jnp.exp(last - cum))
                whole.append(jnp.exp(jnp.broadcast_to(last, (8, LANES))))
                earlier.append(jnp.exp(sofar))
                sofar = sofar + last
            sofar_ref[...] = sofar
            factors = expand(
                jnp.concatenate([step] + to_end + whole + earlier, axis=0), heads, spreader
            )
            ext_ref[8 : 8 + size, :] = projected[:, :mixed].astype(bf16).astype(f32)
            conv = jnp.zeros((size, mixed), f32)
            for tap in range(tap_count):
                first = 9 - tap_count + tap
                conv = conv + taps[tap : tap + 1, :] * ext_ref[first : first + size, :]
            conv = conv * jax.nn.sigmoid(conv)
            ext_ref[0:8, :] = ext_ref[size : size + 8, :]
            x = conv[:, :inner]
            b_all = conv[:, inner : inner + STATE]
            b_ref[rows, :] = b_all.astype(bf16)
            c_ref[rows, :] = conv[:, inner + STATE :].astype(bf16)
            feed_ref[rows, :] = (x * factors[:size]).astype(bf16)
            y_ref[rows, :] = skip * x
            ending = (x * factors[size : 2 * size]).astype(bf16)
            state = state_ref[...]
            for b in range(parts):
                part = slice(b * STRETCH, (b + 1) * STRETCH)
                index = k * parts + b
                fresh = jnp.dot(
                    b_all[part].T.astype(bf16), ending[part], preferred_element_type=f32
                )
                first = 2 * size + 8 * b
                states_ref[index] = state
                sofar_exp_ref[index] = factors[first + 8 * parts : first + 8 * parts + 8]
                state = state * factors[first : first + 1] + fresh
            state_ref[...] = state

        each(0, length // size, project)

    def within(layer, k):
        if layer:
            rows = rows_of(k, ROWS)
            gate = gate_ref[rows, :] + jnp.dot(
                late_tokens(rows), wz_ref[late * width :, :], preferred_element_type=f32
            )
            z_ref[rows, :] = (gate * scale_ref[rows, 0:1]).astype(bf16)

        def block(b):
            rows = rows_of(k * per + b, STRETCH)
            cum = cum_ref[rows, :]
            cum_t = cum.T
            feed = feed_ref[rows, :]
            meet = lax.dot_general(
                c_ref[rows, :], b_ref[rows, :], (((1,), (1,)), ((), ())),
                preferred_element_type=f32,
            )
            for pair in range(heads // 2):
                lanes = slice(pair * 2 * HEAD_DIM, (pair + 1) * 2 * HEAD_DIM)
                weights = []
                for h in (2 * pair, 2 * pair + 1):
                    spread = jnp.where(lower, cum[:, h : h + 1] - cum_t[h : h + 1, :], -jnp.inf)
                    weights.append((meet * jnp.exp(spread)).astype(bf16))
                fed = feed[:, lanes]
                nought = jnp.zeros_like(fed)
                stacked = jnp.concatenate(
                    [jnp.where(left, fed, nought), jnp.where(left, nought, fed)], axis=0
                )
                inside = jnp.dot(
                    jnp.concatenate(weights, axis=1), stacked, preferred_element_type=f32
                )
                y_ref[rows, lanes] = y_ref[rows, lanes] + inside

        each(0, per, block)

    def exchange(layer):
        def end_copy(d):
            other = other_of(d)
            return remote(
                end_ref.at[layer, other], got_ref.at[layer, seq],
                end_send.at[layer], end_recv.at[layer], (other, own),
            )

        def log_copy(d):
            return remote(
                log_ref.at[layer], logs_ref.at[layer, seq],
                log_send.at[layer], log_recv.at[layer], (other_of(d), own),
            )

        def give_copy(d):
            other = other_of(d)
            return remote(
                give_ref.at[layer, other], arriving_ref.at[layer, seq],
                give_send.at[layer], give_recv.at[layer], (other, own),
            )

        others = pl.ds(0, count - 1)

        def all_of(ref, send, recv):
            block = ref.at[layer, others]
            return remote(block, block, send.at[layer], recv.at[layer], (following, own))

        all_ends = all_of(got_ref, end_send, end_recv)
        all_logs = all_of(logs_ref, log_send, log_recv)
        all_given = all_of(arriving_ref, give_send, give_recv)

        state = state_ref[...]
        for d in range(count):
            end_ref[layer, d] = state[d * state_rows : (d + 1) * state_rows].astype(bf16)
        log_ref[layer] = sofar_ref[...]

        def send(d):
            log_copy(d).start()
            end_copy(d).start()

        each(0, count - 1, send)
        each(0, chunks // 2, lambda k: within(layer, k))
        all_logs.wait_recv()
        all_ends.wait_recv()
        got_ref[layer, seq] = end_ref[layer, seq]
        logs_ref[layer, seq] = log_ref[layer]
        logs = jnp.concatenate([logs_ref[layer, d, 0:1] for d in range(count)], axis=0)
        factors = expand(jnp.exp(logs), heads, spreader)
        prefix = jnp.zeros((state_rows, inner), f32)
        for d in range(count):
            give_ref[layer, d] = prefix.astype(bf16)
            if d + 1 < count:
                prefix = prefix * factors[d : d + 1] + got_ref[layer, d].astype(f32)
        each(0, count - 1, lambda d: give_copy(d).start())
        each(chunks // 2, chunks, lambda k: within(layer, k))
        all_given.wait_recv()
        arriving_ref[layer, seq] = give_ref[layer, seq]
        prefix_ref[...] = jnp.concatenate(
            [arriving_ref[layer, d].astype(f32) for d in range(count)], axis=0
        )

        all_logs.wait_send()
        all_ends.wait_send()
        all_given.wait_send()

    pair = 2 * HEAD_DIM
    one = iota((2 * pair, pair), 0) % pair // HEAD_DIM
    two = iota((2 * pair, pair), 1) // HEAD_DIM
    averager = jnp.where(one == two, 1.0 / HEAD_DIM, 0.0).astype(bf16)

    def mixed_of(layer, k):
        rows = rows_of(k, ROWS)
        grown = expand(jnp.exp(cum_ref[rows, :]), heads, spreader)
        carried = []
        for block in range(per):
            index = k * per + block
            state = states_ref[index] + prefix_ref[...] * sofar_exp_ref[index][0:1]
            carried.append(
                jnp.dot(
                    c_ref[rows_of(index, STRETCH), :], state.astype(bf16),
                    preferred_element_type=f32,
                )
            )
        gate = z_ref[rows, :].astype(f32)
        ssd = y_ref[rows, :] + jnp.concatenate(carried, axis=0) * grown
        gated = ssd * (gate * jax.nn.sigmoid(gate))
        square = gated * gated
        high = square.astype(bf16)
        low = (square - high.astype(f32)).astype(bf16)
        results = []
        for p in range(inner // pair):
            lanes = slice(p * pair, (p + 1) * pair)
            both = jnp.concatenate([high[:, lanes], low[:, lanes]], axis=1)
            mean = jnp.dot(both, averager, preferred_element_type=f32)
            scaled = gated[:, lanes] * lax.rsqrt(mean + epsilon)
            results.append((scaled * out_gain_ref[layer : layer + 1, lanes]).astype(bf16))
        return jnp.concatenate(results, axis=1)

    def part_of(layer, i):
        if layer == 1:
            rows = rows_of(i, ROWS)
            blocks_of = [ref.at[rows] for ref in (sum_row_ref, far_row_ref)]
            nears = [near_row_ref.at[side, rows] for side in range(2)]
            return rows, lambda t: lanes_of(t, width), nears, blocks_of, i
        if isinstance(i, int):
            rows, j, slot = pl.ds(0, length), i, chunks + i - 1
        else:
            rows, j, slot = rows_of(i[0], ROWS), 0, i[0]
        blocks_of = [ref.at[j, rows] for ref in (sum_col_ref, far_col_ref)]
        nears = [near_col_ref.at[side, j, rows] for side in range(2)]
        return rows, lambda t: lanes_of(j * members + t, COLUMNS), nears, blocks_of, slot

    def near_part(layer, side, i):
        rows, lanes, nears, _, slot = part_of(layer, i)
        block = diagonal_id if side == 0 else near_id
        return remote(
            partial_ref.at[rows, lanes(block)], nears[side],
            near_send.at[layer, side], near_recv.at[layer, side, slot], sibling,
        )

    def far_part(layer, i):
        _, _, _, (summing, far), slot = part_of(layer, i)
        return remote(summing, far, far_send.at[layer], far_recv.at[layer, slot], across)

    def send_near(layer, i):
        near_part(layer, 0, i).start()
        near_part(layer, 1, i).start()

    def send_far(layer, i):
        rows, lanes, nears, (summing, _), _ = part_of(layer, i)
        near_part(layer, 0, i).wait_recv()
        summing[...] = (
            partial_ref[rows, lanes(across_id)].astype(f32) + nears[0][...].astype(f32)
        ).astype(bf16)
        far_part(layer, i).start()

    def summed(layer, i, stream):
        rows, lanes, nears, (_, far), _ = part_of(layer, i)
        near_part(layer, 1, i).wait_recv()
        far_part(layer, i).wait_recv()
        return (
            stream.astype(f32)
            + partial_ref[rows, lanes(own)].astype(f32)
            + nears[1][...].astype(f32)
            + far[...].astype(f32)
        ).astype(bf16)

    def drain_sums(layer):
        near_ref, sum_ref = ((near_col_ref, sum_col_ref), (near_row_ref, sum_row_ref))[layer]
        for side in range(2):
            block = near_ref.at[side]
            remote(
                block, block, near_send.at[layer, side], near_recv.at[layer, side, 0], sibling
            ).wait_send()
        remote(sum_ref, sum_ref, far_send.at[layer], far_recv.at[layer, 0], across).wait_send()

    def plan():
        shift = length.bit_length() - 1
        all_orders().wait_recv()
        orders_ref[seq] = order_ref[...]
        orders = jnp.concatenate([orders_ref[d] for d in range(count)], axis=0)

        def count_up(r):
            first = iota((LANES, length), 0) + r * LANES
            place_ref[rows_of(r, LANES), :] = jnp.where(
                first <= iota((LANES, length), 1), 1.0, 0.0
            ).astype(bf16)

        each(0, length // LANES, count_up)
        device = iota((count, length), 0)
        wanted_here = jnp.right_shift(orders, shift) == seq
        from_each = jnp.right_shift(order_ref[...], shift) == device
        ones = jnp.concatenate(
            [jnp.where(wanted_here, 1.0, 0.0), jnp.where(from_each, 1.0, 0.0)], axis=0
        ).astype(bf16)
        counted = jnp.dot(ones, place_ref[...], preferred_element_type=f32).astype(jnp.int32) - 1
        slot = jnp.where(wanted_here, counted[:count], -1)
        local = jnp.bitwise_and(orders, length - 1)
        short = iota((share, length), 0)
        long = iota((share, length), 1)
        for d in range(count):
            chosen = slot[d : d + 1, :] == short
            found = jnp.where(chosen, local[d : d + 1, :], 0).astype(f32)
            wanted = jnp.sum(found, axis=1, keepdims=True).astype(jnp.int32)
            hand_ref[d * share : (d + 1) * share, :] = jnp.where(
                wanted == long, 1.0, 0.0
            ).astype(bf16)
        target = jnp.where(from_each, counted[count:] + share * device, 0).astype(f32)
        target = jnp.sum(target, axis=0, keepdims=True)
        target = jnp.broadcast_to(target, (LANES, length)).T.astype(jnp.int32)
        for c in range(length // LANES):
            place_ref[:, c * LANES : (c + 1) * LANES] = jnp.where(
                target == iota((length, LANES), 1) + c * LANES, 1.0, 0.0
            ).astype(bf16)

    def move_copy(j, d):
        other = other_of(d)
        return remote(
            leaving_ref.at[j, rows_of(other, share)], arrived_ref.at[j, rows_of(seq, share)],
            move_send, move_recv.at[j], (other, own),
        )

    def all_moves(j):
        others = arrived_ref.at[j, pl.ds(0, length - share)]
        return remote(others, others, move_send, move_recv.at[j], (following, own))

    def hand_over(j):
        if j:
            held = summed(0, j, full_ref[j, :, own_lanes])
        else:

            def first(k):
                rows = rows_of(k, ROWS)
                held_ref[rows, :] = summed(0, (k,), full_ref[0, rows, own_lanes])

            each(0, chunks, first)
            held = held_ref[...]
        leaving_ref[j] = jnp.dot(hand_ref[...], held, preferred_element_type=f32).astype(bf16)
        each(0, count - 1, lambda d: move_copy(j, d).start())
        arrived_ref[j, rows_of(seq, share), :] = leaving_ref[j, rows_of(seq, share), :]

    def put(j):
        lanes = slice(j * COLUMNS, (j + 1) * COLUMNS)
        all_moves(j).wait_recv()
        rows = jnp.dot(place_ref[...], arrived_ref[j], preferred_element_type=f32).astype(bf16)
        tail_ref[:, lanes] = rows[length - HALO :]
        full_ref[j, :, own_lanes] = rows
        for t in range(members):
            halo_piece(j, t).start()
        if j < last_piece:
            send_block(1, j)
        else:
            each(0, chunks, lambda k: send_block(1, (k,)))
        own_ref[:, lanes] = rows

    def accumulate(j):
        part = slice(j * width, (j + 1) * width)

        def product(k):
            rows = rows_of(k, ROWS)
            result = jnp.dot(
                full_ref[j, rows, :], w_ref[part, :], preferred_element_type=f32
            )
            acc_ref[rows, :] = result if j == 0 else acc_ref[rows, :] + result
            gate = jnp.dot(full_ref[j, rows, :], wz_ref[part, :], preferred_element_type=f32)
            gate_ref[rows, :] = gate if j == 0 else gate_ref[rows, :] + gate
            square = jnp.broadcast_to(squares_of(full_ref[j, rows, :]), (ROWS, LANES))
            scale_ref[rows, :] = square if j == 0 else scale_ref[rows, :] + square

        each(0, chunks, product)

    for copy in weight_loads(0):
        copy.wait()
    for j in range(pieces):
        prepare(0, j)
    for copy in weight_loads(1):
        copy.start()
    own_columns = full_ref.at[:, :, own_lanes]
    pltpu.make_async_copy(own_columns, own_columns, self_sem).wait()

    def arrive_first(k):
        forward_block(0, k)
        rest_of_block(0, k)

    scan(0, arrive_first)
    exchange(0)
    drain_gather(0)
    pltpu.make_async_copy(w_out_ref.at[0], wo_col_ref, wo_sem.at[0]).wait()
    pltpu.make_async_copy(w_out_ref.at[1], wo_ref, wo_sem.at[1]).wait()

    def product_of(k, j):
        rows, lanes = rows_of(k, ROWS), lanes_of(j, members * COLUMNS)
        partial_ref[rows, lanes] = jnp.dot(
            mixed_ref[rows, :], wo_col_ref[:, lanes], preferred_element_type=f32
        ).astype(bf16)

    def mix(k):
        mixed_ref[rows_of(k, ROWS), :] = mixed_of(0, k)
        product_of(k, 0)
        send_near(0, (k,))

        @pl.when(k > 0)
        def _():
            send_far(0, (k - 1,))

    each(0, chunks, mix)
    for j in range(1, pieces):
        each(0, chunks, lambda k: product_of(k, j))
        send_near(0, j)
        send_far(0, j - 1 if j > 1 else (chunks - 1,))
    send_far(0, pieces - 1)
    plan()
    for copy in weight_loads(1):
        copy.wait()

    for j in range(pieces):
        hand_over(j)
        if j > 1:
            put(j - 2)
        prepare(1, j)
    put(pieces - 2)
    forward_block(1, 0)
    rest_of_block(1, 0)
    accumulate(0)
    put(pieces - 1)
    drain_sums(0)

    for j in range(1, last_piece):
        forward_block(1, j)
        if j == last_piece - 1:
            forward_block(1, (0,))
        rest_of_block(1, j)
        if j < late:
            accumulate(j)

    def arrive_second(k):
        @pl.when(k + 1 < chunks)
        def _():
            forward_block(1, (k + 1,))

        rest_of_block(1, (k,))

    scan(1, arrive_second)
    exchange(1)

    def output_rows(k):
        rows = rows_of(k, ROWS)
        mixed_heads = mixed_of(1, k)
        for side, block in enumerate((diagonal_id, near_id, across_id, own)):
            lanes = lanes_of(block, width)
            partial_ref[rows, lanes] = jnp.dot(
                mixed_heads, wo_ref[:, lanes], preferred_element_type=f32
            ).astype(bf16)
            if side < 2:
                near_part(1, side, k).start()
        send_far(1, k)

    each(0, chunks, output_rows)

    def out_copy(k):
        rows = rows_of(k, ROWS)
        return pltpu.make_async_copy(own_ref.at[rows], out_ref.at[rows], out_sem.at[k])

    def finish(k):
        rows = rows_of(k, ROWS)
        own_ref[rows, :] = summed(1, k, own_ref[rows, :])
        out_copy(k).start()

    each(0, chunks, finish)
    drain_gather(1)
    drain_sums(1)
    for layer in range(2):
        block = halo_ref.at[layer]
        remote(
            block, block, halo_send.at[layer], halo_recv.at[layer, 0], (following, own)
        ).wait_send()
    all_orders().wait_send()
    others = arrived_ref.at[:, pl.ds(0, length - share)]
    remote(others, others, move_send, move_recv.at[0], (following, own)).wait_send()
    each(0, chunks, lambda k: out_copy(k).wait())


def body(
    tokens, col_order, in_gain, w_in, w_bc, w_dt, conv_x, conv_bc,
    dt_bias, a_log, d_skip, out_gain, w_out,
):
    count, members = lax.axis_size("seq"), lax.axis_size("tp")
    length, width = tokens.shape
    inner = w_out.shape[1]
    heads = inner // HEAD_DIM
    mixed = inner + 2 * STATE
    depth = w_in.shape[1]
    chunks, fines = length // ROWS, length // FINE
    blocks = length // STRETCH
    pieces = width // COLUMNS
    state_rows = STATE // count
    vmem = pl.BlockSpec(memory_space=pltpu.VMEM)
    hbm = pl.BlockSpec(memory_space=pl.ANY)
    dma = pltpu.SemaphoreType.DMA
    return pl.pallas_call(
        functools.partial(layers_kernel, count, members),
        in_specs=[hbm, vmem, vmem, hbm, hbm] + [vmem] * 7 + [hbm],
        out_specs=hbm,
        out_shape=jax.ShapeDtypeStruct(tokens.shape, bf16),
        scratch_shapes=[
            pltpu.VMEM((pieces, length, members * COLUMNS), bf16),
            pltpu.VMEM((HALO, width), bf16),
            pltpu.VMEM((2, members, HALO, width), bf16),
            pltpu.VMEM((count, 1, length), jnp.int32),
            pltpu.VMEM((depth, 2, inner), bf16),
            pltpu.VMEM((depth, 2 * STATE), bf16),
            pltpu.VMEM((depth, mixed + LANES), bf16),
            pltpu.VMEM((depth, inner), bf16),
            pltpu.VMEM((inner, depth), bf16),
            pltpu.VMEM((inner, depth), bf16),
            pltpu.VMEM((ROWS + 8, mixed), f32),
            pltpu.VMEM((length, inner), f32),
            pltpu.VMEM((length, inner), bf16),
            pltpu.VMEM((length, inner), bf16),
            pltpu.VMEM((length, STATE), bf16),
            pltpu.VMEM((length, STATE), bf16),
            pltpu.VMEM((length, LANES), f32),
            pltpu.VMEM((length, LANES), f32),
            pltpu.VMEM((blocks, STATE, inner), f32),
            pltpu.VMEM((blocks, 8, inner), f32),
            pltpu.VMEM((STATE, inner), f32),
            pltpu.VMEM((8, LANES), f32),
            pltpu.VMEM((2, count, state_rows, inner), bf16),
            pltpu.VMEM((2, 8, LANES), f32),
            pltpu.VMEM((2, count, state_rows, inner), bf16),
            pltpu.VMEM((2, count, 8, LANES), f32),
            pltpu.VMEM((2, count, state_rows, inner), bf16),
            pltpu.VMEM((2, count, state_rows, inner), bf16),
            pltpu.VMEM((STATE, inner), f32),
            pltpu.VMEM((length, depth), bf16),
            pltpu.VMEM((2, pieces, length, COLUMNS), bf16),
            pltpu.VMEM((pieces, length, COLUMNS), bf16),
            pltpu.VMEM((pieces, length, COLUMNS), bf16),
            pltpu.VMEM((2, length, width), bf16),
            pltpu.VMEM((length, width), bf16),
            pltpu.VMEM((length, width), bf16),
            pltpu.VMEM((length, inner), bf16),
            pltpu.VMEM((length, length), bf16),
            pltpu.VMEM((length, length), bf16),
            pltpu.VMEM((pieces, length, COLUMNS), bf16),
            pltpu.VMEM((pieces, length, COLUMNS), bf16),
            pltpu.VMEM((length, COLUMNS), bf16),
            pltpu.VMEM((length, mixed + LANES), f32),
            pltpu.VMEM((length, inner), f32),
            pltpu.VMEM((length, width), bf16),
            dma((2, 2)), dma((2,)), dma,
            dma((2, 3)), dma((3, fines + chunks + pieces - 1)),
            dma((2,)), dma((2, members)), dma, dma,
            dma((2,)), dma((2,)), dma((2,)), dma((2,)), dma((2,)), dma((2,)),
            dma((2, 2)), dma((2, 2, chunks + pieces - 1)),
            dma((2,)), dma((2, chunks + pieces - 1)),
            dma, dma((pieces,)), dma((chunks,)),
        ],
        compiler_params=pltpu.CompilerParams(
            collective_id=0, has_side_effects=True, vmem_limit_bytes=63 * 1024 * 1024
        ),
        name="mixer_layers",
    )(
        tokens, col_order[None], in_gain, w_in, w_bc, jnp.swapaxes(w_dt, 1, 2), conv_x, conv_bc,
        dt_bias, a_log, d_skip, out_gain, w_out,
    )


def solution(mesh):
    placed = (
        P("seq", "tp"),
        P("seq"),
        P(),
        P(None, None, None, "tp"),
        P(),
        P(None, None, "tp"),
        P(None, None, "tp"),
        P(),
        P(None, "tp"),
        P(None, "tp"),
        P(None, "tp"),
        P(None, "tp"),
        P(None, "tp", None),
    )
    return jax.shard_map(
        body, mesh=mesh, in_specs=placed, out_specs=P("seq", "tp"), check_vma=False
    )
```

```python
import functools

import jax
import jax.numpy as jnp
from jax import lax
from jax.experimental import pallas as pl
from jax.experimental.pallas import tpu as pltpu
from jax.sharding import PartitionSpec as P

HEAD_DIM = 64
STATE = 128
STRETCH = 128
LANES = 128
HALO = 16
ROWS = 256
FINE = 128
COLUMNS = 128

epsilon = 1e-05
f32 = jnp.float32
bf16 = jnp.bfloat16
MESH = pl.DeviceIdType.MESH


def iota(shape, axis):
    return lax.broadcasted_iota(jnp.int32, shape, axis)


def spreader_of(heads, inner):
    row = iota((LANES, inner), 0)
    channel = iota((LANES, inner), 1)
    chosen = (row % heads == channel // HEAD_DIM) & (row < 3 * heads)
    return jnp.where(chosen, 1.0, 0.0).astype(bf16)


def pack_pieces(values, heads):
    values = jnp.where(iota(values.shape, 1) < heads, values, 0.0)
    high = values.astype(bf16).astype(f32)
    rest = values - high
    middle = rest.astype(bf16).astype(f32)
    low = rest - middle
    packed = high + pltpu.roll(middle, heads, 1) + pltpu.roll(low, 2 * heads, 1)
    return packed.astype(bf16)


def expand(values, heads, spreader):
    return jnp.dot(pack_pieces(values, heads), spreader, preferred_element_type=f32)


def unpack_sum(pieces, heads):
    total = (
        pieces
        + pltpu.roll(pieces, LANES - heads, 1)
        + pltpu.roll(pieces, LANES - 2 * heads, 1)
    )
    return jnp.where(iota(total.shape, 1) < heads, total, 0.0)


def rows_of(k, size):
    return pl.ds(pl.multiple_of(k * size, size), size)


def lanes_of(k, size):
    return pl.ds(pl.multiple_of(k * size, LANES), size)


def pad_row(row):
    return jnp.concatenate([row, jnp.zeros((1, LANES - row.shape[1]), f32)], axis=1)


def layers_kernel(
    count, members,
    stream_ref, order_ref, in_gain_ref, w_in_ref, w_bc_ref, w_dt_ref, conv_x_ref, conv_bc_ref,
    bias_ref, a_log_ref, d_skip_ref, out_gain_ref, w_out_ref,
    out_ref,
    full_ref, tail_ref, halo_ref, orders_ref, raw_ref, raw_bc_ref, w_ref, wz_ref, wo_col_ref, wo_ref,
    ext_ref, y_ref, z_ref, feed_ref, b_ref, c_ref, cum_ref, scale_ref, states_ref, sofar_exp_ref,
    state_ref, sofar_ref,
    end_ref, log_ref, got_ref, logs_ref, give_ref, arriving_ref, prefix_ref,
    partial_ref, near_ref, sum_ref, far_ref,
    mixed_ref, hand_ref, place_ref, leaving_ref, arrived_ref, held_ref, acc_ref, gate_ref, own_ref,
    load_sem, wo_sem, self_sem, ag_send, ag_recv, halo_send, halo_recv, order_send, order_recv,
    end_send, end_recv, log_send, log_recv, give_send, give_recv,
    near_send, near_recv, far_send, far_recv, move_send, move_recv, out_sem,
):
    seq = lax.axis_index("seq")
    own = lax.axis_index("tp")
    chip, core = own // 2, own % 2
    near_id = chip * 2 + 1 - core
    across_id = (1 - chip) * 2 + core
    diagonal_id = (1 - chip) * 2 + 1 - core
    sibling = (seq, near_id)
    across = (seq, across_id)
    length, width = stream_ref.shape
    depth = w_ref.shape[0]
    inner = y_ref.shape[1]
    mixed = inner + 2 * STATE
    heads = inner // HEAD_DIM
    chunks = length // ROWS
    fines = length // FINE
    per = ROWS // STRETCH
    blocks = length // STRETCH
    pieces = width // COLUMNS
    share = length // count
    state_rows = STATE // count
    following = (seq + 1) % count
    before = (seq + count - 1) % count

    def remote(src, dst, send, recv, device):
        return pltpu.make_async_remote_copy(
            src_ref=src, dst_ref=dst, send_sem=send, recv_sem=recv,
            device_id=device, device_id_type=MESH,
        )

    def other_of(i):
        low = seq < count // 2
        other = jnp.where(low, count - 1 - i, i)
        return jnp.where(low, other - (other <= seq), other + (other >= seq))

    def each(first, last, act):
        def step(i, _):
            act(i)
            return 0

        lax.fori_loop(first, last, step, 0)

    greeted = [sibling, across]
    greeted += [(before, t) for t in range(members)]
    greeted += [((seq + d) % count, own) for d in range(1, count)]
    barrier = pltpu.get_barrier_semaphore()
    for device in greeted:
        pl.semaphore_signal(barrier, inc=1, device_id=device, device_id_type=MESH)

    def load_in(layer, t):
        return pltpu.make_async_copy(
            w_in_ref.at[layer, t * width : (t + 1) * width], raw_ref.at[t % 2], load_sem.at[t % 2]
        )

    def load_bc(layer):
        return pltpu.make_async_copy(w_bc_ref.at[layer], raw_bc_ref, load_sem.at[2])

    own_lanes = lanes_of(own, COLUMNS)
    self_loads, wo_loads = [], []
    for j in range(pieces):
        self_loads.append(
            pltpu.make_async_copy(
                stream_ref.at[:, j * COLUMNS : (j + 1) * COLUMNS],
                full_ref.at[j, :, own_lanes], self_sem,
            )
        )
        for t in range(members):
            first = t * width + j * COLUMNS
            place = j * members + t
            wo_loads.append(
                pltpu.make_async_copy(
                    w_out_ref.at[0, :, first : first + COLUMNS],
                    wo_col_ref.at[:, place * COLUMNS : (place + 1) * COLUMNS],
                    wo_sem.at[0],
                )
            )
    wo_loads.append(pltpu.make_async_copy(w_out_ref.at[1], wo_ref, wo_sem.at[1]))
    for copy in [load_in(0, 0), load_bc(0), load_in(0, 1)] + self_loads + wo_loads:
        copy.start()

    pl.semaphore_wait(barrier, len(greeted))

    last_piece = pieces - 1
    late = pieces - 2

    def block_of(layer, i, owner):
        lanes = lanes_of(owner, COLUMNS)
        if layer == 0:
            return full_ref.at[:, rows_of(i, FINE), lanes], i
        if isinstance(i, int):
            return full_ref.at[i, :, lanes], fines + i
        k, j = i
        slot = fines + late + (j - late) * chunks + k
        return full_ref.at[j, rows_of(k, ROWS), lanes], slot

    def gather_copy(layer, kind, i, owner):
        block, slot = block_of(layer, i, owner)
        return remote(
            block, block, ag_send.at[layer, kind], ag_recv.at[kind, slot],
            across if kind == 0 else sibling,
        )

    def send_rows(k):
        rows = rows_of(k, FINE)
        for kind, device in ((0, across), (1, sibling)):
            for j in range(pieces):
                remote(
                    stream_ref.at[rows, lanes_of(j, COLUMNS)], full_ref.at[j, rows, own_lanes],
                    ag_send.at[0, kind], ag_recv.at[kind, k], device,
                ).start()

    def send_block(layer, i):
        gather_copy(layer, 0, i, own).start()
        gather_copy(layer, 1, i, own).start()

    def forward_block(layer, i):
        gather_copy(layer, 0, i, across_id).wait_recv()
        gather_copy(layer, 2, i, across_id).start()

    def rest_of_block(layer, i):
        gather_copy(layer, 1, i, near_id).wait_recv()
        gather_copy(layer, 2, i, diagonal_id).wait_recv()

    def drain_gather(layer):
        for kind, owner in ((0, own), (1, own), (2, across_id)):
            block = full_ref.at[:, :, lanes_of(owner, COLUMNS)]
            remote(block, block, ag_send.at[layer, kind], ag_recv.at[kind, 0], sibling).wait_send()

    def halo_copy(layer, t, source):
        tail = tail_ref if layer else stream_ref.at[pl.ds(length - HALO, HALO)]
        return remote(
            tail, halo_ref.at[layer, source],
            halo_send.at[layer], halo_recv.at[layer, source], (following, t),
        )

    def halo_piece(j, t):
        lanes = lanes_of(j, COLUMNS)
        return remote(
            tail_ref.at[:, lanes], halo_ref.at[1, own, :, lanes],
            halo_send.at[1], halo_recv.at[1, own], (following, t),
        )

    def order_copy(d):
        return remote(
            order_ref, orders_ref.at[seq], order_send, order_recv, (other_of(d), own)
        )

    def all_orders():
        others = orders_ref.at[pl.ds(0, count - 1)]
        return remote(others, others, order_send, order_recv, (following, own))

    for t in range(members):
        halo_copy(0, t, own).start()

    each(0, fines, send_rows)
    each(0, count - 1, lambda d: order_copy(d).start())

    row = iota((2 * LANES, 2 * LANES), 0)
    col = iota((2 * LANES, 2 * LANES), 1)
    apart = jnp.where(col == 2 * (row % LANES) + row // LANES, 1.0, 0.0).astype(bf16)

    def prepare(layer, t):
        load_in(layer, t).wait()

        def block(j):
            i = t * pieces + j
            rows = rows_of(i, LANES)
            to = rows_of(j * members + t, LANES)
            gain = in_gain_ref[layer : layer + 1, lanes_of(i, LANES)]
            gain = jnp.broadcast_to(gain, (LANES, LANES)).T
            both = raw_ref[t % 2, rows_of(j, LANES)].reshape(2 * LANES, inner)
            halves = jnp.dot(apart, both, preferred_element_type=f32)
            for p in range(inner // LANES):
                lanes = slice(p * LANES, (p + 1) * LANES)
                w_ref[to, lanes] = (halves[:LANES, lanes] * gain).astype(bf16)
                wz_ref[to, lanes] = (halves[LANES:, lanes] * gain).astype(bf16)
            for p in range(2 * STATE // LANES):
                lanes = slice(p * LANES, (p + 1) * LANES)
                w_ref[to, inner + p * LANES : inner + (p + 1) * LANES] = (
                    raw_bc_ref[rows, lanes].astype(f32) * gain
                ).astype(bf16)
            dt = w_dt_ref[layer, :, lanes_of(i, LANES)].astype(f32)
            dt = jnp.concatenate([dt, jnp.zeros((LANES - heads, LANES), f32)], axis=0)
            w_ref[to, mixed:] = (dt.T * gain).astype(bf16)

        each(0, pieces, block)
        if t + 2 < members:
            load_in(layer, t + 2).start()
        elif layer == 0:
            load_in(1, t + 2 - members).start()

    spreader = spreader_of(heads, inner)
    line = iota((STRETCH, STRETCH), 0)
    lane = iota((STRETCH, STRETCH), 1)
    lower = line >= lane
    tri = jnp.where(lower, 1.0, 0.0).astype(bf16)
    left = iota((STRETCH, 2 * HEAD_DIM), 1) < HEAD_DIM

    def late_tokens(rows):
        return jnp.concatenate([full_ref[j, rows, :] for j in range(late, pieces)], axis=1)

    def squares_of(v):
        wide = v.astype(f32)
        return jnp.sum(wide * wide, axis=-1, keepdims=True)

    def scale_of(v):
        return lax.rsqrt(squares_of(v) / depth + epsilon)

    def scan(layer, arrive):
        for t in range(members):
            halo_copy(layer, t, t).wait_recv()
        ahead = jnp.concatenate(
            [
                halo_ref[layer, t, :, j * COLUMNS : (j + 1) * COLUMNS]
                for j in range(pieces) for t in range(members)
            ],
            axis=1,
        )
        ahead = jnp.dot(ahead, w_ref[:, :mixed], preferred_element_type=f32) * scale_of(ahead)
        ahead = ahead[HALO - 8 :, :].astype(bf16).astype(f32)
        ext_ref[0:8, :] = jnp.where(seq > 0, ahead, 0.0)
        state_ref[...] = jnp.zeros_like(state_ref)
        sofar_ref[...] = jnp.zeros_like(sofar_ref)
        bias = pad_row(bias_ref[layer : layer + 1, :])
        rate = pad_row(jnp.exp(a_log_ref[layer : layer + 1, :]))
        skip = pad_row(d_skip_ref[layer : layer + 1, :])
        skip = expand(jnp.broadcast_to(skip, (8, LANES)), heads, spreader)[0:1]
        taps = jnp.concatenate([conv_x_ref[layer], conv_bc_ref[layer]], axis=1)
        tap_count = taps.shape[0]

        size = ROWS if layer else FINE
        parts = size // STRETCH

        def project(k):
            rows = rows_of(k, size)
            arrive(k)
            if layer == 0:
                tokens = jnp.concatenate([full_ref[j, rows, :] for j in range(pieces)], axis=1)
                scale = scale_of(tokens)
                projected = jnp.dot(tokens, w_ref[...], preferred_element_type=f32)
                gate = jnp.dot(tokens, wz_ref[...], preferred_element_type=f32)
                z_ref[rows, :] = (gate * scale).astype(bf16)
            else:
                tokens = late_tokens(rows)
                square = scale_ref[rows, 0:1] + squares_of(tokens)
                scale = lax.rsqrt(square / depth + epsilon)
                projected = acc_ref[rows, :] + jnp.dot(
                    tokens, w_ref[late * width :, :], preferred_element_type=f32
                )
                scale_ref[rows, :] = jnp.broadcast_to(scale, (size, LANES))
            projected = projected * scale
            raw = projected[:, mixed:] + bias
            step = jnp.maximum(raw, 0.0) + jnp.log1p(jnp.exp(-jnp.abs(raw)))
            logs = pack_pieces(-step * rate, heads)
            sofar = sofar_ref[...]
            summed_logs = jnp.dot(
                tri,
                jnp.concatenate(
                    [logs[b * STRETCH : (b + 1) * STRETCH] for b in range(parts)], axis=1
                ),
                preferred_element_type=f32,
            )
            to_end, whole, earlier = [], [], []
            for b in range(parts):
                cum = unpack_sum(summed_logs[:, b * LANES : (b + 1) * LANES], heads)
                last = cum[STRETCH - 1 : STRETCH, :]
                cum_ref[rows_of(k * parts + b, STRETCH), :] = cum
                to_end.append(step[b * STRETCH : (b + 1) * STRETCH] * jnp.exp(last - cum))
                whole.append(jnp.exp(jnp.broadcast_to(last, (8, LANES))))
                earlier.append(jnp.exp(sofar))
                sofar = sofar + last
            sofar_ref[...] = sofar
            factors = expand(
                jnp.concatenate([step] + to_end + whole + earlier, axis=0), heads, spreader
            )
            ext_ref[8 : 8 + size, :] = projected[:, :mixed].astype(bf16).astype(f32)
            conv = jnp.zeros((size, mixed), f32)
            for tap in range(tap_count):
                first = 9 - tap_count + tap
                conv = conv + taps[tap : tap + 1, :] * ext_ref[first : first + size, :]
            conv = conv * jax.nn.sigmoid(conv)
            ext_ref[0:8, :] = ext_ref[size : size + 8, :]
            x = conv[:, :inner]
            b_all = conv[:, inner : inner + STATE]
            b_ref[rows, :] = b_all.astype(bf16)
            c_ref[rows, :] = conv[:, inner + STATE :].astype(bf16)
            feed_ref[rows, :] = (x * factors[:size]).astype(bf16)
            y_ref[rows, :] = skip * x
            ending = (x * factors[size : 2 * size]).astype(bf16)
            state = state_ref[...]
            for b in range(parts):
                part = slice(b * STRETCH, (b + 1) * STRETCH)
                index = k * parts + b
                fresh = jnp.dot(
                    b_all[part].T.astype(bf16), ending[part], preferred_element_type=f32
                )
                first = 2 * size + 8 * b
                states_ref[index] = state
                sofar_exp_ref[index] = factors[first + 8 * parts : first + 8 * parts + 8]
                state = state * factors[first : first + 1] + fresh
            state_ref[...] = state

        each(0, length // size, project)

    def within(layer, k):
        if layer:
            rows = rows_of(k, ROWS)
            gate = gate_ref[rows, :] + jnp.dot(
                late_tokens(rows), wz_ref[late * width :, :], preferred_element_type=f32
            )
            z_ref[rows, :] = (gate * scale_ref[rows, 0:1]).astype(bf16)

        def block(b):
            rows = rows_of(k * per + b, STRETCH)
            cum = cum_ref[rows, :]
            cum_t = cum.T
            feed = feed_ref[rows, :]
            meet = lax.dot_general(
                c_ref[rows, :], b_ref[rows, :], (((1,), (1,)), ((), ())),
                preferred_element_type=f32,
            )
            for pair in range(heads // 2):
                lanes = slice(pair * 2 * HEAD_DIM, (pair + 1) * 2 * HEAD_DIM)
                weights = []
                for h in (2 * pair, 2 * pair + 1):
                    spread = jnp.where(lower, cum[:, h : h + 1] - cum_t[h : h + 1, :], -jnp.inf)
                    weights.append((meet * jnp.exp(spread)).astype(bf16))
                fed = feed[:, lanes]
                nought = jnp.zeros_like(fed)
                stacked = jnp.concatenate(
                    [jnp.where(left, fed, nought), jnp.where(left, nought, fed)], axis=0
                )
                inside = jnp.dot(
                    jnp.concatenate(weights, axis=1), stacked, preferred_element_type=f32
                )
                y_ref[rows, lanes] = y_ref[rows, lanes] + inside

        each(0, per, block)

    def exchange(layer):
        def end_copy(d):
            other = other_of(d)
            return remote(
                end_ref.at[layer, other], got_ref.at[layer, seq],
                end_send.at[layer], end_recv.at[layer], (other, own),
            )

        def log_copy(d):
            return remote(
                log_ref.at[layer], logs_ref.at[layer, seq],
                log_send.at[layer], log_recv.at[layer], (other_of(d), own),
            )

        def give_copy(d):
            other = other_of(d)
            return remote(
                give_ref.at[layer, other], arriving_ref.at[layer, seq],
                give_send.at[layer], give_recv.at[layer], (other, own),
            )

        others = pl.ds(0, count - 1)

        def all_of(ref, send, recv):
            block = ref.at[layer, others]
            return remote(block, block, send.at[layer], recv.at[layer], (following, own))

        all_ends = all_of(got_ref, end_send, end_recv)
        all_logs = all_of(logs_ref, log_send, log_recv)
        all_given = all_of(arriving_ref, give_send, give_recv)

        state = state_ref[...]
        for d in range(count):
            end_ref[layer, d] = state[d * state_rows : (d + 1) * state_rows].astype(bf16)
        log_ref[layer] = sofar_ref[0:1, :]

        def send(d):
            log_copy(d).start()
            end_copy(d).start()

        each(0, count - 1, send)
        each(0, chunks // 2, lambda k: within(layer, k))
        all_logs.wait_recv()
        all_ends.wait_recv()
        got_ref[layer, seq] = end_ref[layer, seq]
        logs_ref[layer, seq] = log_ref[layer]
        logs = jnp.concatenate([logs_ref[layer, d] for d in range(count)], axis=0)
        factors = expand(jnp.exp(logs), heads, spreader)
        prefix = jnp.zeros((state_rows, inner), f32)
        for d in range(count):
            give_ref[layer, d] = prefix.astype(bf16)
            if d + 1 < count:
                prefix = prefix * factors[d : d + 1] + got_ref[layer, d].astype(f32)
        each(0, count - 1, lambda d: give_copy(d).start())
        each(chunks // 2, chunks, lambda k: within(layer, k))
        all_given.wait_recv()
        arriving_ref[layer, seq] = give_ref[layer, seq]
        prefix_ref[...] = jnp.concatenate(
            [arriving_ref[layer, d].astype(f32) for d in range(count)], axis=0
        )

        all_logs.wait_send()
        all_ends.wait_send()
        all_given.wait_send()

    pair = 2 * HEAD_DIM
    one = iota((2 * pair, pair), 0) % pair // HEAD_DIM
    two = iota((2 * pair, pair), 1) // HEAD_DIM
    averager = jnp.where(one == two, 1.0 / HEAD_DIM, 0.0).astype(bf16)

    def mixed_of(layer, k):
        rows = rows_of(k, ROWS)
        grown = expand(jnp.exp(cum_ref[rows, :]), heads, spreader)
        carried = []
        for block in range(per):
            index = k * per + block
            state = states_ref[index] + prefix_ref[...] * sofar_exp_ref[index][0:1]
            carried.append(
                jnp.dot(
                    c_ref[rows_of(index, STRETCH), :], state.astype(bf16),
                    preferred_element_type=f32,
                )
            )
        gate = z_ref[rows, :].astype(f32)
        ssd = y_ref[rows, :] + jnp.concatenate(carried, axis=0) * grown
        gated = ssd * (gate * jax.nn.sigmoid(gate))
        square = gated * gated
        high = square.astype(bf16)
        low = (square - high.astype(f32)).astype(bf16)
        results = []
        for p in range(inner // pair):
            lanes = slice(p * pair, (p + 1) * pair)
            both = jnp.concatenate([high[:, lanes], low[:, lanes]], axis=1)
            mean = jnp.dot(both, averager, preferred_element_type=f32)
            scaled = gated[:, lanes] * lax.rsqrt(mean + epsilon)
            results.append((scaled * out_gain_ref[layer : layer + 1, lanes]).astype(bf16))
        return jnp.concatenate(results, axis=1)

    def part_of(layer, i):
        if layer == 1:
            rows, slot = rows_of(i, ROWS), i
            lanes, held = (lambda t: lanes_of(t, width)), pl.ds(0, width)
        else:
            if isinstance(i, int):
                rows, j, slot = pl.ds(0, length), i, chunks + i - 1
            else:
                rows, j, slot = rows_of(i[0], ROWS), 0, i[0]
            lanes, held = (lambda t: lanes_of(j * members + t, COLUMNS)), lanes_of(j, COLUMNS)
        nears = [near_ref.at[side, rows, held] for side in range(2)]
        return rows, lanes, nears, (sum_ref.at[rows, held], far_ref.at[rows, held]), slot

    def near_part(layer, side, i):
        rows, lanes, nears, _, slot = part_of(layer, i)
        block = diagonal_id if side == 0 else near_id
        return remote(
            partial_ref.at[rows, lanes(block)], nears[side],
            near_send.at[layer, side], near_recv.at[layer, side, slot], sibling,
        )

    def far_part(layer, i):
        _, _, _, (summing, far), slot = part_of(layer, i)
        return remote(summing, far, far_send.at[layer], far_recv.at[layer, slot], across)

    def send_near(layer, i):
        near_part(layer, 0, i).start()
        near_part(layer, 1, i).start()

    def send_far(layer, i):
        rows, lanes, nears, (summing, _), _ = part_of(layer, i)
        near_part(layer, 0, i).wait_recv()
        summing[...] = (
            partial_ref[rows, lanes(across_id)].astype(f32) + nears[0][...].astype(f32)
        ).astype(bf16)
        far_part(layer, i).start()

    def summed(layer, i, stream):
        rows, lanes, nears, (_, far), _ = part_of(layer, i)
        near_part(layer, 1, i).wait_recv()
        far_part(layer, i).wait_recv()
        return (
            stream.astype(f32)
            + partial_ref[rows, lanes(own)].astype(f32)
            + nears[1][...].astype(f32)
            + far[...].astype(f32)
        ).astype(bf16)

    def drain_sums(layer):
        for side in range(2):
            block = near_ref.at[side]
            remote(
                block, block, near_send.at[layer, side], near_recv.at[layer, side, 0], sibling
            ).wait_send()
        remote(sum_ref, sum_ref, far_send.at[layer], far_recv.at[layer, 0], across).wait_send()

    def plan():
        shift = length.bit_length() - 1
        all_orders().wait_recv()
        orders_ref[seq] = order_ref[...]
        orders = jnp.concatenate([orders_ref[d] for d in range(count)], axis=0)

        def count_up(r):
            first = iota((LANES, length), 0) + r * LANES
            place_ref[rows_of(r, LANES), :] = jnp.where(
                first <= iota((LANES, length), 1), 1.0, 0.0
            ).astype(bf16)

        each(0, length // LANES, count_up)
        device = iota((count, length), 0)
        wanted_here = jnp.right_shift(orders, shift) == seq
        from_each = jnp.right_shift(order_ref[...], shift) == device
        ones = jnp.concatenate(
            [jnp.where(wanted_here, 1.0, 0.0), jnp.where(from_each, 1.0, 0.0)], axis=0
        ).astype(bf16)
        counted = jnp.dot(ones, place_ref[...], preferred_element_type=f32).astype(jnp.int32) - 1
        slot = jnp.where(wanted_here, counted[:count], -1)
        local = jnp.bitwise_and(orders, length - 1)
        short = iota((share, length), 0)
        long = iota((share, length), 1)
        for d in range(count):
            chosen = slot[d : d + 1, :] == short
            found = jnp.where(chosen, local[d : d + 1, :], 0).astype(f32)
            wanted = jnp.sum(found, axis=1, keepdims=True).astype(jnp.int32)
            hand_ref[d * share : (d + 1) * share, :] = jnp.where(
                wanted == long, 1.0, 0.0
            ).astype(bf16)
        target = jnp.where(from_each, counted[count:] + share * device, 0).astype(f32)
        target = jnp.sum(target, axis=0, keepdims=True)
        target = jnp.broadcast_to(target, (LANES, length)).T.astype(jnp.int32)
        for c in range(length // LANES):
            place_ref[:, c * LANES : (c + 1) * LANES] = jnp.where(
                target == iota((length, LANES), 1) + c * LANES, 1.0, 0.0
            ).astype(bf16)

    def move_copy(j, d):
        other = other_of(d)
        return remote(
            leaving_ref.at[j, rows_of(other, share)], arrived_ref.at[j, rows_of(seq, share)],
            move_send, move_recv.at[j], (other, own),
        )

    def all_moves(j):
        others = arrived_ref.at[j, pl.ds(0, length - share)]
        return remote(others, others, move_send, move_recv.at[j], (following, own))

    def hand_over(j):
        if j:
            held = summed(0, j, full_ref[j, :, own_lanes])
        else:

            def first(k):
                rows = rows_of(k, ROWS)
                held_ref[rows, :] = summed(0, (k,), full_ref[0, rows, own_lanes])

            each(0, chunks, first)
            held = held_ref[...]
        leaving_ref[j] = jnp.dot(hand_ref[...], held, preferred_element_type=f32).astype(bf16)
        each(0, count - 1, lambda d: move_copy(j, d).start())
        arrived_ref[j, rows_of(seq, share), :] = leaving_ref[j, rows_of(seq, share), :]

    def put(j):
        lanes = slice(j * COLUMNS, (j + 1) * COLUMNS)
        all_moves(j).wait_recv()
        rows = jnp.dot(place_ref[...], arrived_ref[j], preferred_element_type=f32).astype(bf16)
        tail_ref[:, lanes] = rows[length - HALO :]
        full_ref[j, :, own_lanes] = rows
        for t in range(members):
            halo_piece(j, t).start()
        if j < late:
            send_block(1, j)
        elif j < last_piece:
            send_block(1, (0, j))
        else:
            send_block(1, (0, j))

            def send_late(k):
                for other in range(late, pieces):
                    send_block(1, (k, other))

            each(1, chunks, send_late)
        own_ref[:, lanes] = rows

    def accumulate(j):
        part = slice(j * width, (j + 1) * width)

        def product(k):
            rows = rows_of(k, ROWS)
            result = jnp.dot(
                full_ref[j, rows, :], w_ref[part, :], preferred_element_type=f32
            )
            acc_ref[rows, :] = result if j == 0 else acc_ref[rows, :] + result
            gate = jnp.dot(full_ref[j, rows, :], wz_ref[part, :], preferred_element_type=f32)
            gate_ref[rows, :] = gate if j == 0 else gate_ref[rows, :] + gate
            square = jnp.broadcast_to(squares_of(full_ref[j, rows, :]), (ROWS, LANES))
            scale_ref[rows, :] = square if j == 0 else scale_ref[rows, :] + square

        each(0, chunks, product)

    load_bc(0).wait()
    for t in range(members):
        prepare(0, t)
    load_bc(1).start()
    own_columns = full_ref.at[:, :, own_lanes]
    pltpu.make_async_copy(own_columns, own_columns, self_sem).wait()

    def arrive_first(k):
        forward_block(0, k)
        rest_of_block(0, k)

    scan(0, arrive_first)
    exchange(0)
    drain_gather(0)
    pltpu.make_async_copy(w_out_ref.at[0], wo_col_ref, wo_sem.at[0]).wait()
    pltpu.make_async_copy(w_out_ref.at[1], wo_ref, wo_sem.at[1]).wait()

    def product_of(k, j):
        rows, lanes = rows_of(k, ROWS), lanes_of(j, members * COLUMNS)
        partial_ref[rows, lanes] = jnp.dot(
            mixed_ref[rows, :], wo_col_ref[:, lanes], preferred_element_type=f32
        ).astype(bf16)

    def mix(k):
        mixed_ref[rows_of(k, ROWS), :] = mixed_of(0, k)
        product_of(k, 0)
        send_near(0, (k,))

        @pl.when(k > 0)
        def _():
            send_far(0, (k - 1,))

    each(0, chunks, mix)
    for j in range(1, pieces):
        each(0, chunks, lambda k: product_of(k, j))
        send_near(0, j)
        send_far(0, j - 1 if j > 1 else (chunks - 1,))
    send_far(0, pieces - 1)
    plan()
    load_bc(1).wait()

    for j in range(pieces):
        hand_over(j)
        if j > 1:
            put(j - 2)
        prepare(1, j)
    put(pieces - 2)
    forward_block(1, 0)
    rest_of_block(1, 0)
    accumulate(0)
    put(pieces - 1)
    drain_sums(0)

    for j in range(1, late):
        forward_block(1, j)
        rest_of_block(1, j)
        accumulate(j)

    def forward_late(k):
        for j in range(late, pieces):
            forward_block(1, (k, j))

    forward_late(0)

    def arrive_second(k):
        @pl.when(k + 1 < chunks)
        def _():
            forward_late(k + 1)

        for j in range(late, pieces):
            rest_of_block(1, (k, j))

    scan(1, arrive_second)
    exchange(1)

    def output_rows(k):
        rows = rows_of(k, ROWS)
        mixed_heads = mixed_of(1, k)
        for side, block in enumerate((diagonal_id, near_id, across_id, own)):
            lanes = lanes_of(block, width)
            partial_ref[rows, lanes] = jnp.dot(
                mixed_heads, wo_ref[:, lanes], preferred_element_type=f32
            ).astype(bf16)
            if side < 2:
                near_part(1, side, k).start()
        send_far(1, k)

    each(0, chunks, output_rows)

    def out_copy(k):
        rows = rows_of(k, ROWS)
        return pltpu.make_async_copy(own_ref.at[rows], out_ref.at[rows], out_sem.at[k])

    def finish(k):
        rows = rows_of(k, ROWS)
        own_ref[rows, :] = summed(1, k, own_ref[rows, :])
        out_copy(k).start()

    each(0, chunks, finish)
    drain_gather(1)
    drain_sums(1)
    for layer in range(2):
        block = halo_ref.at[layer]
        remote(
            block, block, halo_send.at[layer], halo_recv.at[layer, 0], (following, own)
        ).wait_send()
    all_orders().wait_send()
    others = arrived_ref.at[:, pl.ds(0, length - share)]
    remote(others, others, move_send, move_recv.at[0], (following, own)).wait_send()
    each(0, chunks, lambda k: out_copy(k).wait())


def body(
    tokens, col_order, in_gain, w_in, w_bc, w_dt, conv_x, conv_bc,
    dt_bias, a_log, d_skip, out_gain, w_out,
):
    count, members = lax.axis_size("seq"), lax.axis_size("tp")
    length, width = tokens.shape
    inner = w_out.shape[1]
    heads = inner // HEAD_DIM
    mixed = inner + 2 * STATE
    depth = w_in.shape[1]
    chunks, fines = length // ROWS, length // FINE
    blocks = length // STRETCH
    pieces = width // COLUMNS
    state_rows = STATE // count
    vmem = pl.BlockSpec(memory_space=pltpu.VMEM)
    hbm = pl.BlockSpec(memory_space=pltpu.HBM)
    dma = pltpu.SemaphoreType.DMA
    return pl.pallas_call(
        functools.partial(layers_kernel, count, members),
        in_specs=[hbm, vmem, vmem, hbm, hbm] + [vmem] * 7 + [hbm],
        out_specs=hbm,
        out_shape=jax.ShapeDtypeStruct(tokens.shape, bf16),
        scratch_shapes=[
            pltpu.VMEM((pieces, length, members * COLUMNS), bf16),
            pltpu.VMEM((HALO, width), bf16),
            pltpu.VMEM((2, members, HALO, width), bf16),
            pltpu.VMEM((count, 1, length), jnp.int32),
            pltpu.VMEM((2, width, 2, inner), bf16),
            pltpu.VMEM((depth, 2 * STATE), bf16),
            pltpu.VMEM((depth, mixed + LANES), bf16),
            pltpu.VMEM((depth, inner), bf16),
            pltpu.VMEM((inner, depth), bf16),
            pltpu.VMEM((inner, depth), bf16),
            pltpu.VMEM((ROWS + 8, mixed), f32),
            pltpu.VMEM((length, inner), f32),
            pltpu.VMEM((length, inner), bf16),
            pltpu.VMEM((length, inner), bf16),
            pltpu.VMEM((length, STATE), bf16),
            pltpu.VMEM((length, STATE), bf16),
            pltpu.VMEM((length, LANES), f32),
            pltpu.VMEM((length, LANES), f32),
            pltpu.VMEM((blocks, STATE, inner), f32),
            pltpu.VMEM((blocks, 8, inner), f32),
            pltpu.VMEM((STATE, inner), f32),
            pltpu.VMEM((8, LANES), f32),
            pltpu.VMEM((2, count, state_rows, inner), bf16),
            pltpu.VMEM((2, 1, LANES), f32),
            pltpu.VMEM((2, count, state_rows, inner), bf16),
            pltpu.VMEM((2, count, 1, LANES), f32),
            pltpu.VMEM((2, count, state_rows, inner), bf16),
            pltpu.VMEM((2, count, state_rows, inner), bf16),
            pltpu.VMEM((STATE, inner), f32),
            pltpu.VMEM((length, depth), bf16),
            pltpu.VMEM((2, length, width), bf16),
            pltpu.VMEM((length, width), bf16),
            pltpu.VMEM((length, width), bf16),
            pltpu.VMEM((length, inner), bf16),
            pltpu.VMEM((length, length), bf16),
            pltpu.VMEM((length, length), bf16),
            pltpu.VMEM((pieces, length, COLUMNS), bf16),
            pltpu.VMEM((pieces, length, COLUMNS), bf16),
            pltpu.VMEM((length, COLUMNS), bf16),
            pltpu.VMEM((length, mixed + LANES), f32),
            pltpu.VMEM((length, inner), f32),
            pltpu.VMEM((length, width), bf16),
            dma((3,)), dma((2,)), dma,
            dma((2, 3)), dma((3, fines + 2 * chunks + pieces - 2)),
            dma((2,)), dma((2, members)), dma, dma,
            dma((2,)), dma((2,)), dma((2,)), dma((2,)), dma((2,)), dma((2,)),
            dma((2, 2)), dma((2, 2, chunks + pieces - 1)),
            dma((2,)), dma((2, chunks + pieces - 1)),
            dma, dma((pieces,)), dma((chunks,)),
        ],
        compiler_params=pltpu.CompilerParams(
            collective_id=0, has_side_effects=True, vmem_limit_bytes=63 * 1024 * 1024
        ),
        name="mixer_layers",
    )(
        tokens, col_order[None], in_gain, w_in, w_bc, jnp.swapaxes(w_dt, 1, 2), conv_x, conv_bc,
        dt_bias, a_log, d_skip, out_gain, w_out,
    )


def solution(mesh):
    placed = (
        P("seq", "tp"),
        P("seq"),
        P(),
        P(None, None, None, "tp"),
        P(),
        P(None, None, "tp"),
        P(None, None, "tp"),
        P(),
        P(None, "tp"),
        P(None, "tp"),
        P(None, "tp"),
        P(None, "tp"),
        P(None, "tp", None),
    )
    return jax.shard_map(
        body, mesh=mesh, in_specs=placed, out_specs=P("seq", "tp"), check_vma=False
    )
```

```python
import functools

import jax
import jax.numpy as jnp
from jax import lax
from jax.experimental import pallas as pl
from jax.experimental.pallas import tpu as pltpu
from jax.sharding import PartitionSpec as P

HEAD_DIM = 64
STATE = 128
STRETCH = 128
LANES = 128
HALO = 16
ROWS = 256
FINE = 128
HALVES = 2
COLUMNS = 128

epsilon = 1e-05
f32 = jnp.float32
bf16 = jnp.bfloat16
MESH = pl.DeviceIdType.MESH


def iota(shape, axis):
    return lax.broadcasted_iota(jnp.int32, shape, axis)


def spreader_of(heads, inner):
    row = iota((LANES, inner), 0)
    channel = iota((LANES, inner), 1)
    chosen = (row % heads == channel // HEAD_DIM) & (row < 3 * heads)
    return jnp.where(chosen, 1.0, 0.0).astype(bf16)


def pack_pieces(values, heads):
    values = jnp.where(iota(values.shape, 1) < heads, values, 0.0)
    high = values.astype(bf16).astype(f32)
    rest = values - high
    middle = rest.astype(bf16).astype(f32)
    low = rest - middle
    packed = high + pltpu.roll(middle, heads, 1) + pltpu.roll(low, 2 * heads, 1)
    return packed.astype(bf16)


def expand(values, heads, spreader):
    return jnp.dot(pack_pieces(values, heads), spreader, preferred_element_type=f32)


def unpack_sum(pieces, heads):
    total = (
        pieces
        + pltpu.roll(pieces, LANES - heads, 1)
        + pltpu.roll(pieces, LANES - 2 * heads, 1)
    )
    return jnp.where(iota(total.shape, 1) < heads, total, 0.0)


def rows_of(k, size):
    return pl.ds(pl.multiple_of(k * size, size), size)


def lanes_of(k, size):
    return pl.ds(pl.multiple_of(k * size, LANES), size)


def pad_row(row):
    return jnp.concatenate([row, jnp.zeros((1, LANES - row.shape[1]), f32)], axis=1)


def layers_kernel(
    count, members,
    stream_ref, order_ref, in_gain_ref, w_in_ref, w_bc_ref, w_dt_ref, conv_x_ref, conv_bc_ref,
    bias_ref, a_log_ref, d_skip_ref, out_gain_ref, w_out_ref,
    out_ref,
    full_ref, tail_ref, halo_ref, orders_ref, raw_ref, raw_bc_ref, w_ref, wz_ref, wo_col_ref, wo_ref,
    ext_ref, y_ref, z_ref, feed_ref, b_ref, c_ref, cum_ref, scale_ref, states_ref, sofar_exp_ref,
    state_ref, sofar_ref,
    end_ref, log_ref, got_ref, logs_ref, give_ref, arriving_ref, prefix_ref,
    partial_ref, near_ref, sum_ref, far_ref,
    mixed_ref, hand_ref, place_ref, leaving_ref, arrived_ref, held_ref, acc_ref, gate_ref, own_ref,
    load_sem, wo_sem, self_sem, ag_send, ag_recv, halo_send, halo_recv, order_send, order_recv,
    end_send, end_recv, log_send, log_recv, give_send, give_recv,
    near_send, near_recv, far_send, far_recv, move_send, move_recv, out_sem,
):
    seq = lax.axis_index("seq")
    own = lax.axis_index("tp")
    chip, core = own // 2, own % 2
    near_id = chip * 2 + 1 - core
    across_id = (1 - chip) * 2 + core
    diagonal_id = (1 - chip) * 2 + 1 - core
    sibling = (seq, near_id)
    across = (seq, across_id)
    length, width = stream_ref.shape
    depth = w_ref.shape[0]
    inner = y_ref.shape[1]
    mixed = inner + 2 * STATE
    heads = inner // HEAD_DIM
    chunks = length // ROWS
    fines = length // FINE
    per = ROWS // STRETCH
    blocks = length // STRETCH
    pieces = width // COLUMNS
    share = length // count
    state_rows = STATE // count
    half_rows = state_rows // HALVES
    following = (seq + 1) % count
    before = (seq + count - 1) % count

    def remote(src, dst, send, recv, device):
        return pltpu.make_async_remote_copy(
            src_ref=src, dst_ref=dst, send_sem=send, recv_sem=recv,
            device_id=device, device_id_type=MESH,
        )

    def other_of(i):
        low = seq < count // 2
        other = jnp.where(low, count - 1 - i, i)
        return jnp.where(low, other - (other <= seq), other + (other >= seq))

    def each(first, last, act):
        def step(i, _):
            act(i)
            return 0

        lax.fori_loop(first, last, step, 0)

    greeted = [sibling, across]
    greeted += [(before, t) for t in range(members)]
    greeted += [((seq + d) % count, own) for d in range(1, count)]
    barrier = pltpu.get_barrier_semaphore()
    for device in greeted:
        pl.semaphore_signal(barrier, inc=1, device_id=device, device_id_type=MESH)

    def load_in(layer, t):
        return pltpu.make_async_copy(
            w_in_ref.at[layer, t * width : (t + 1) * width], raw_ref.at[t % 2], load_sem.at[t % 2]
        )

    def load_bc(layer):
        return pltpu.make_async_copy(w_bc_ref.at[layer], raw_bc_ref, load_sem.at[2])

    own_lanes = lanes_of(own, COLUMNS)
    self_loads, wo_loads = [], []
    for j in range(pieces):
        self_loads.append(
            pltpu.make_async_copy(
                stream_ref.at[:, j * COLUMNS : (j + 1) * COLUMNS],
                full_ref.at[j, :, own_lanes], self_sem,
            )
        )
        for t in range(members):
            first = t * width + j * COLUMNS
            place = j * members + t
            wo_loads.append(
                pltpu.make_async_copy(
                    w_out_ref.at[0, :, first : first + COLUMNS],
                    wo_col_ref.at[:, place * COLUMNS : (place + 1) * COLUMNS],
                    wo_sem.at[0],
                )
            )
    wo_loads.append(pltpu.make_async_copy(w_out_ref.at[1], wo_ref, wo_sem.at[1]))
    for copy in [load_in(0, 0), load_bc(0), load_in(0, 1)] + self_loads + wo_loads:
        copy.start()

    pl.semaphore_wait(barrier, len(greeted))

    last_piece = pieces - 1
    early = chunks // 2
    late = pieces - 2

    def block_of(layer, i, owner):
        lanes = lanes_of(owner, COLUMNS)
        if layer == 0:
            return full_ref.at[:, rows_of(i, FINE), lanes], i
        if isinstance(i, int):
            return full_ref.at[i, :, lanes], fines + i
        slot = fines + late + i[0]
        return full_ref.at[pl.ds(late, pieces - late), rows_of(i[0], ROWS), lanes], slot

    def send_part(j, k):
        part = full_ref.at[j, rows_of(k, ROWS), own_lanes]
        slot = fines + late + k
        for kind, device in ((0, across), (1, sibling)):
            remote(part, part, ag_send.at[1, kind], ag_recv.at[kind, slot], device).start()

    def gather_copy(layer, kind, i, owner):
        block, slot = block_of(layer, i, owner)
        return remote(
            block, block, ag_send.at[layer, kind], ag_recv.at[kind, slot],
            across if kind == 0 else sibling,
        )

    def send_rows(k):
        rows = rows_of(k, FINE)
        for kind, device in ((0, across), (1, sibling)):
            for j in range(pieces):
                remote(
                    stream_ref.at[rows, lanes_of(j, COLUMNS)], full_ref.at[j, rows, own_lanes],
                    ag_send.at[0, kind], ag_recv.at[kind, k], device,
                ).start()

    def send_block(layer, i):
        gather_copy(layer, 0, i, own).start()
        gather_copy(layer, 1, i, own).start()

    def forward_block(layer, i):
        gather_copy(layer, 0, i, across_id).wait_recv()
        gather_copy(layer, 2, i, across_id).start()

    def rest_of_block(layer, i):
        gather_copy(layer, 1, i, near_id).wait_recv()
        gather_copy(layer, 2, i, diagonal_id).wait_recv()

    def drain_gather(layer):
        for kind, owner in ((0, own), (1, own), (2, across_id)):
            block = full_ref.at[:, :, lanes_of(owner, COLUMNS)]
            remote(block, block, ag_send.at[layer, kind], ag_recv.at[kind, 0], sibling).wait_send()

    def halo_copy(layer, t, source):
        tail = tail_ref if layer else stream_ref.at[pl.ds(length - HALO, HALO)]
        return remote(
            tail, halo_ref.at[layer, source],
            halo_send.at[layer], halo_recv.at[layer, source], (following, t),
        )

    def halo_piece(j, t):
        lanes = lanes_of(j, COLUMNS)
        return remote(
            tail_ref.at[:, lanes], halo_ref.at[1, own, :, lanes],
            halo_send.at[1], halo_recv.at[1, own], (following, t),
        )

    def order_copy(d):
        return remote(
            order_ref, orders_ref.at[seq], order_send, order_recv, (other_of(d), own)
        )

    def all_orders():
        others = orders_ref.at[pl.ds(0, count - 1)]
        return remote(others, others, order_send, order_recv, (following, own))

    for t in range(members):
        halo_copy(0, t, own).start()

    each(0, fines, send_rows)
    each(0, count - 1, lambda d: order_copy(d).start())

    row = iota((2 * LANES, 2 * LANES), 0)
    col = iota((2 * LANES, 2 * LANES), 1)
    apart = jnp.where(col == 2 * (row % LANES) + row // LANES, 1.0, 0.0).astype(bf16)

    def prepare(layer, t):
        load_in(layer, t).wait()

        def block(j):
            i = t * pieces + j
            rows = rows_of(i, LANES)
            to = rows_of(j * members + t, LANES)
            gain = in_gain_ref[layer : layer + 1, lanes_of(i, LANES)]
            gain = jnp.broadcast_to(gain, (LANES, LANES)).T
            both = raw_ref[t % 2, rows_of(j, LANES)].reshape(2 * LANES, inner)
            halves = jnp.dot(apart, both, preferred_element_type=f32)
            for p in range(inner // LANES):
                lanes = slice(p * LANES, (p + 1) * LANES)
                w_ref[to, lanes] = (halves[:LANES, lanes] * gain).astype(bf16)
                wz_ref[to, lanes] = (halves[LANES:, lanes] * gain).astype(bf16)
            for p in range(2 * STATE // LANES):
                lanes = slice(p * LANES, (p + 1) * LANES)
                w_ref[to, inner + p * LANES : inner + (p + 1) * LANES] = (
                    raw_bc_ref[rows, lanes].astype(f32) * gain
                ).astype(bf16)
            dt = w_dt_ref[layer, :, lanes_of(i, LANES)].astype(f32)
            dt = jnp.concatenate([dt, jnp.zeros((LANES - heads, LANES), f32)], axis=0)
            w_ref[to, mixed:] = (dt.T * gain).astype(bf16)

        each(0, pieces, block)
        if t + 2 < members:
            load_in(layer, t + 2).start()
        elif layer == 0:
            load_in(1, t + 2 - members).start()

    spreader = spreader_of(heads, inner)
    line = iota((STRETCH, STRETCH), 0)
    lane = iota((STRETCH, STRETCH), 1)
    lower = line >= lane
    tri = jnp.where(lower, 1.0, 0.0).astype(bf16)
    left = iota((STRETCH, 2 * HEAD_DIM), 1) < HEAD_DIM

    def late_tokens(rows):
        return jnp.concatenate([full_ref[j, rows, :] for j in range(late, pieces)], axis=1)

    def squares_of(v):
        wide = v.astype(f32)
        return jnp.sum(wide * wide, axis=-1, keepdims=True)

    def scale_of(v):
        return lax.rsqrt(squares_of(v) / depth + epsilon)

    def scan(layer, arrive):
        for t in range(members):
            halo_copy(layer, t, t).wait_recv()
        ahead = jnp.concatenate(
            [
                halo_ref[layer, t, :, j * COLUMNS : (j + 1) * COLUMNS]
                for j in range(pieces) for t in range(members)
            ],
            axis=1,
        )
        ahead = jnp.dot(ahead, w_ref[:, :mixed], preferred_element_type=f32) * scale_of(ahead)
        ahead = ahead[HALO - 8 :, :].astype(bf16).astype(f32)
        ext_ref[0:8, :] = jnp.where(seq > 0, ahead, 0.0)
        state_ref[...] = jnp.zeros_like(state_ref)
        sofar_ref[...] = jnp.zeros_like(sofar_ref)
        bias = pad_row(bias_ref[layer : layer + 1, :])
        rate = pad_row(jnp.exp(a_log_ref[layer : layer + 1, :]))
        skip = pad_row(d_skip_ref[layer : layer + 1, :])
        skip = expand(jnp.broadcast_to(skip, (8, LANES)), heads, spreader)[0:1]
        taps = jnp.concatenate([conv_x_ref[layer], conv_bc_ref[layer]], axis=1)
        tap_count = taps.shape[0]

        size = ROWS if layer else FINE
        parts = size // STRETCH

        def project(k):
            rows = rows_of(k, size)
            arrive(k)
            if layer == 0:
                tokens = jnp.concatenate([full_ref[j, rows, :] for j in range(pieces)], axis=1)
                scale = scale_of(tokens)
                projected = jnp.dot(tokens, w_ref[...], preferred_element_type=f32)
                gate = jnp.dot(tokens, wz_ref[...], preferred_element_type=f32)
                z_ref[rows, :] = (gate * scale).astype(bf16)
            else:
                tokens = late_tokens(rows)
                square = scale_ref[rows, 0:1] + squares_of(tokens)
                scale = lax.rsqrt(square / depth + epsilon)
                projected = acc_ref[rows, :] + jnp.dot(
                    tokens, w_ref[late * width :, :], preferred_element_type=f32
                )
                scale_ref[rows, :] = jnp.broadcast_to(scale, (size, LANES))
            projected = projected * scale
            raw = projected[:, mixed:] + bias
            step = jnp.maximum(raw, 0.0) + jnp.log1p(jnp.exp(-jnp.abs(raw)))
            logs = pack_pieces(-step * rate, heads)
            sofar = sofar_ref[...]
            summed_logs = jnp.dot(
                tri,
                jnp.concatenate(
                    [logs[b * STRETCH : (b + 1) * STRETCH] for b in range(parts)], axis=1
                ),
                preferred_element_type=f32,
            )
            to_end, whole, earlier = [], [], []
            for b in range(parts):
                cum = unpack_sum(summed_logs[:, b * LANES : (b + 1) * LANES], heads)
                last = cum[STRETCH - 1 : STRETCH, :]
                cum_ref[rows_of(k * parts + b, STRETCH), :] = cum
                to_end.append(step[b * STRETCH : (b + 1) * STRETCH] * jnp.exp(last - cum))
                whole.append(jnp.exp(jnp.broadcast_to(last, (8, LANES))))
                earlier.append(jnp.exp(sofar))
                sofar = sofar + last
            sofar_ref[...] = sofar
            factors = expand(
                jnp.concatenate([step] + to_end + whole + earlier, axis=0), heads, spreader
            )
            ext_ref[8 : 8 + size, :] = projected[:, :mixed].astype(bf16).astype(f32)
            conv = jnp.zeros((size, mixed), f32)
            for tap in range(tap_count):
                first = 9 - tap_count + tap
                conv = conv + taps[tap : tap + 1, :] * ext_ref[first : first + size, :]
            conv = conv * jax.nn.sigmoid(conv)
            ext_ref[0:8, :] = ext_ref[size : size + 8, :]
            x = conv[:, :inner]
            b_all = conv[:, inner : inner + STATE]
            b_ref[rows, :] = b_all.astype(bf16)
            c_ref[rows, :] = conv[:, inner + STATE :].astype(bf16)
            feed_ref[rows, :] = (x * factors[:size]).astype(bf16)
            y_ref[rows, :] = skip * x
            ending = (x * factors[size : 2 * size]).astype(bf16)
            state = state_ref[...]
            for b in range(parts):
                part = slice(b * STRETCH, (b + 1) * STRETCH)
                index = k * parts + b
                fresh = jnp.dot(
                    b_all[part].T.astype(bf16), ending[part], preferred_element_type=f32
                )
                first = 2 * size + 8 * b
                states_ref[index] = state
                sofar_exp_ref[index] = factors[first + 8 * parts : first + 8 * parts + 8]
                state = state * factors[first : first + 1] + fresh
            state_ref[...] = state

        each(0, length // size, project)

    def within(layer, k):
        if layer:
            rows = rows_of(k, ROWS)
            gate = gate_ref[rows, :] + jnp.dot(
                late_tokens(rows), wz_ref[late * width :, :], preferred_element_type=f32
            )
            z_ref[rows, :] = (gate * scale_ref[rows, 0:1]).astype(bf16)

        def block(b):
            rows = rows_of(k * per + b, STRETCH)
            cum = cum_ref[rows, :]
            cum_t = cum.T
            feed = feed_ref[rows, :]
            meet = lax.dot_general(
                c_ref[rows, :], b_ref[rows, :], (((1,), (1,)), ((), ())),
                preferred_element_type=f32,
            )
            for pair in range(heads // 2):
                lanes = slice(pair * 2 * HEAD_DIM, (pair + 1) * 2 * HEAD_DIM)
                weights = []
                for h in (2 * pair, 2 * pair + 1):
                    spread = jnp.where(lower, cum[:, h : h + 1] - cum_t[h : h + 1, :], -jnp.inf)
                    weights.append((meet * jnp.exp(spread)).astype(bf16))
                fed = feed[:, lanes]
                nought = jnp.zeros_like(fed)
                stacked = jnp.concatenate(
                    [jnp.where(left, fed, nought), jnp.where(left, nought, fed)], axis=0
                )
                inside = jnp.dot(
                    jnp.concatenate(weights, axis=1), stacked, preferred_element_type=f32
                )
                y_ref[rows, lanes] = y_ref[rows, lanes] + inside

        each(0, per, block)

    def exchange(layer):
        def end_copy(h, d):
            other = other_of(d)
            return remote(
                end_ref.at[layer, h, other], got_ref.at[layer, h, seq],
                end_send.at[layer, h], end_recv.at[layer, h], (other, own),
            )

        def log_copy(d):
            return remote(
                log_ref.at[layer], logs_ref.at[layer, seq],
                log_send.at[layer], log_recv.at[layer], (other_of(d), own),
            )

        def give_copy(h, d):
            other = other_of(d)
            return remote(
                give_ref.at[layer, h, other], arriving_ref.at[layer, h, seq],
                give_send.at[layer, h], give_recv.at[layer, h], (other, own),
            )

        others = pl.ds(0, count - 1)

        def all_of(block, send, recv):
            return remote(block, block, send, recv, (following, own))

        def all_ends(h):
            block = got_ref.at[layer, h, others]
            return all_of(block, end_send.at[layer, h], end_recv.at[layer, h])

        def all_given(h):
            block = arriving_ref.at[layer, h, others]
            return all_of(block, give_send.at[layer, h], give_recv.at[layer, h])

        all_logs = all_of(logs_ref.at[layer, others], log_send.at[layer], log_recv.at[layer])

        state = state_ref[...]
        log_ref[layer] = sofar_ref[0:1, :]
        for d in range(count):
            for h in range(HALVES):
                first = d * state_rows + h * half_rows
                end_ref[layer, h, d] = state[first : first + half_rows].astype(bf16)
        each(0, count - 1, lambda d: log_copy(d).start())
        for h in range(HALVES):
            each(0, count - 1, lambda d: end_copy(h, d).start())
        first_part = chunks * 3 // 4
        each(0, first_part, lambda k: within(layer, k))
        all_logs.wait_recv()
        logs_ref[layer, seq] = log_ref[layer]
        logs = jnp.concatenate([logs_ref[layer, d] for d in range(count)], axis=0)
        factors = expand(jnp.exp(logs), heads, spreader)
        for h in range(HALVES):
            all_ends(h).wait_recv()
            got_ref[layer, h, seq] = end_ref[layer, h, seq]
            prefix = jnp.zeros((half_rows, inner), f32)
            for d in range(count):
                give_ref[layer, h, d] = prefix.astype(bf16)
                if d + 1 < count:
                    prefix = prefix * factors[d : d + 1] + got_ref[layer, h, d].astype(f32)
            each(0, count - 1, lambda d: give_copy(h, d).start())
        each(first_part, chunks, lambda k: within(layer, k))
        for h in range(HALVES):
            all_given(h).wait_recv()
            arriving_ref[layer, h, seq] = give_ref[layer, h, seq]
        prefix_ref[...] = jnp.concatenate(
            [
                arriving_ref[layer, h, d].astype(f32)
                for d in range(count) for h in range(HALVES)
            ],
            axis=0,
        )
        all_logs.wait_send()
        for h in range(HALVES):
            all_ends(h).wait_send()
            all_given(h).wait_send()

    pair = 2 * HEAD_DIM
    one = iota((2 * pair, pair), 0) % pair // HEAD_DIM
    two = iota((2 * pair, pair), 1) // HEAD_DIM
    averager = jnp.where(one == two, 1.0 / HEAD_DIM, 0.0).astype(bf16)

    def mixed_of(layer, k):
        rows = rows_of(k, ROWS)
        grown = expand(jnp.exp(cum_ref[rows, :]), heads, spreader)
        carried = []
        for block in range(per):
            index = k * per + block
            state = states_ref[index] + prefix_ref[...] * sofar_exp_ref[index][0:1]
            carried.append(
                jnp.dot(
                    c_ref[rows_of(index, STRETCH), :], state.astype(bf16),
                    preferred_element_type=f32,
                )
            )
        gate = z_ref[rows, :].astype(f32)
        ssd = y_ref[rows, :] + jnp.concatenate(carried, axis=0) * grown
        gated = ssd * (gate * jax.nn.sigmoid(gate))
        square = gated * gated
        high = square.astype(bf16)
        low = (square - high.astype(f32)).astype(bf16)
        results = []
        for p in range(inner // pair):
            lanes = slice(p * pair, (p + 1) * pair)
            both = jnp.concatenate([high[:, lanes], low[:, lanes]], axis=1)
            mean = jnp.dot(both, averager, preferred_element_type=f32)
            scaled = gated[:, lanes] * lax.rsqrt(mean + epsilon)
            results.append((scaled * out_gain_ref[layer : layer + 1, lanes]).astype(bf16))
        return jnp.concatenate(results, axis=1)

    def part_of(layer, i):
        if layer == 1:
            rows, slot = rows_of(i, ROWS), i
            lanes, held = (lambda t: lanes_of(t, width)), pl.ds(0, width)
        else:
            if isinstance(i, int):
                rows, j, slot = pl.ds(0, length), i, chunks + i - 1
            else:
                rows, j, slot = rows_of(i[0], ROWS), 0, i[0]
            lanes, held = (lambda t: lanes_of(j * members + t, COLUMNS)), lanes_of(j, COLUMNS)
        nears = [near_ref.at[side, rows, held] for side in range(2)]
        return rows, lanes, nears, (sum_ref.at[rows, held], far_ref.at[rows, held]), slot

    def near_part(layer, side, i):
        rows, lanes, nears, _, slot = part_of(layer, i)
        block = diagonal_id if side == 0 else near_id
        return remote(
            partial_ref.at[rows, lanes(block)], nears[side],
            near_send.at[layer, side], near_recv.at[layer, side, slot], sibling,
        )

    def far_part(layer, i):
        _, _, _, (summing, far), slot = part_of(layer, i)
        return remote(summing, far, far_send.at[layer], far_recv.at[layer, slot], across)

    def send_near(layer, i):
        near_part(layer, 0, i).start()
        near_part(layer, 1, i).start()

    def send_far(layer, i):
        rows, lanes, nears, (summing, _), _ = part_of(layer, i)
        near_part(layer, 0, i).wait_recv()
        summing[...] = (
            partial_ref[rows, lanes(across_id)].astype(f32) + nears[0][...].astype(f32)
        ).astype(bf16)
        far_part(layer, i).start()

    def summed(layer, i, stream):
        rows, lanes, nears, (_, far), _ = part_of(layer, i)
        near_part(layer, 1, i).wait_recv()
        far_part(layer, i).wait_recv()
        return (
            stream.astype(f32)
            + partial_ref[rows, lanes(own)].astype(f32)
            + nears[1][...].astype(f32)
            + far[...].astype(f32)
        ).astype(bf16)

    def drain_sums(layer):
        for side in range(2):
            block = near_ref.at[side]
            remote(
                block, block, near_send.at[layer, side], near_recv.at[layer, side, 0], sibling
            ).wait_send()
        remote(sum_ref, sum_ref, far_send.at[layer], far_recv.at[layer, 0], across).wait_send()

    def plan():
        shift = length.bit_length() - 1
        all_orders().wait_recv()
        orders_ref[seq] = order_ref[...]
        orders = jnp.concatenate([orders_ref[d] for d in range(count)], axis=0)

        def count_up(r):
            first = iota((LANES, length), 0) + r * LANES
            place_ref[rows_of(r, LANES), :] = jnp.where(
                first <= iota((LANES, length), 1), 1.0, 0.0
            ).astype(bf16)

        each(0, length // LANES, count_up)
        device = iota((count, length), 0)
        wanted_here = jnp.right_shift(orders, shift) == seq
        from_each = jnp.right_shift(order_ref[...], shift) == device
        ones = jnp.concatenate(
            [jnp.where(wanted_here, 1.0, 0.0), jnp.where(from_each, 1.0, 0.0)], axis=0
        ).astype(bf16)
        counted = jnp.dot(ones, place_ref[...], preferred_element_type=f32).astype(jnp.int32) - 1
        slot = jnp.where(wanted_here, counted[:count], -1)
        local = jnp.bitwise_and(orders, length - 1)
        short = iota((share, length), 0)
        long = iota((share, length), 1)
        for d in range(count):
            chosen = slot[d : d + 1, :] == short
            found = jnp.where(chosen, local[d : d + 1, :], 0).astype(f32)
            wanted = jnp.sum(found, axis=1, keepdims=True).astype(jnp.int32)
            hand_ref[d * share : (d + 1) * share, :] = jnp.where(
                wanted == long, 1.0, 0.0
            ).astype(bf16)
        target = jnp.where(from_each, counted[count:] + share * device, 0).astype(f32)
        target = jnp.sum(target, axis=0, keepdims=True)
        target = jnp.broadcast_to(target, (LANES, length)).T.astype(jnp.int32)
        for c in range(length // LANES):
            place_ref[:, c * LANES : (c + 1) * LANES] = jnp.where(
                target == iota((length, LANES), 1) + c * LANES, 1.0, 0.0
            ).astype(bf16)

    def move_copy(j, d):
        other = other_of(d)
        return remote(
            leaving_ref.at[j, rows_of(other, share)], arrived_ref.at[j, rows_of(seq, share)],
            move_send, move_recv.at[j], (other, own),
        )

    def all_moves(j):
        others = arrived_ref.at[j, pl.ds(0, length - share)]
        return remote(others, others, move_send, move_recv.at[j], (following, own))

    def hand_over(j):
        if j:
            held = summed(0, j, full_ref[j, :, own_lanes])
        else:

            def first(k):
                rows = rows_of(k, ROWS)
                held_ref[rows, :] = summed(0, (k,), full_ref[0, rows, own_lanes])

            each(0, chunks, first)
            held = held_ref[...]
        leaving_ref[j] = jnp.dot(hand_ref[...], held, preferred_element_type=f32).astype(bf16)
        each(0, count - 1, lambda d: move_copy(j, d).start())
        arrived_ref[j, rows_of(seq, share), :] = leaving_ref[j, rows_of(seq, share), :]

    def put(j):
        lanes = slice(j * COLUMNS, (j + 1) * COLUMNS)
        all_moves(j).wait_recv()
        rows = jnp.dot(place_ref[...], arrived_ref[j], preferred_element_type=f32).astype(bf16)
        tail_ref[:, lanes] = rows[length - HALO :]
        full_ref[j, :, own_lanes] = rows
        for t in range(members):
            halo_piece(j, t).start()
        if j < late:
            send_block(1, j)
        else:
            each(0, early, lambda k: send_part(j, k))
        if j == last_piece:
            each(early, chunks, lambda k: send_block(1, (k,)))
        own_ref[:, lanes] = rows

    def accumulate(j):
        part = slice(j * width, (j + 1) * width)

        def product(k):
            rows = rows_of(k, ROWS)
            result = jnp.dot(
                full_ref[j, rows, :], w_ref[part, :], preferred_element_type=f32
            )
            acc_ref[rows, :] = result if j == 0 else acc_ref[rows, :] + result
            gate = jnp.dot(full_ref[j, rows, :], wz_ref[part, :], preferred_element_type=f32)
            gate_ref[rows, :] = gate if j == 0 else gate_ref[rows, :] + gate
            square = jnp.broadcast_to(squares_of(full_ref[j, rows, :]), (ROWS, LANES))
            scale_ref[rows, :] = square if j == 0 else scale_ref[rows, :] + square

        each(0, chunks, product)

    load_bc(0).wait()
    for t in range(members):
        prepare(0, t)
    load_bc(1).start()
    own_columns = full_ref.at[:, :, own_lanes]
    pltpu.make_async_copy(own_columns, own_columns, self_sem).wait()

    def arrive_first(k):
        forward_block(0, k)
        rest_of_block(0, k)

    scan(0, arrive_first)
    exchange(0)
    drain_gather(0)
    pltpu.make_async_copy(w_out_ref.at[0], wo_col_ref, wo_sem.at[0]).wait()
    pltpu.make_async_copy(w_out_ref.at[1], wo_ref, wo_sem.at[1]).wait()

    def product_of(k, j):
        rows, lanes = rows_of(k, ROWS), lanes_of(j, members * COLUMNS)
        partial_ref[rows, lanes] = jnp.dot(
            mixed_ref[rows, :], wo_col_ref[:, lanes], preferred_element_type=f32
        ).astype(bf16)

    def mix(k):
        mixed_ref[rows_of(k, ROWS), :] = mixed_of(0, k)
        product_of(k, 0)
        send_near(0, (k,))

        @pl.when(k > 0)
        def _():
            send_far(0, (k - 1,))

    each(0, chunks, mix)
    for j in range(1, pieces):
        each(0, chunks, lambda k: product_of(k, j))
        send_near(0, j)
        send_far(0, j - 1 if j > 1 else (chunks - 1,))
    send_far(0, pieces - 1)
    plan()
    load_bc(1).wait()

    for j in range(pieces):
        hand_over(j)
        if j > 1:
            put(j - 2)
        prepare(1, j)
    put(pieces - 2)
    forward_block(1, 0)
    rest_of_block(1, 0)
    accumulate(0)
    put(pieces - 1)
    drain_sums(0)

    for j in range(1, late):
        forward_block(1, j)
        rest_of_block(1, j)
        accumulate(j)

    forward_block(1, (0,))

    def arrive_second(k):
        @pl.when(k + 1 < chunks)
        def _():
            forward_block(1, (k + 1,))

        rest_of_block(1, (k,))

    scan(1, arrive_second)
    exchange(1)

    def output_rows(k):
        rows = rows_of(k, ROWS)
        mixed_heads = mixed_of(1, k)
        for side, block in enumerate((diagonal_id, near_id, across_id, own)):
            lanes = lanes_of(block, width)
            partial_ref[rows, lanes] = jnp.dot(
                mixed_heads, wo_ref[:, lanes], preferred_element_type=f32
            ).astype(bf16)
            if side < 2:
                near_part(1, side, k).start()
        send_far(1, k)

    each(0, chunks, output_rows)

    def out_copy(k):
        rows = rows_of(k, ROWS)
        return pltpu.make_async_copy(own_ref.at[rows], out_ref.at[rows], out_sem.at[k])

    def finish(k):
        rows = rows_of(k, ROWS)
        own_ref[rows, :] = summed(1, k, own_ref[rows, :])
        out_copy(k).start()

    each(0, chunks, finish)
    drain_gather(1)
    drain_sums(1)
    for layer in range(2):
        block = halo_ref.at[layer]
        remote(
            block, block, halo_send.at[layer], halo_recv.at[layer, 0], (following, own)
        ).wait_send()
    all_orders().wait_send()
    others = arrived_ref.at[:, pl.ds(0, length - share)]
    remote(others, others, move_send, move_recv.at[0], (following, own)).wait_send()
    each(0, chunks, lambda k: out_copy(k).wait())


def body(
    tokens, col_order, in_gain, w_in, w_bc, w_dt, conv_x, conv_bc,
    dt_bias, a_log, d_skip, out_gain, w_out,
):
    count, members = lax.axis_size("seq"), lax.axis_size("tp")
    length, width = tokens.shape
    inner = w_out.shape[1]
    heads = inner // HEAD_DIM
    mixed = inner + 2 * STATE
    depth = w_in.shape[1]
    chunks, fines = length // ROWS, length // FINE
    blocks = length // STRETCH
    pieces = width // COLUMNS
    state_rows = STATE // count
    half_rows = state_rows // HALVES
    vmem = pl.BlockSpec(memory_space=pltpu.VMEM)
    hbm = pl.BlockSpec(memory_space=pltpu.HBM)
    dma = pltpu.SemaphoreType.DMA
    return pl.pallas_call(
        functools.partial(layers_kernel, count, members),
        in_specs=[hbm, vmem, vmem, hbm, hbm] + [vmem] * 7 + [hbm],
        out_specs=hbm,
        out_shape=jax.ShapeDtypeStruct(tokens.shape, bf16),
        scratch_shapes=[
            pltpu.VMEM((pieces, length, members * COLUMNS), bf16),
            pltpu.VMEM((HALO, width), bf16),
            pltpu.VMEM((2, members, HALO, width), bf16),
            pltpu.VMEM((count, 1, length), jnp.int32),
            pltpu.VMEM((2, width, 2, inner), bf16),
            pltpu.VMEM((depth, 2 * STATE), bf16),
            pltpu.VMEM((depth, mixed + LANES), bf16),
            pltpu.VMEM((depth, inner), bf16),
            pltpu.VMEM((inner, depth), bf16),
            pltpu.VMEM((inner, depth), bf16),
            pltpu.VMEM((ROWS + 8, mixed), f32),
            pltpu.VMEM((length, inner), f32),
            pltpu.VMEM((length, inner), bf16),
            pltpu.VMEM((length, inner), bf16),
            pltpu.VMEM((length, STATE), bf16),
            pltpu.VMEM((length, STATE), bf16),
            pltpu.VMEM((length, LANES), f32),
            pltpu.VMEM((length, LANES), f32),
            pltpu.VMEM((blocks, STATE, inner), f32),
            pltpu.VMEM((blocks, 8, inner), f32),
            pltpu.VMEM((STATE, inner), f32),
            pltpu.VMEM((8, LANES), f32),
            pltpu.VMEM((2, HALVES, count, half_rows, inner), bf16),
            pltpu.VMEM((2, 1, LANES), f32),
            pltpu.VMEM((2, HALVES, count, half_rows, inner), bf16),
            pltpu.VMEM((2, count, 1, LANES), f32),
            pltpu.VMEM((2, HALVES, count, half_rows, inner), bf16),
            pltpu.VMEM((2, HALVES, count, half_rows, inner), bf16),
            pltpu.VMEM((STATE, inner), f32),
            pltpu.VMEM((length, depth), bf16),
            pltpu.VMEM((2, length, width), bf16),
            pltpu.VMEM((length, width), bf16),
            pltpu.VMEM((length, width), bf16),
            pltpu.VMEM((length, inner), bf16),
            pltpu.VMEM((length, length), bf16),
            pltpu.VMEM((length, length), bf16),
            pltpu.VMEM((pieces, length, COLUMNS), bf16),
            pltpu.VMEM((pieces, length, COLUMNS), bf16),
            pltpu.VMEM((length, COLUMNS), bf16),
            pltpu.VMEM((length, mixed + LANES), f32),
            pltpu.VMEM((length, inner), f32),
            pltpu.VMEM((length, width), bf16),
            dma((3,)), dma((2,)), dma,
            dma((2, 3)), dma((3, fines + chunks + pieces - 2)),
            dma((2,)), dma((2, members)), dma, dma,
            dma((2, HALVES)), dma((2, HALVES)), dma((2,)), dma((2,)),
            dma((2, HALVES)), dma((2, HALVES)),
            dma((2, 2)), dma((2, 2, chunks + pieces - 1)),
            dma((2,)), dma((2, chunks + pieces - 1)),
            dma, dma((pieces,)), dma((chunks,)),
        ],
        compiler_params=pltpu.CompilerParams(
            collective_id=0, has_side_effects=True, vmem_limit_bytes=63 * 1024 * 1024
        ),
        name="mixer_layers",
    )(
        tokens, col_order[None], in_gain, w_in, w_bc, jnp.swapaxes(w_dt, 1, 2), conv_x, conv_bc,
        dt_bias, a_log, d_skip, out_gain, w_out,
    )


def solution(mesh):
    placed = (
        P("seq", "tp"),
        P("seq"),
        P(),
        P(None, None, None, "tp"),
        P(),
        P(None, None, "tp"),
        P(None, None, "tp"),
        P(),
        P(None, "tp"),
        P(None, "tp"),
        P(None, "tp"),
        P(None, "tp"),
        P(None, "tp", None),
    )
    return jax.shard_map(
        body, mesh=mesh, in_specs=placed, out_specs=P("seq", "tp"), check_vma=False
    )
```

```python
import functools

import jax
import jax.numpy as jnp
from jax import lax
from jax.experimental import pallas as pl
from jax.experimental.pallas import tpu as pltpu
from jax.sharding import PartitionSpec as P

HEAD_DIM = 64
STATE = 128
STRETCH = 128
LANES = 128
HALO = 16
ROWS = 256
FINE = 128
HALVES = 2
SMALLS = 9
COLUMNS = 128

epsilon = 1e-05
f32 = jnp.float32
bf16 = jnp.bfloat16
MESH = pl.DeviceIdType.MESH


def iota(shape, axis):
    return lax.broadcasted_iota(jnp.int32, shape, axis)


def spreader_of(heads, inner):
    row = iota((LANES, inner), 0)
    channel = iota((LANES, inner), 1)
    chosen = (row % heads == channel // HEAD_DIM) & (row < 3 * heads)
    return jnp.where(chosen, 1.0, 0.0).astype(bf16)


def pack_pieces(values, heads):
    values = jnp.where(iota(values.shape, 1) < heads, values, 0.0)
    high = values.astype(bf16).astype(f32)
    rest = values - high
    middle = rest.astype(bf16).astype(f32)
    low = rest - middle
    packed = high + pltpu.roll(middle, heads, 1) + pltpu.roll(low, 2 * heads, 1)
    return packed.astype(bf16)


def expand(values, heads, spreader):
    return jnp.dot(pack_pieces(values, heads), spreader, preferred_element_type=f32)


def unpack_sum(pieces, heads):
    total = (
        pieces
        + pltpu.roll(pieces, LANES - heads, 1)
        + pltpu.roll(pieces, LANES - 2 * heads, 1)
    )
    return jnp.where(iota(total.shape, 1) < heads, total, 0.0)


def rows_of(k, size):
    return pl.ds(pl.multiple_of(k * size, size), size)


def lanes_of(k, size):
    return pl.ds(pl.multiple_of(k * size, LANES), size)


def pad_row(row):
    return jnp.concatenate([row, jnp.zeros((1, LANES - row.shape[1]), f32)], axis=1)


def layers_kernel(
    count, members,
    stream_ref, w_in_ref, w_bc_ref, w_out_ref, *refs,
):
    smalls = refs[:SMALLS]
    (
        out_ref, order_ref, in_gain_ref, w_dt_ref, conv_x_ref, conv_bc_ref,
        bias_ref, a_log_ref, d_skip_ref, out_gain_ref,
        full_ref, tail_ref, halo_ref, orders_ref, raw_ref, raw_bc_ref, w_ref, wz_ref, wo_col_ref, wo_ref,
        ext_ref, y_ref, z_ref, feed_ref, b_ref, c_ref, cum_ref, scale_ref, states_ref, sofar_exp_ref,
        state_ref, sofar_ref,
        end_ref, log_ref, got_ref, logs_ref, give_ref, arriving_ref, prefix_ref,
        partial_ref, near_ref, sum_ref, far_ref,
        mixed_ref, hand_ref, place_ref, leaving_ref, arrived_ref, held_ref, acc_ref, gate_ref, own_ref,
        load_sem, wo_sem, self_sem, ag_send, ag_recv, halo_send, halo_recv, order_send, order_recv,
        end_send, end_recv, log_send, log_recv, give_send, give_recv,
        near_send, near_recv, far_send, far_recv, move_send, move_recv, out_sem,
        small_sem,
    ) = refs[SMALLS:]
    seq = lax.axis_index("seq")
    own = lax.axis_index("tp")
    chip, core = own // 2, own % 2
    near_id = chip * 2 + 1 - core
    across_id = (1 - chip) * 2 + core
    diagonal_id = (1 - chip) * 2 + 1 - core
    sibling = (seq, near_id)
    across = (seq, across_id)
    length, width = stream_ref.shape
    depth = w_ref.shape[0]
    inner = y_ref.shape[1]
    mixed = inner + 2 * STATE
    heads = inner // HEAD_DIM
    chunks = length // ROWS
    fines = length // FINE
    per = ROWS // STRETCH
    blocks = length // STRETCH
    pieces = width // COLUMNS
    share = length // count
    state_rows = STATE // count
    half_rows = state_rows // HALVES
    following = (seq + 1) % count
    before = (seq + count - 1) % count

    def remote(src, dst, send, recv, device):
        return pltpu.make_async_remote_copy(
            src_ref=src, dst_ref=dst, send_sem=send, recv_sem=recv,
            device_id=device, device_id_type=MESH,
        )

    def other_of(i):
        low = seq < count // 2
        other = jnp.where(low, count - 1 - i, i)
        return jnp.where(low, other - (other <= seq), other + (other >= seq))

    def each(first, last, act):
        def step(i, _):
            act(i)
            return 0

        lax.fori_loop(first, last, step, 0)

    greeted = [(other_of(d), own) for d in range(count - 1)]
    greeted += [(before, t) for t in range(members)]
    greeted += [across, sibling]
    barrier = pltpu.get_barrier_semaphore()
    for device in greeted:
        pl.semaphore_signal(barrier, inc=1, device_id=device, device_id_type=MESH)

    kept = (
        order_ref, in_gain_ref, w_dt_ref, conv_x_ref, conv_bc_ref,
        bias_ref, a_log_ref, d_skip_ref, out_gain_ref,
    )
    small_loads = [
        pltpu.make_async_copy(small, keep, small_sem.at[i])
        for i, (small, keep) in enumerate(zip(smalls, kept))
    ]

    def load_in(layer, t):
        return pltpu.make_async_copy(
            w_in_ref.at[layer, t * width : (t + 1) * width], raw_ref.at[t % 2], load_sem.at[t % 2]
        )

    def load_bc(layer):
        return pltpu.make_async_copy(w_bc_ref.at[layer], raw_bc_ref, load_sem.at[2])

    own_lanes = lanes_of(own, COLUMNS)
    self_loads, wo_loads = [], []
    for j in range(pieces):
        self_loads.append(
            pltpu.make_async_copy(
                stream_ref.at[:, j * COLUMNS : (j + 1) * COLUMNS],
                full_ref.at[j, :, own_lanes], self_sem,
            )
        )
        for t in range(members):
            first = t * width + j * COLUMNS
            place = j * members + t
            wo_loads.append(
                pltpu.make_async_copy(
                    w_out_ref.at[0, :, first : first + COLUMNS],
                    wo_col_ref.at[:, place * COLUMNS : (place + 1) * COLUMNS],
                    wo_sem.at[0],
                )
            )
    wo_loads.append(pltpu.make_async_copy(w_out_ref.at[1], wo_ref, wo_sem.at[1]))
    for copy in small_loads + [load_in(0, 0), load_bc(0), load_in(0, 1)] + self_loads + wo_loads:
        copy.start()

    pl.semaphore_wait(barrier, len(greeted))

    last_piece = pieces - 1
    early = chunks // 2
    late = pieces - 2

    def block_of(layer, i, owner):
        lanes = lanes_of(owner, COLUMNS)
        if layer == 0:
            return full_ref.at[:, rows_of(i, FINE), lanes], i
        if isinstance(i, int):
            return full_ref.at[i, :, lanes], fines + i
        slot = fines + late + i[0]
        return full_ref.at[pl.ds(late, pieces - late), rows_of(i[0], ROWS), lanes], slot

    def send_part(j, k):
        part = full_ref.at[j, rows_of(k, ROWS), own_lanes]
        slot = fines + late + k
        for kind, device in ((0, across), (1, sibling)):
            remote(part, part, ag_send.at[1, kind], ag_recv.at[kind, slot], device).start()

    def gather_copy(layer, kind, i, owner):
        block, slot = block_of(layer, i, owner)
        return remote(
            block, block, ag_send.at[layer, kind], ag_recv.at[kind, slot],
            across if kind == 0 else sibling,
        )

    def send_rows(k):
        rows = rows_of(k, FINE)
        for kind, device in ((0, across), (1, sibling)):
            for j in range(pieces):
                remote(
                    stream_ref.at[rows, lanes_of(j, COLUMNS)], full_ref.at[j, rows, own_lanes],
                    ag_send.at[0, kind], ag_recv.at[kind, k], device,
                ).start()

    def send_block(layer, i):
        gather_copy(layer, 0, i, own).start()
        gather_copy(layer, 1, i, own).start()

    def forward_block(layer, i):
        gather_copy(layer, 0, i, across_id).wait_recv()
        gather_copy(layer, 2, i, across_id).start()

    def rest_of_block(layer, i):
        gather_copy(layer, 1, i, near_id).wait_recv()
        gather_copy(layer, 2, i, diagonal_id).wait_recv()

    def drain_gather(layer):
        for kind, owner in ((0, own), (1, own), (2, across_id)):
            block = full_ref.at[:, :, lanes_of(owner, COLUMNS)]
            remote(block, block, ag_send.at[layer, kind], ag_recv.at[kind, 0], sibling).wait_send()

    def halo_copy(layer, t, source):
        tail = tail_ref if layer else stream_ref.at[pl.ds(length - HALO, HALO)]
        return remote(
            tail, halo_ref.at[layer, source],
            halo_send.at[layer], halo_recv.at[layer, source], (following, t),
        )

    def halo_piece(j, t):
        lanes = lanes_of(j, COLUMNS)
        return remote(
            tail_ref.at[:, lanes], halo_ref.at[1, own, :, lanes],
            halo_send.at[1], halo_recv.at[1, own], (following, t),
        )

    def order_copy(d):
        return remote(
            order_ref, orders_ref.at[seq], order_send, order_recv, (other_of(d), own)
        )

    def all_orders():
        others = orders_ref.at[pl.ds(0, count - 1)]
        return remote(others, others, order_send, order_recv, (following, own))

    for t in range(members):
        halo_copy(0, t, own).start()

    each(0, fines, send_rows)
    for copy in small_loads:
        copy.wait()
    each(0, count - 1, lambda d: order_copy(d).start())

    row = iota((2 * LANES, 2 * LANES), 0)
    col = iota((2 * LANES, 2 * LANES), 1)
    apart = jnp.where(col == 2 * (row % LANES) + row // LANES, 1.0, 0.0).astype(bf16)

    def prepare(layer, t):
        load_in(layer, t).wait()

        def block(j):
            i = t * pieces + j
            rows = rows_of(i, LANES)
            to = rows_of(j * members + t, LANES)
            gain = in_gain_ref[layer : layer + 1, lanes_of(i, LANES)]
            gain = jnp.broadcast_to(gain, (LANES, LANES)).T
            both = raw_ref[t % 2, rows_of(j, LANES)].reshape(2 * LANES, inner)
            halves = jnp.dot(apart, both, preferred_element_type=f32)
            for p in range(inner // LANES):
                lanes = slice(p * LANES, (p + 1) * LANES)
                w_ref[to, lanes] = (halves[:LANES, lanes] * gain).astype(bf16)
                wz_ref[to, lanes] = (halves[LANES:, lanes] * gain).astype(bf16)
            for p in range(2 * STATE // LANES):
                lanes = slice(p * LANES, (p + 1) * LANES)
                w_ref[to, inner + p * LANES : inner + (p + 1) * LANES] = (
                    raw_bc_ref[rows, lanes].astype(f32) * gain
                ).astype(bf16)
            dt = w_dt_ref[layer, :, lanes_of(i, LANES)].astype(f32)
            dt = jnp.concatenate([dt, jnp.zeros((LANES - heads, LANES), f32)], axis=0)
            w_ref[to, mixed:] = (dt.T * gain).astype(bf16)

        each(0, pieces, block)
        if t + 2 < members:
            load_in(layer, t + 2).start()
        elif layer == 0:
            load_in(1, t + 2 - members).start()

    spreader = spreader_of(heads, inner)
    line = iota((STRETCH, STRETCH), 0)
    lane = iota((STRETCH, STRETCH), 1)
    lower = line >= lane
    tri = jnp.where(lower, 1.0, 0.0).astype(bf16)
    left = iota((STRETCH, 2 * HEAD_DIM), 1) < HEAD_DIM

    def late_tokens(rows):
        return jnp.concatenate([full_ref[j, rows, :] for j in range(late, pieces)], axis=1)

    def squares_of(v):
        wide = v.astype(f32)
        return jnp.sum(wide * wide, axis=-1, keepdims=True)

    def scale_of(v):
        return lax.rsqrt(squares_of(v) / depth + epsilon)

    def scan(layer, arrive):
        for t in range(members):
            halo_copy(layer, t, t).wait_recv()
        ahead = jnp.concatenate(
            [
                halo_ref[layer, t, :, j * COLUMNS : (j + 1) * COLUMNS]
                for j in range(pieces) for t in range(members)
            ],
            axis=1,
        )
        ahead = jnp.dot(ahead, w_ref[:, :mixed], preferred_element_type=f32) * scale_of(ahead)
        ahead = ahead[HALO - 8 :, :].astype(bf16).astype(f32)
        ext_ref[0:8, :] = jnp.where(seq > 0, ahead, 0.0)
        state_ref[...] = jnp.zeros_like(state_ref)
        sofar_ref[...] = jnp.zeros_like(sofar_ref)
        bias = pad_row(bias_ref[layer : layer + 1, :])
        rate = pad_row(jnp.exp(a_log_ref[layer : layer + 1, :]))
        skip = pad_row(d_skip_ref[layer : layer + 1, :])
        skip = expand(jnp.broadcast_to(skip, (8, LANES)), heads, spreader)[0:1]
        taps = jnp.concatenate([conv_x_ref[layer], conv_bc_ref[layer]], axis=1)
        tap_count = taps.shape[0]

        size = ROWS if layer else FINE
        parts = size // STRETCH

        def project(k):
            rows = rows_of(k, size)
            arrive(k)
            if layer == 0:
                tokens = jnp.concatenate([full_ref[j, rows, :] for j in range(pieces)], axis=1)
                scale = scale_of(tokens)
                projected = jnp.dot(tokens, w_ref[...], preferred_element_type=f32)
                gate = jnp.dot(tokens, wz_ref[...], preferred_element_type=f32)
                z_ref[rows, :] = (gate * scale).astype(bf16)
            else:
                tokens = late_tokens(rows)
                square = scale_ref[rows, 0:1] + squares_of(tokens)
                scale = lax.rsqrt(square / depth + epsilon)
                projected = acc_ref[rows, :] + jnp.dot(
                    tokens, w_ref[late * width :, :], preferred_element_type=f32
                )
                scale_ref[rows, :] = jnp.broadcast_to(scale, (size, LANES))
            projected = projected * scale
            raw = projected[:, mixed:] + bias
            step = jnp.maximum(raw, 0.0) + jnp.log1p(jnp.exp(-jnp.abs(raw)))
            logs = pack_pieces(-step * rate, heads)
            sofar = sofar_ref[...]
            summed_logs = jnp.dot(
                tri,
                jnp.concatenate(
                    [logs[b * STRETCH : (b + 1) * STRETCH] for b in range(parts)], axis=1
                ),
                preferred_element_type=f32,
            )
            to_end, whole, earlier = [], [], []
            for b in range(parts):
                cum = unpack_sum(summed_logs[:, b * LANES : (b + 1) * LANES], heads)
                last = cum[STRETCH - 1 : STRETCH, :]
                cum_ref[rows_of(k * parts + b, STRETCH), :] = cum
                to_end.append(step[b * STRETCH : (b + 1) * STRETCH] * jnp.exp(last - cum))
                whole.append(jnp.exp(jnp.broadcast_to(last, (8, LANES))))
                earlier.append(jnp.exp(sofar))
                sofar = sofar + last
            sofar_ref[...] = sofar
            factors = expand(
                jnp.concatenate([step] + to_end + whole + earlier, axis=0), heads, spreader
            )
            ext_ref[8 : 8 + size, :] = projected[:, :mixed].astype(bf16).astype(f32)
            conv = jnp.zeros((size, mixed), f32)
            for tap in range(tap_count):
                first = 9 - tap_count + tap
                conv = conv + taps[tap : tap + 1, :] * ext_ref[first : first + size, :]
            conv = conv * jax.nn.sigmoid(conv)
            ext_ref[0:8, :] = ext_ref[size : size + 8, :]
            x = conv[:, :inner]
            b_all = conv[:, inner : inner + STATE]
            b_ref[rows, :] = b_all.astype(bf16)
            c_ref[rows, :] = conv[:, inner + STATE :].astype(bf16)
            feed_ref[rows, :] = (x * factors[:size]).astype(bf16)
            y_ref[rows, :] = skip * x
            ending = (x * factors[size : 2 * size]).astype(bf16)
            state = state_ref[...]
            for b in range(parts):
                part = slice(b * STRETCH, (b + 1) * STRETCH)
                index = k * parts + b
                fresh = jnp.dot(
                    b_all[part].T.astype(bf16), ending[part], preferred_element_type=f32
                )
                first = 2 * size + 8 * b
                states_ref[index] = state
                sofar_exp_ref[index] = factors[first + 8 * parts : first + 8 * parts + 8]
                state = state * factors[first : first + 1] + fresh
            state_ref[...] = state

        each(0, length // size, project)

    def within(layer, k):
        if layer:
            rows = rows_of(k, ROWS)
            gate = gate_ref[rows, :] + jnp.dot(
                late_tokens(rows), wz_ref[late * width :, :], preferred_element_type=f32
            )
            z_ref[rows, :] = (gate * scale_ref[rows, 0:1]).astype(bf16)

        def block(b):
            rows = rows_of(k * per + b, STRETCH)
            cum = cum_ref[rows, :]
            cum_t = cum.T
            feed = feed_ref[rows, :]
            meet = lax.dot_general(
                c_ref[rows, :], b_ref[rows, :], (((1,), (1,)), ((), ())),
                preferred_element_type=f32,
            )
            for pair in range(heads // 2):
                lanes = slice(pair * 2 * HEAD_DIM, (pair + 1) * 2 * HEAD_DIM)
                weights = []
                for h in (2 * pair, 2 * pair + 1):
                    spread = jnp.where(lower, cum[:, h : h + 1] - cum_t[h : h + 1, :], -jnp.inf)
                    weights.append((meet * jnp.exp(spread)).astype(bf16))
                fed = feed[:, lanes]
                nought = jnp.zeros_like(fed)
                stacked = jnp.concatenate(
                    [jnp.where(left, fed, nought), jnp.where(left, nought, fed)], axis=0
                )
                inside = jnp.dot(
                    jnp.concatenate(weights, axis=1), stacked, preferred_element_type=f32
                )
                y_ref[rows, lanes] = y_ref[rows, lanes] + inside

        each(0, per, block)

    def exchange(layer):
        def end_copy(h, d):
            other = other_of(d)
            return remote(
                end_ref.at[layer, h, other], got_ref.at[layer, h, seq],
                end_send.at[layer, h], end_recv.at[layer, h], (other, own),
            )

        def log_copy(d):
            return remote(
                log_ref.at[layer], logs_ref.at[layer, seq],
                log_send.at[layer], log_recv.at[layer], (other_of(d), own),
            )

        def give_copy(h, d):
            other = other_of(d)
            return remote(
                give_ref.at[layer, h, other], arriving_ref.at[layer, h, seq],
                give_send.at[layer, h], give_recv.at[layer, h], (other, own),
            )

        others = pl.ds(0, count - 1)

        def all_of(block, send, recv):
            return remote(block, block, send, recv, (following, own))

        def all_ends(h):
            block = got_ref.at[layer, h, others]
            return all_of(block, end_send.at[layer, h], end_recv.at[layer, h])

        def all_given(h):
            block = arriving_ref.at[layer, h, others]
            return all_of(block, give_send.at[layer, h], give_recv.at[layer, h])

        all_logs = all_of(logs_ref.at[layer, others], log_send.at[layer], log_recv.at[layer])

        state = state_ref[...]
        log_ref[layer] = sofar_ref[0:1, :]
        for d in range(count):
            for h in range(HALVES):
                first = d * state_rows + h * half_rows
                end_ref[layer, h, d] = state[first : first + half_rows].astype(bf16)
        each(0, count - 1, lambda d: log_copy(d).start())
        for h in range(HALVES):
            each(0, count - 1, lambda d: end_copy(h, d).start())
        first_part = chunks * 3 // 4
        each(0, first_part, lambda k: within(layer, k))
        all_logs.wait_recv()
        logs_ref[layer, seq] = log_ref[layer]
        logs = jnp.concatenate([logs_ref[layer, d] for d in range(count)], axis=0)
        factors = expand(jnp.exp(logs), heads, spreader)
        for h in range(HALVES):
            all_ends(h).wait_recv()
            got_ref[layer, h, seq] = end_ref[layer, h, seq]
            prefix = jnp.zeros((half_rows, inner), f32)
            for d in range(count):
                give_ref[layer, h, d] = prefix.astype(bf16)
                if d + 1 < count:
                    prefix = prefix * factors[d : d + 1] + got_ref[layer, h, d].astype(f32)
            each(0, count - 1, lambda d: give_copy(h, d).start())
        each(first_part, chunks, lambda k: within(layer, k))
        for h in range(HALVES):
            all_given(h).wait_recv()
            arriving_ref[layer, h, seq] = give_ref[layer, h, seq]
        prefix_ref[...] = jnp.concatenate(
            [
                arriving_ref[layer, h, d].astype(f32)
                for d in range(count) for h in range(HALVES)
            ],
            axis=0,
        )
        all_logs.wait_send()
        for h in range(HALVES):
            all_ends(h).wait_send()
            all_given(h).wait_send()

    pair = 2 * HEAD_DIM
    one = iota((2 * pair, pair), 0) % pair // HEAD_DIM
    two = iota((2 * pair, pair), 1) // HEAD_DIM
    averager = jnp.where(one == two, 1.0 / HEAD_DIM, 0.0).astype(bf16)

    def mixed_of(layer, k):
        rows = rows_of(k, ROWS)
        grown = expand(jnp.exp(cum_ref[rows, :]), heads, spreader)
        carried = []
        for block in range(per):
            index = k * per + block
            state = states_ref[index] + prefix_ref[...] * sofar_exp_ref[index][0:1]
            carried.append(
                jnp.dot(
                    c_ref[rows_of(index, STRETCH), :], state.astype(bf16),
                    preferred_element_type=f32,
                )
            )
        gate = z_ref[rows, :].astype(f32)
        ssd = y_ref[rows, :] + jnp.concatenate(carried, axis=0) * grown
        gated = ssd * (gate * jax.nn.sigmoid(gate))
        square = gated * gated
        high = square.astype(bf16)
        low = (square - high.astype(f32)).astype(bf16)
        results = []
        for p in range(inner // pair):
            lanes = slice(p * pair, (p + 1) * pair)
            both = jnp.concatenate([high[:, lanes], low[:, lanes]], axis=1)
            mean = jnp.dot(both, averager, preferred_element_type=f32)
            scaled = gated[:, lanes] * lax.rsqrt(mean + epsilon)
            results.append((scaled * out_gain_ref[layer : layer + 1, lanes]).astype(bf16))
        return jnp.concatenate(results, axis=1)

    def part_of(layer, i):
        if layer == 1:
            rows, slot = rows_of(i, ROWS), i
            lanes, held = (lambda t: lanes_of(t, width)), pl.ds(0, width)
        else:
            if isinstance(i, int):
                rows, j, slot = pl.ds(0, length), i, chunks + i - 1
            else:
                rows, j, slot = rows_of(i[0], ROWS), 0, i[0]
            lanes, held = (lambda t: lanes_of(j * members + t, COLUMNS)), lanes_of(j, COLUMNS)
        nears = [near_ref.at[side, rows, held] for side in range(2)]
        return rows, lanes, nears, (sum_ref.at[rows, held], far_ref.at[rows, held]), slot

    def near_part(layer, side, i):
        rows, lanes, nears, _, slot = part_of(layer, i)
        block = diagonal_id if side == 0 else near_id
        return remote(
            partial_ref.at[rows, lanes(block)], nears[side],
            near_send.at[layer, side], near_recv.at[layer, side, slot], sibling,
        )

    def far_part(layer, i):
        _, _, _, (summing, far), slot = part_of(layer, i)
        return remote(summing, far, far_send.at[layer], far_recv.at[layer, slot], across)

    def send_near(layer, i):
        near_part(layer, 0, i).start()
        near_part(layer, 1, i).start()

    def send_far(layer, i):
        rows, lanes, nears, (summing, _), _ = part_of(layer, i)
        near_part(layer, 0, i).wait_recv()
        summing[...] = (
            partial_ref[rows, lanes(across_id)].astype(f32) + nears[0][...].astype(f32)
        ).astype(bf16)
        far_part(layer, i).start()

    def summed(layer, i, stream):
        rows, lanes, nears, (_, far), _ = part_of(layer, i)
        near_part(layer, 1, i).wait_recv()
        far_part(layer, i).wait_recv()
        return (
            stream.astype(f32)
            + partial_ref[rows, lanes(own)].astype(f32)
            + nears[1][...].astype(f32)
            + far[...].astype(f32)
        ).astype(bf16)

    def drain_sums(layer):
        for side in range(2):
            block = near_ref.at[side]
            remote(
                block, block, near_send.at[layer, side], near_recv.at[layer, side, 0], sibling
            ).wait_send()
        remote(sum_ref, sum_ref, far_send.at[layer], far_recv.at[layer, 0], across).wait_send()

    def plan():
        shift = length.bit_length() - 1
        all_orders().wait_recv()
        orders_ref[seq] = order_ref[...]
        orders = jnp.concatenate([orders_ref[d] for d in range(count)], axis=0)

        def count_up(r):
            first = iota((LANES, length), 0) + r * LANES
            place_ref[rows_of(r, LANES), :] = jnp.where(
                first <= iota((LANES, length), 1), 1.0, 0.0
            ).astype(bf16)

        each(0, length // LANES, count_up)
        device = iota((count, length), 0)
        wanted_here = jnp.right_shift(orders, shift) == seq
        from_each = jnp.right_shift(order_ref[...], shift) == device
        ones = jnp.concatenate(
            [jnp.where(wanted_here, 1.0, 0.0), jnp.where(from_each, 1.0, 0.0)], axis=0
        ).astype(bf16)
        counted = jnp.dot(ones, place_ref[...], preferred_element_type=f32).astype(jnp.int32) - 1
        slot = jnp.where(wanted_here, counted[:count], -1)
        local = jnp.bitwise_and(orders, length - 1)
        short = iota((share, length), 0)
        long = iota((share, length), 1)
        for d in range(count):
            chosen = slot[d : d + 1, :] == short
            found = jnp.where(chosen, local[d : d + 1, :], 0).astype(f32)
            wanted = jnp.sum(found, axis=1, keepdims=True).astype(jnp.int32)
            hand_ref[d * share : (d + 1) * share, :] = jnp.where(
                wanted == long, 1.0, 0.0
            ).astype(bf16)
        target = jnp.where(from_each, counted[count:] + share * device, 0).astype(f32)
        target = jnp.sum(target, axis=0, keepdims=True)
        target = jnp.broadcast_to(target, (LANES, length)).T.astype(jnp.int32)
        for c in range(length // LANES):
            place_ref[:, c * LANES : (c + 1) * LANES] = jnp.where(
                target == iota((length, LANES), 1) + c * LANES, 1.0, 0.0
            ).astype(bf16)

    def move_copy(j, d):
        other = other_of(d)
        return remote(
            leaving_ref.at[j, rows_of(other, share)], arrived_ref.at[j, rows_of(seq, share)],
            move_send, move_recv.at[j], (other, own),
        )

    def all_moves(j):
        others = arrived_ref.at[j, pl.ds(0, length - share)]
        return remote(others, others, move_send, move_recv.at[j], (following, own))

    def hand_over(j):
        if j:
            held = summed(0, j, full_ref[j, :, own_lanes])
        else:

            def first(k):
                rows = rows_of(k, ROWS)
                held_ref[rows, :] = summed(0, (k,), full_ref[0, rows, own_lanes])

            each(0, chunks, first)
            held = held_ref[...]
        leaving_ref[j] = jnp.dot(hand_ref[...], held, preferred_element_type=f32).astype(bf16)
        each(0, count - 1, lambda d: move_copy(j, d).start())
        arrived_ref[j, rows_of(seq, share), :] = leaving_ref[j, rows_of(seq, share), :]

    def put(j):
        lanes = slice(j * COLUMNS, (j + 1) * COLUMNS)
        all_moves(j).wait_recv()
        rows = jnp.dot(place_ref[...], arrived_ref[j], preferred_element_type=f32).astype(bf16)
        tail_ref[:, lanes] = rows[length - HALO :]
        full_ref[j, :, own_lanes] = rows
        for t in range(members):
            halo_piece(j, t).start()
        if j < late:
            send_block(1, j)
        else:
            each(0, early, lambda k: send_part(j, k))
        if j == last_piece:
            each(early, chunks, lambda k: send_block(1, (k,)))
        own_ref[:, lanes] = rows

    def accumulate(j):
        part = slice(j * width, (j + 1) * width)

        def product(k):
            rows = rows_of(k, ROWS)
            result = jnp.dot(
                full_ref[j, rows, :], w_ref[part, :], preferred_element_type=f32
            )
            acc_ref[rows, :] = result if j == 0 else acc_ref[rows, :] + result
            gate = jnp.dot(full_ref[j, rows, :], wz_ref[part, :], preferred_element_type=f32)
            gate_ref[rows, :] = gate if j == 0 else gate_ref[rows, :] + gate
            square = jnp.broadcast_to(squares_of(full_ref[j, rows, :]), (ROWS, LANES))
            scale_ref[rows, :] = square if j == 0 else scale_ref[rows, :] + square

        each(0, chunks, product)

    load_bc(0).wait()
    for t in range(members):
        prepare(0, t)
    load_bc(1).start()
    own_columns = full_ref.at[:, :, own_lanes]
    pltpu.make_async_copy(own_columns, own_columns, self_sem).wait()

    def arrive_first(k):
        forward_block(0, k)
        rest_of_block(0, k)

    scan(0, arrive_first)
    exchange(0)
    drain_gather(0)
    pltpu.make_async_copy(w_out_ref.at[0], wo_col_ref, wo_sem.at[0]).wait()
    pltpu.make_async_copy(w_out_ref.at[1], wo_ref, wo_sem.at[1]).wait()

    def product_of(k, j):
        rows, lanes = rows_of(k, ROWS), lanes_of(j, members * COLUMNS)
        partial_ref[rows, lanes] = jnp.dot(
            mixed_ref[rows, :], wo_col_ref[:, lanes], preferred_element_type=f32
        ).astype(bf16)

    def mix(k):
        mixed_ref[rows_of(k, ROWS), :] = mixed_of(0, k)
        product_of(k, 0)
        send_near(0, (k,))

        @pl.when(k > 0)
        def _():
            send_far(0, (k - 1,))

    each(0, chunks, mix)
    for j in range(1, pieces):
        each(0, chunks, lambda k: product_of(k, j))
        send_near(0, j)
        send_far(0, j - 1 if j > 1 else (chunks - 1,))
    send_far(0, pieces - 1)
    plan()
    load_bc(1).wait()

    for j in range(pieces):
        hand_over(j)
        if j > 1:
            put(j - 2)
        prepare(1, j)
    put(pieces - 2)
    forward_block(1, 0)
    rest_of_block(1, 0)
    accumulate(0)
    put(pieces - 1)
    drain_sums(0)

    for j in range(1, late):
        forward_block(1, j)
        rest_of_block(1, j)
        accumulate(j)

    forward_block(1, (0,))

    def arrive_second(k):
        @pl.when(k + 1 < chunks)
        def _():
            forward_block(1, (k + 1,))

        rest_of_block(1, (k,))

    scan(1, arrive_second)
    exchange(1)

    def output_rows(k):
        rows = rows_of(k, ROWS)
        mixed_heads = mixed_of(1, k)
        for side, block in enumerate((diagonal_id, near_id, across_id, own)):
            lanes = lanes_of(block, width)
            partial_ref[rows, lanes] = jnp.dot(
                mixed_heads, wo_ref[:, lanes], preferred_element_type=f32
            ).astype(bf16)
            if side < 2:
                near_part(1, side, k).start()
        send_far(1, k)

    each(0, chunks, output_rows)

    def out_copy(k):
        rows = rows_of(k, ROWS)
        return pltpu.make_async_copy(own_ref.at[rows], out_ref.at[rows], out_sem.at[k])

    def finish(k):
        rows = rows_of(k, ROWS)
        own_ref[rows, :] = summed(1, k, own_ref[rows, :])
        out_copy(k).start()

    each(0, chunks, finish)
    drain_gather(1)
    drain_sums(1)
    for layer in range(2):
        block = halo_ref.at[layer]
        remote(
            block, block, halo_send.at[layer], halo_recv.at[layer, 0], (following, own)
        ).wait_send()
    all_orders().wait_send()
    others = arrived_ref.at[:, pl.ds(0, length - share)]
    remote(others, others, move_send, move_recv.at[0], (following, own)).wait_send()
    each(0, chunks, lambda k: out_copy(k).wait())


def body(
    tokens, col_order, in_gain, w_in, w_bc, w_dt, conv_x, conv_bc,
    dt_bias, a_log, d_skip, out_gain, w_out,
):
    count, members = lax.axis_size("seq"), lax.axis_size("tp")
    length, width = tokens.shape
    inner = w_out.shape[1]
    heads = inner // HEAD_DIM
    mixed = inner + 2 * STATE
    depth = w_in.shape[1]
    chunks, fines = length // ROWS, length // FINE
    blocks = length // STRETCH
    pieces = width // COLUMNS
    state_rows = STATE // count
    half_rows = state_rows // HALVES
    smalls = (
        col_order[None], in_gain, jnp.swapaxes(w_dt, 1, 2), conv_x, conv_bc,
        dt_bias, a_log, d_skip, out_gain,
    )
    hbm = pl.BlockSpec(memory_space=pltpu.HBM)
    dma = pltpu.SemaphoreType.DMA
    return pl.pallas_call(
        functools.partial(layers_kernel, count, members),
        in_specs=[hbm] * (4 + SMALLS),
        out_specs=hbm,
        out_shape=jax.ShapeDtypeStruct(tokens.shape, bf16),
        scratch_shapes=[
            *[pltpu.VMEM(small.shape, small.dtype) for small in smalls],
            pltpu.VMEM((pieces, length, members * COLUMNS), bf16),
            pltpu.VMEM((HALO, width), bf16),
            pltpu.VMEM((2, members, HALO, width), bf16),
            pltpu.VMEM((count, 1, length), jnp.int32),
            pltpu.VMEM((2, width, 2, inner), bf16),
            pltpu.VMEM((depth, 2 * STATE), bf16),
            pltpu.VMEM((depth, mixed + LANES), bf16),
            pltpu.VMEM((depth, inner), bf16),
            pltpu.VMEM((inner, depth), bf16),
            pltpu.VMEM((inner, depth), bf16),
            pltpu.VMEM((ROWS + 8, mixed), f32),
            pltpu.VMEM((length, inner), f32),
            pltpu.VMEM((length, inner), bf16),
            pltpu.VMEM((length, inner), bf16),
            pltpu.VMEM((length, STATE), bf16),
            pltpu.VMEM((length, STATE), bf16),
            pltpu.VMEM((length, LANES), f32),
            pltpu.VMEM((length, LANES), f32),
            pltpu.VMEM((blocks, STATE, inner), f32),
            pltpu.VMEM((blocks, 8, inner), f32),
            pltpu.VMEM((STATE, inner), f32),
            pltpu.VMEM((8, LANES), f32),
            pltpu.VMEM((2, HALVES, count, half_rows, inner), bf16),
            pltpu.VMEM((2, 1, LANES), f32),
            pltpu.VMEM((2, HALVES, count, half_rows, inner), bf16),
            pltpu.VMEM((2, count, 1, LANES), f32),
            pltpu.VMEM((2, HALVES, count, half_rows, inner), bf16),
            pltpu.VMEM((2, HALVES, count, half_rows, inner), bf16),
            pltpu.VMEM((STATE, inner), f32),
            pltpu.VMEM((length, depth), bf16),
            pltpu.VMEM((2, length, width), bf16),
            pltpu.VMEM((length, width), bf16),
            pltpu.VMEM((length, width), bf16),
            pltpu.VMEM((length, inner), bf16),
            pltpu.VMEM((length, length), bf16),
            pltpu.VMEM((length, length), bf16),
            pltpu.VMEM((pieces, length, COLUMNS), bf16),
            pltpu.VMEM((pieces, length, COLUMNS), bf16),
            pltpu.VMEM((length, COLUMNS), bf16),
            pltpu.VMEM((length, mixed + LANES), f32),
            pltpu.VMEM((length, inner), f32),
            pltpu.VMEM((length, width), bf16),
            dma((3,)), dma((2,)), dma,
            dma((2, 3)), dma((3, fines + chunks + pieces - 2)),
            dma((2,)), dma((2, members)), dma, dma,
            dma((2, HALVES)), dma((2, HALVES)), dma((2,)), dma((2,)),
            dma((2, HALVES)), dma((2, HALVES)),
            dma((2, 2)), dma((2, 2, chunks + pieces - 1)),
            dma((2,)), dma((2, chunks + pieces - 1)),
            dma, dma((pieces,)), dma((chunks,)), dma((SMALLS,)),
        ],
        compiler_params=pltpu.CompilerParams(
            collective_id=0, has_side_effects=True, vmem_limit_bytes=63 * 1024 * 1024
        ),
        name="mixer_layers",
    )(
        tokens, w_in, w_bc, w_out, *smalls,
    )


def solution(mesh):
    placed = (
        P("seq", "tp"),
        P("seq"),
        P(),
        P(None, None, None, "tp"),
        P(),
        P(None, None, "tp"),
        P(None, None, "tp"),
        P(),
        P(None, "tp"),
        P(None, "tp"),
        P(None, "tp"),
        P(None, "tp"),
        P(None, "tp", None),
    )
    return jax.shard_map(
        body, mesh=mesh, in_specs=placed, out_specs=P("seq", "tp"), check_vma=False
    )
```

```python
import functools

import jax
import jax.numpy as jnp
from jax import lax
from jax.experimental import pallas as pl
from jax.experimental.pallas import tpu as pltpu
from jax.sharding import PartitionSpec as P

HEAD_DIM = 64
STATE = 128
STRETCH = 128
LANES = 128
HALO = 16
ROWS = 256
FINE = 128
HALVES = 2
SMALLS = 9
COLUMNS = 128

epsilon = 1e-05
f32 = jnp.float32
bf16 = jnp.bfloat16
MESH = pl.DeviceIdType.MESH


def iota(shape, axis):
    return lax.broadcasted_iota(jnp.int32, shape, axis)


def spreader_of(heads, inner):
    row = iota((LANES, inner), 0)
    channel = iota((LANES, inner), 1)
    chosen = (row % heads == channel // HEAD_DIM) & (row < 3 * heads)
    return jnp.where(chosen, 1.0, 0.0).astype(bf16)


def pack_pieces(values, heads):
    values = jnp.where(iota(values.shape, 1) < heads, values, 0.0)
    high = values.astype(bf16).astype(f32)
    rest = values - high
    middle = rest.astype(bf16).astype(f32)
    low = rest - middle
    packed = high + pltpu.roll(middle, heads, 1) + pltpu.roll(low, 2 * heads, 1)
    return packed.astype(bf16)


def expand(values, heads, spreader):
    return jnp.dot(pack_pieces(values, heads), spreader, preferred_element_type=f32)


def unpack_sum(pieces, heads):
    total = (
        pieces
        + pltpu.roll(pieces, LANES - heads, 1)
        + pltpu.roll(pieces, LANES - 2 * heads, 1)
    )
    return jnp.where(iota(total.shape, 1) < heads, total, 0.0)


def rows_of(k, size):
    return pl.ds(pl.multiple_of(k * size, size), size)


def lanes_of(k, size):
    return pl.ds(pl.multiple_of(k * size, LANES), size)


def pad_row(row):
    return jnp.concatenate([row, jnp.zeros((1, LANES - row.shape[1]), f32)], axis=1)


def layers_kernel(
    count, members,
    stream_ref, w_in_ref, w_bc_ref, w_out_ref, *refs,
):
    smalls = refs[:SMALLS]
    (
        out_ref, order_ref, in_gain_ref, w_dt_ref, conv_x_ref, conv_bc_ref,
        bias_ref, a_log_ref, d_skip_ref, out_gain_ref,
        full_ref, tail_ref, halo_ref, orders_ref, raw_ref, raw_bc_ref, w_ref, wz_ref, wo_col_ref, wo_ref,
        ext_ref, y_ref, z_ref, feed_ref, b_ref, c_ref, cum_ref, scale_ref, states_ref, sofar_exp_ref,
        state_ref, sofar_ref,
        end_ref, log_ref, got_ref, logs_ref, give_ref, arriving_ref, prefix_ref,
        partial_ref, near_ref, sum_ref, far_ref,
        mixed_ref, hand_ref, place_ref, leaving_ref, arrived_ref, held_ref, acc_ref, gate_ref, own_ref,
        load_sem, wo_sem, self_sem, ag_send, ag_recv, halo_send, halo_recv, order_send, order_recv,
        end_send, end_recv, log_send, log_recv, give_send, give_recv,
        near_send, near_recv, far_send, far_recv, move_send, move_recv, out_sem,
        small_sem,
    ) = refs[SMALLS:]
    seq = lax.axis_index("seq")
    own = lax.axis_index("tp")
    chip, core = own // 2, own % 2
    near_id = chip * 2 + 1 - core
    across_id = (1 - chip) * 2 + core
    diagonal_id = (1 - chip) * 2 + 1 - core
    sibling = (seq, near_id)
    across = (seq, across_id)
    length, width = stream_ref.shape
    depth = w_ref.shape[0]
    inner = y_ref.shape[1]
    mixed = inner + 2 * STATE
    heads = inner // HEAD_DIM
    chunks = length // ROWS
    fines = length // FINE
    per = ROWS // STRETCH
    blocks = length // STRETCH
    pieces = width // COLUMNS
    share = length // count
    state_rows = STATE // count
    half_rows = state_rows // HALVES
    following = (seq + 1) % count
    before = (seq + count - 1) % count

    def remote(src, dst, send, recv, device):
        return pltpu.make_async_remote_copy(
            src_ref=src, dst_ref=dst, send_sem=send, recv_sem=recv,
            device_id=device, device_id_type=MESH,
        )

    def other_of(i):
        low = seq < count // 2
        other = jnp.where(low, count - 1 - i, i)
        return jnp.where(low, other - (other <= seq), other + (other >= seq))

    def each(first, last, act):
        def step(i, _):
            act(i)
            return 0

        lax.fori_loop(first, last, step, 0)

    greeted = [(other_of(d), own) for d in range(count - 1)]
    greeted += [(before, t) for t in range(members)]
    greeted += [across, sibling]
    barrier = pltpu.get_barrier_semaphore()
    for device in greeted:
        pl.semaphore_signal(barrier, inc=1, device_id=device, device_id_type=MESH)

    kept = (
        order_ref, in_gain_ref, w_dt_ref, conv_x_ref, conv_bc_ref,
        bias_ref, a_log_ref, d_skip_ref, out_gain_ref,
    )
    small_loads = [
        pltpu.make_async_copy(small, keep, small_sem.at[i])
        for i, (small, keep) in enumerate(zip(smalls, kept))
    ]

    def load_in(layer, t):
        return pltpu.make_async_copy(
            w_in_ref.at[layer, t * width : (t + 1) * width], raw_ref.at[t % 2], load_sem.at[t % 2]
        )

    def load_bc(layer):
        return pltpu.make_async_copy(w_bc_ref.at[layer], raw_bc_ref, load_sem.at[2])

    own_lanes = lanes_of(own, COLUMNS)
    self_loads, wo_loads = [], []
    for j in range(pieces):
        self_loads.append(
            pltpu.make_async_copy(
                stream_ref.at[:, j * COLUMNS : (j + 1) * COLUMNS],
                full_ref.at[j, :, own_lanes], self_sem,
            )
        )
        for t in range(members):
            first = t * width + j * COLUMNS
            place = j * members + t
            wo_loads.append(
                pltpu.make_async_copy(
                    w_out_ref.at[0, :, first : first + COLUMNS],
                    wo_col_ref.at[:, place * COLUMNS : (place + 1) * COLUMNS],
                    wo_sem.at[0],
                )
            )
    wo_loads.append(pltpu.make_async_copy(w_out_ref.at[1], wo_ref, wo_sem.at[1]))
    for copy in small_loads + [load_in(0, 0), load_bc(0), load_in(0, 1)] + self_loads + wo_loads:
        copy.start()

    pl.semaphore_wait(barrier, len(greeted))

    last_piece = pieces - 1
    early = chunks // 2
    late = pieces - 2

    def block_of(layer, i, owner):
        lanes = lanes_of(owner, COLUMNS)
        if layer == 0:
            return full_ref.at[:, rows_of(i, FINE), lanes], i
        if isinstance(i, int):
            return full_ref.at[i, :, lanes], fines + i
        slot = fines + late + i[0]
        return full_ref.at[pl.ds(late, pieces - late), rows_of(i[0], ROWS), lanes], slot

    def send_part(j, k):
        part = full_ref.at[j, rows_of(k, ROWS), own_lanes]
        slot = fines + late + k
        for kind, device in ((0, across), (1, sibling)):
            remote(part, part, ag_send.at[1, kind], ag_recv.at[kind, slot], device).start()

    def gather_copy(layer, kind, i, owner):
        block, slot = block_of(layer, i, owner)
        return remote(
            block, block, ag_send.at[layer, kind], ag_recv.at[kind, slot],
            across if kind == 0 else sibling,
        )

    def send_rows(k):
        rows = rows_of(k, FINE)
        for kind, device in ((0, across), (1, sibling)):
            for j in range(pieces):
                remote(
                    stream_ref.at[rows, lanes_of(j, COLUMNS)], full_ref.at[j, rows, own_lanes],
                    ag_send.at[0, kind], ag_recv.at[kind, k], device,
                ).start()

    def send_block(layer, i):
        gather_copy(layer, 0, i, own).start()
        gather_copy(layer, 1, i, own).start()

    def forward_block(layer, i):
        gather_copy(layer, 0, i, across_id).wait_recv()
        gather_copy(layer, 2, i, across_id).start()

    def rest_of_block(layer, i):
        gather_copy(layer, 1, i, near_id).wait_recv()
        gather_copy(layer, 2, i, diagonal_id).wait_recv()

    def drain_gather(layer):
        for kind, owner in ((0, own), (1, own), (2, across_id)):
            block = full_ref.at[:, :, lanes_of(owner, COLUMNS)]
            remote(block, block, ag_send.at[layer, kind], ag_recv.at[kind, 0], sibling).wait_send()

    def halo_copy(layer, t, source):
        tail = tail_ref if layer else stream_ref.at[pl.ds(length - HALO, HALO)]
        return remote(
            tail, halo_ref.at[layer, source],
            halo_send.at[layer], halo_recv.at[layer, source], (following, t),
        )

    def halo_piece(j, t):
        lanes = lanes_of(j, COLUMNS)
        return remote(
            tail_ref.at[:, lanes], halo_ref.at[1, own, :, lanes],
            halo_send.at[1], halo_recv.at[1, own], (following, t),
        )

    def order_copy(d):
        return remote(
            order_ref, orders_ref.at[seq], order_send, order_recv, (other_of(d), own)
        )

    def all_orders():
        others = orders_ref.at[pl.ds(0, count - 1)]
        return remote(others, others, order_send, order_recv, (following, own))

    for t in range(members):
        halo_copy(0, t, own).start()

    each(0, fines, send_rows)
    for copy in small_loads:
        copy.wait()
    each(0, count - 1, lambda d: order_copy(d).start())

    row = iota((2 * LANES, 2 * LANES), 0)
    col = iota((2 * LANES, 2 * LANES), 1)
    apart = jnp.where(col == 2 * (row % LANES) + row // LANES, 1.0, 0.0).astype(bf16)

    def prepare(layer, t):
        load_in(layer, t).wait()

        def block(j):
            i = t * pieces + j
            rows = rows_of(i, LANES)
            to = rows_of(j * members + t, LANES)
            gain = in_gain_ref[layer : layer + 1, lanes_of(i, LANES)]
            gain = jnp.broadcast_to(gain, (LANES, LANES)).T
            both = raw_ref[t % 2, rows_of(j, LANES)].reshape(2 * LANES, inner)
            halves = jnp.dot(apart, both, preferred_element_type=f32)
            for p in range(inner // LANES):
                lanes = slice(p * LANES, (p + 1) * LANES)
                w_ref[to, lanes] = (halves[:LANES, lanes] * gain).astype(bf16)
                wz_ref[to, lanes] = (halves[LANES:, lanes] * gain).astype(bf16)
            for p in range(2 * STATE // LANES):
                lanes = slice(p * LANES, (p + 1) * LANES)
                w_ref[to, inner + p * LANES : inner + (p + 1) * LANES] = (
                    raw_bc_ref[rows, lanes].astype(f32) * gain
                ).astype(bf16)
            dt = w_dt_ref[layer, :, lanes_of(i, LANES)].astype(f32)
            dt = jnp.concatenate([dt, jnp.zeros((LANES - heads, LANES), f32)], axis=0)
            w_ref[to, mixed:] = (dt.T * gain).astype(bf16)

        each(0, pieces, block)
        if t + 2 < members:
            load_in(layer, t + 2).start()
        elif layer == 0:
            load_in(1, t + 2 - members).start()

    spreader = spreader_of(heads, inner)
    line = iota((STRETCH, STRETCH), 0)
    lane = iota((STRETCH, STRETCH), 1)
    lower = line >= lane
    tri = jnp.where(lower, 1.0, 0.0).astype(bf16)
    left = iota((STRETCH, 2 * HEAD_DIM), 1) < HEAD_DIM

    def late_tokens(rows):
        return jnp.concatenate([full_ref[j, rows, :] for j in range(late, pieces)], axis=1)

    def squares_of(v):
        wide = v.astype(f32)
        return jnp.sum(wide * wide, axis=-1, keepdims=True)

    def scale_of(v):
        return lax.rsqrt(squares_of(v) / depth + epsilon)

    def scan(layer, arrive):
        for t in range(members):
            halo_copy(layer, t, t).wait_recv()
        ahead = jnp.concatenate(
            [
                halo_ref[layer, t, :, j * COLUMNS : (j + 1) * COLUMNS]
                for j in range(pieces) for t in range(members)
            ],
            axis=1,
        )
        ahead = jnp.dot(ahead, w_ref[:, :mixed], preferred_element_type=f32) * scale_of(ahead)
        ahead = ahead[HALO - 8 :, :].astype(bf16).astype(f32)
        ext_ref[0:8, :] = jnp.where(seq > 0, ahead, 0.0)
        state_ref[...] = jnp.zeros_like(state_ref)
        sofar_ref[...] = jnp.zeros_like(sofar_ref)
        bias = pad_row(bias_ref[layer : layer + 1, :])
        rate = pad_row(jnp.exp(a_log_ref[layer : layer + 1, :]))
        skip = pad_row(d_skip_ref[layer : layer + 1, :])
        skip = expand(jnp.broadcast_to(skip, (8, LANES)), heads, spreader)[0:1]
        taps = jnp.concatenate([conv_x_ref[layer], conv_bc_ref[layer]], axis=1)
        tap_count = taps.shape[0]

        size = ROWS if layer else FINE
        parts = size // STRETCH

        def project(k):
            rows = rows_of(k, size)
            arrive(k)
            if layer == 0:
                tokens = jnp.concatenate([full_ref[j, rows, :] for j in range(pieces)], axis=1)
                scale = scale_of(tokens)
                projected = jnp.dot(tokens, w_ref[...], preferred_element_type=f32)
                gate = jnp.dot(tokens, wz_ref[...], preferred_element_type=f32)
                z_ref[rows, :] = (gate * scale).astype(bf16)
            else:
                tokens = late_tokens(rows)
                square = scale_ref[rows, 0:1] + squares_of(tokens)
                scale = lax.rsqrt(square / depth + epsilon)
                projected = acc_ref[rows, :] + jnp.dot(
                    tokens, w_ref[late * width :, :], preferred_element_type=f32
                )
                scale_ref[rows, :] = jnp.broadcast_to(scale, (size, LANES))
            projected = projected * scale
            raw = projected[:, mixed:] + bias
            step = jnp.maximum(raw, 0.0) + jnp.log1p(jnp.exp(-jnp.abs(raw)))
            logs = pack_pieces(-step * rate, heads)
            sofar = sofar_ref[...]
            summed_logs = jnp.dot(
                tri,
                jnp.concatenate(
                    [logs[b * STRETCH : (b + 1) * STRETCH] for b in range(parts)], axis=1
                ),
                preferred_element_type=f32,
            )
            to_end, whole, earlier = [], [], []
            for b in range(parts):
                cum = unpack_sum(summed_logs[:, b * LANES : (b + 1) * LANES], heads)
                last = cum[STRETCH - 1 : STRETCH, :]
                cum_ref[rows_of(k * parts + b, STRETCH), :] = cum
                to_end.append(step[b * STRETCH : (b + 1) * STRETCH] * jnp.exp(last - cum))
                whole.append(jnp.exp(jnp.broadcast_to(last, (8, LANES))))
                earlier.append(jnp.exp(sofar))
                sofar = sofar + last
            sofar_ref[...] = sofar
            factors = expand(
                jnp.concatenate([step] + to_end + whole + earlier, axis=0), heads, spreader
            )
            ext_ref[8 : 8 + size, :] = projected[:, :mixed].astype(bf16).astype(f32)
            conv = jnp.zeros((size, mixed), f32)
            for tap in range(tap_count):
                first = 9 - tap_count + tap
                conv = conv + taps[tap : tap + 1, :] * ext_ref[first : first + size, :]
            conv = conv * jax.nn.sigmoid(conv)
            ext_ref[0:8, :] = ext_ref[size : size + 8, :]
            x = conv[:, :inner]
            b_all = conv[:, inner : inner + STATE]
            b_ref[rows, :] = b_all.astype(bf16)
            c_ref[rows, :] = conv[:, inner + STATE :].astype(bf16)
            feed_ref[rows, :] = (x * factors[:size]).astype(bf16)
            y_ref[rows, :] = skip * x
            ending = (x * factors[size : 2 * size]).astype(bf16)
            state = state_ref[...]
            for b in range(parts):
                part = slice(b * STRETCH, (b + 1) * STRETCH)
                index = k * parts + b
                fresh = jnp.dot(
                    b_all[part].T.astype(bf16), ending[part], preferred_element_type=f32
                )
                first = 2 * size + 8 * b
                states_ref[index] = state
                sofar_exp_ref[index] = factors[first + 8 * parts : first + 8 * parts + 8]
                state = state * factors[first : first + 1] + fresh
            state_ref[...] = state

        each(0, length // size, project)

    def within(layer, k):
        if layer:
            rows = rows_of(k, ROWS)
            gate = gate_ref[rows, :] + jnp.dot(
                late_tokens(rows), wz_ref[late * width :, :], preferred_element_type=f32
            )
            z_ref[rows, :] = (gate * scale_ref[rows, 0:1]).astype(bf16)

        def block(b):
            rows = rows_of(k * per + b, STRETCH)
            cum = cum_ref[rows, :]
            cum_t = cum.T
            feed = feed_ref[rows, :]
            meet = lax.dot_general(
                c_ref[rows, :], b_ref[rows, :], (((1,), (1,)), ((), ())),
                preferred_element_type=f32,
            )
            for pair in range(heads // 2):
                lanes = slice(pair * 2 * HEAD_DIM, (pair + 1) * 2 * HEAD_DIM)
                weights = []
                for h in (2 * pair, 2 * pair + 1):
                    spread = jnp.where(lower, cum[:, h : h + 1] - cum_t[h : h + 1, :], -jnp.inf)
                    weights.append((meet * jnp.exp(spread)).astype(bf16))
                fed = feed[:, lanes]
                nought = jnp.zeros_like(fed)
                stacked = jnp.concatenate(
                    [jnp.where(left, fed, nought), jnp.where(left, nought, fed)], axis=0
                )
                inside = jnp.dot(
                    jnp.concatenate(weights, axis=1), stacked, preferred_element_type=f32
                )
                y_ref[rows, lanes] = y_ref[rows, lanes] + inside

        each(0, per, block)

    def exchange(layer):
        def end_copy(h, d):
            other = other_of(d)
            return remote(
                end_ref.at[layer, h, other], got_ref.at[layer, h, seq],
                end_send.at[layer, h], end_recv.at[layer, h], (other, own),
            )

        def log_copy(d):
            return remote(
                log_ref.at[layer], logs_ref.at[layer, seq],
                log_send.at[layer], log_recv.at[layer], (other_of(d), own),
            )

        def give_copy(h, d):
            other = other_of(d)
            return remote(
                give_ref.at[layer, h, other], arriving_ref.at[layer, h, seq],
                give_send.at[layer, h], give_recv.at[layer, h], (other, own),
            )

        others = pl.ds(0, count - 1)

        def all_of(block, send, recv):
            return remote(block, block, send, recv, (following, own))

        def all_ends(h):
            block = got_ref.at[layer, h, others]
            return all_of(block, end_send.at[layer, h], end_recv.at[layer, h])

        def all_given(h):
            block = arriving_ref.at[layer, h, others]
            return all_of(block, give_send.at[layer, h], give_recv.at[layer, h])

        all_logs = all_of(logs_ref.at[layer, others], log_send.at[layer], log_recv.at[layer])

        state = state_ref[...]
        log_ref[layer] = sofar_ref[0:1, :]
        for d in range(count):
            for h in range(HALVES):
                first = d * state_rows + h * half_rows
                end_ref[layer, h, d] = state[first : first + half_rows].astype(bf16)
        each(0, count - 1, lambda d: log_copy(d).start())
        for h in range(HALVES):
            each(0, count - 1, lambda d: end_copy(h, d).start())
        first_part = chunks // 2
        each(0, first_part, lambda k: within(layer, k))
        all_logs.wait_recv()
        logs_ref[layer, seq] = log_ref[layer]
        logs = jnp.concatenate([logs_ref[layer, d] for d in range(count)], axis=0)
        factors = expand(jnp.exp(logs), heads, spreader)
        for h in range(HALVES):
            all_ends(h).wait_recv()
            got_ref[layer, h, seq] = end_ref[layer, h, seq]
            prefix = jnp.zeros((half_rows, inner), f32)
            for d in range(count):
                give_ref[layer, h, d] = prefix.astype(bf16)
                if d + 1 < count:
                    prefix = prefix * factors[d : d + 1] + got_ref[layer, h, d].astype(f32)
            each(0, count - 1, lambda d: give_copy(h, d).start())
        each(first_part, chunks, lambda k: within(layer, k))
        for h in range(HALVES):
            all_given(h).wait_recv()
            arriving_ref[layer, h, seq] = give_ref[layer, h, seq]
        prefix_ref[...] = jnp.concatenate(
            [
                arriving_ref[layer, h, d].astype(f32)
                for d in range(count) for h in range(HALVES)
            ],
            axis=0,
        )
        all_logs.wait_send()
        for h in range(HALVES):
            all_ends(h).wait_send()
            all_given(h).wait_send()

    pair = 2 * HEAD_DIM
    one = iota((2 * pair, pair), 0) % pair // HEAD_DIM
    two = iota((2 * pair, pair), 1) // HEAD_DIM
    averager = jnp.where(one == two, 1.0 / HEAD_DIM, 0.0).astype(bf16)

    def mixed_of(layer, k):
        rows = rows_of(k, ROWS)
        grown = expand(jnp.exp(cum_ref[rows, :]), heads, spreader)
        carried = []
        for block in range(per):
            index = k * per + block
            state = states_ref[index] + prefix_ref[...] * sofar_exp_ref[index][0:1]
            carried.append(
                jnp.dot(
                    c_ref[rows_of(index, STRETCH), :], state.astype(bf16),
                    preferred_element_type=f32,
                )
            )
        gate = z_ref[rows, :].astype(f32)
        ssd = y_ref[rows, :] + jnp.concatenate(carried, axis=0) * grown
        gated = ssd * (gate * jax.nn.sigmoid(gate))
        square = gated * gated
        high = square.astype(bf16)
        low = (square - high.astype(f32)).astype(bf16)
        results = []
        for p in range(inner // pair):
            lanes = slice(p * pair, (p + 1) * pair)
            both = jnp.concatenate([high[:, lanes], low[:, lanes]], axis=1)
            mean = jnp.dot(both, averager, preferred_element_type=f32)
            scaled = gated[:, lanes] * lax.rsqrt(mean + epsilon)
            results.append((scaled * out_gain_ref[layer : layer + 1, lanes]).astype(bf16))
        return jnp.concatenate(results, axis=1)

    def part_of(layer, i):
        if layer == 1:
            rows, slot = rows_of(i, ROWS), i
            lanes, held = (lambda t: lanes_of(t, width)), pl.ds(0, width)
        else:
            if isinstance(i, int):
                rows, j, slot = pl.ds(0, length), i, chunks + i - 1
            else:
                rows, j, slot = rows_of(i[0], ROWS), 0, i[0]
            lanes, held = (lambda t: lanes_of(j * members + t, COLUMNS)), lanes_of(j, COLUMNS)
        nears = [near_ref.at[side, rows, held] for side in range(2)]
        return rows, lanes, nears, (sum_ref.at[rows, held], far_ref.at[rows, held]), slot

    def near_part(layer, side, i):
        rows, lanes, nears, _, slot = part_of(layer, i)
        block = diagonal_id if side == 0 else near_id
        return remote(
            partial_ref.at[rows, lanes(block)], nears[side],
            near_send.at[layer, side], near_recv.at[layer, side, slot], sibling,
        )

    def far_part(layer, i):
        _, _, _, (summing, far), slot = part_of(layer, i)
        return remote(summing, far, far_send.at[layer], far_recv.at[layer, slot], across)

    def send_near(layer, i):
        near_part(layer, 0, i).start()
        near_part(layer, 1, i).start()

    def send_far(layer, i):
        rows, lanes, nears, (summing, _), _ = part_of(layer, i)
        near_part(layer, 0, i).wait_recv()
        summing[...] = (
            partial_ref[rows, lanes(across_id)].astype(f32) + nears[0][...].astype(f32)
        ).astype(bf16)
        far_part(layer, i).start()

    def summed(layer, i, stream):
        rows, lanes, nears, (_, far), _ = part_of(layer, i)
        near_part(layer, 1, i).wait_recv()
        far_part(layer, i).wait_recv()
        return (
            stream.astype(f32)
            + partial_ref[rows, lanes(own)].astype(f32)
            + nears[1][...].astype(f32)
            + far[...].astype(f32)
        ).astype(bf16)

    def drain_sums(layer):
        for side in range(2):
            block = near_ref.at[side]
            remote(
                block, block, near_send.at[layer, side], near_recv.at[layer, side, 0], sibling
            ).wait_send()
        remote(sum_ref, sum_ref, far_send.at[layer], far_recv.at[layer, 0], across).wait_send()

    def plan():
        shift = length.bit_length() - 1
        all_orders().wait_recv()
        orders_ref[seq] = order_ref[...]
        orders = jnp.concatenate([orders_ref[d] for d in range(count)], axis=0)

        def count_up(r):
            first = iota((LANES, length), 0) + r * LANES
            place_ref[rows_of(r, LANES), :] = jnp.where(
                first <= iota((LANES, length), 1), 1.0, 0.0
            ).astype(bf16)

        each(0, length // LANES, count_up)
        device = iota((count, length), 0)
        wanted_here = jnp.right_shift(orders, shift) == seq
        from_each = jnp.right_shift(order_ref[...], shift) == device
        ones = jnp.concatenate(
            [jnp.where(wanted_here, 1.0, 0.0), jnp.where(from_each, 1.0, 0.0)], axis=0
        ).astype(bf16)
        counted = jnp.dot(ones, place_ref[...], preferred_element_type=f32).astype(jnp.int32) - 1
        slot = jnp.where(wanted_here, counted[:count], -1)
        local = jnp.bitwise_and(orders, length - 1)
        short = iota((share, length), 0)
        long = iota((share, length), 1)
        for d in range(count):
            chosen = slot[d : d + 1, :] == short
            found = jnp.where(chosen, local[d : d + 1, :], 0).astype(f32)
            wanted = jnp.sum(found, axis=1, keepdims=True).astype(jnp.int32)
            hand_ref[d * share : (d + 1) * share, :] = jnp.where(
                wanted == long, 1.0, 0.0
            ).astype(bf16)
        target = jnp.where(from_each, counted[count:] + share * device, 0).astype(f32)
        target = jnp.sum(target, axis=0, keepdims=True)
        target = jnp.broadcast_to(target, (LANES, length)).T.astype(jnp.int32)
        for c in range(length // LANES):
            place_ref[:, c * LANES : (c + 1) * LANES] = jnp.where(
                target == iota((length, LANES), 1) + c * LANES, 1.0, 0.0
            ).astype(bf16)

    def move_copy(j, d):
        other = other_of(d)
        return remote(
            leaving_ref.at[j, rows_of(other, share)], arrived_ref.at[j, rows_of(seq, share)],
            move_send, move_recv.at[j], (other, own),
        )

    def all_moves(j):
        others = arrived_ref.at[j, pl.ds(0, length - share)]
        return remote(others, others, move_send, move_recv.at[j], (following, own))

    def hand_over(j):
        if j:
            held = summed(0, j, full_ref[j, :, own_lanes])
        else:

            def first(k):
                rows = rows_of(k, ROWS)
                held_ref[rows, :] = summed(0, (k,), full_ref[0, rows, own_lanes])

            each(0, chunks, first)
            held = held_ref[...]
        leaving_ref[j] = jnp.dot(hand_ref[...], held, preferred_element_type=f32).astype(bf16)
        each(0, count - 1, lambda d: move_copy(j, d).start())
        arrived_ref[j, rows_of(seq, share), :] = leaving_ref[j, rows_of(seq, share), :]

    def put(j):
        lanes = slice(j * COLUMNS, (j + 1) * COLUMNS)
        all_moves(j).wait_recv()
        rows = jnp.dot(place_ref[...], arrived_ref[j], preferred_element_type=f32).astype(bf16)
        tail_ref[:, lanes] = rows[length - HALO :]
        full_ref[j, :, own_lanes] = rows
        for t in range(members):
            halo_piece(j, t).start()
        if j < late:
            send_block(1, j)
        else:
            each(0, early, lambda k: send_part(j, k))
        if j == last_piece:
            each(early, chunks, lambda k: send_block(1, (k,)))
        own_ref[:, lanes] = rows

    def accumulate(j):
        part = slice(j * width, (j + 1) * width)

        def product(k):
            rows = rows_of(k, ROWS)
            result = jnp.dot(
                full_ref[j, rows, :], w_ref[part, :], preferred_element_type=f32
            )
            acc_ref[rows, :] = result if j == 0 else acc_ref[rows, :] + result
            gate = jnp.dot(full_ref[j, rows, :], wz_ref[part, :], preferred_element_type=f32)
            gate_ref[rows, :] = gate if j == 0 else gate_ref[rows, :] + gate
            square = jnp.broadcast_to(squares_of(full_ref[j, rows, :]), (ROWS, LANES))
            scale_ref[rows, :] = square if j == 0 else scale_ref[rows, :] + square

        each(0, chunks, product)

    load_bc(0).wait()
    for t in range(members):
        prepare(0, t)
    load_bc(1).start()
    own_columns = full_ref.at[:, :, own_lanes]
    pltpu.make_async_copy(own_columns, own_columns, self_sem).wait()

    def arrive_first(k):
        forward_block(0, k)
        rest_of_block(0, k)

    scan(0, arrive_first)
    exchange(0)
    drain_gather(0)
    pltpu.make_async_copy(w_out_ref.at[0], wo_col_ref, wo_sem.at[0]).wait()
    pltpu.make_async_copy(w_out_ref.at[1], wo_ref, wo_sem.at[1]).wait()

    def product_of(k, j):
        rows, lanes = rows_of(k, ROWS), lanes_of(j, members * COLUMNS)
        partial_ref[rows, lanes] = jnp.dot(
            mixed_ref[rows, :], wo_col_ref[:, lanes], preferred_element_type=f32
        ).astype(bf16)

    def mix(k):
        mixed_ref[rows_of(k, ROWS), :] = mixed_of(0, k)
        product_of(k, 0)
        send_near(0, (k,))

        @pl.when(k > 0)
        def _():
            send_far(0, (k - 1,))

    each(0, chunks, mix)
    for j in range(1, pieces):
        each(0, chunks, lambda k: product_of(k, j))
        send_near(0, j)
        send_far(0, j - 1 if j > 1 else (chunks - 1,))
    send_far(0, pieces - 1)
    plan()
    load_bc(1).wait()

    for j in range(pieces):
        hand_over(j)
        if j > 1:
            put(j - 2)
        prepare(1, j)
    put(pieces - 2)
    forward_block(1, 0)
    rest_of_block(1, 0)
    accumulate(0)
    put(pieces - 1)
    drain_sums(0)

    for j in range(1, late):
        forward_block(1, j)
        rest_of_block(1, j)
        accumulate(j)

    forward_block(1, (0,))

    def arrive_second(k):
        @pl.when(k + 1 < chunks)
        def _():
            forward_block(1, (k + 1,))

        rest_of_block(1, (k,))

    scan(1, arrive_second)
    exchange(1)

    def output_rows(k):
        rows = rows_of(k, ROWS)
        mixed_heads = mixed_of(1, k)
        for side, block in enumerate((diagonal_id, near_id, across_id, own)):
            lanes = lanes_of(block, width)
            partial_ref[rows, lanes] = jnp.dot(
                mixed_heads, wo_ref[:, lanes], preferred_element_type=f32
            ).astype(bf16)
            if side < 2:
                near_part(1, side, k).start()
        send_far(1, k)

    each(0, chunks, output_rows)

    def out_copy(k):
        rows = rows_of(k, ROWS)
        return pltpu.make_async_copy(own_ref.at[rows], out_ref.at[rows], out_sem.at[k])

    def finish(k):
        rows = rows_of(k, ROWS)
        own_ref[rows, :] = summed(1, k, own_ref[rows, :])
        out_copy(k).start()

    each(0, chunks, finish)
    drain_gather(1)
    drain_sums(1)
    for layer in range(2):
        block = halo_ref.at[layer]
        remote(
            block, block, halo_send.at[layer], halo_recv.at[layer, 0], (following, own)
        ).wait_send()
    all_orders().wait_send()
    others = arrived_ref.at[:, pl.ds(0, length - share)]
    remote(others, others, move_send, move_recv.at[0], (following, own)).wait_send()
    each(0, chunks, lambda k: out_copy(k).wait())


def body(
    tokens, col_order, in_gain, w_in, w_bc, w_dt, conv_x, conv_bc,
    dt_bias, a_log, d_skip, out_gain, w_out,
):
    count, members = lax.axis_size("seq"), lax.axis_size("tp")
    length, width = tokens.shape
    inner = w_out.shape[1]
    heads = inner // HEAD_DIM
    mixed = inner + 2 * STATE
    depth = w_in.shape[1]
    chunks, fines = length // ROWS, length // FINE
    blocks = length // STRETCH
    pieces = width // COLUMNS
    state_rows = STATE // count
    half_rows = state_rows // HALVES
    smalls = (
        col_order[None], in_gain, jnp.swapaxes(w_dt, 1, 2), conv_x, conv_bc,
        dt_bias, a_log, d_skip, out_gain,
    )
    hbm = pl.BlockSpec(memory_space=pltpu.HBM)
    dma = pltpu.SemaphoreType.DMA
    return pl.pallas_call(
        functools.partial(layers_kernel, count, members),
        in_specs=[hbm] * (4 + SMALLS),
        out_specs=hbm,
        out_shape=jax.ShapeDtypeStruct(tokens.shape, bf16),
        scratch_shapes=[
            *[pltpu.VMEM(small.shape, small.dtype) for small in smalls],
            pltpu.VMEM((pieces, length, members * COLUMNS), bf16),
            pltpu.VMEM((HALO, width), bf16),
            pltpu.VMEM((2, members, HALO, width), bf16),
            pltpu.VMEM((count, 1, length), jnp.int32),
            pltpu.VMEM((2, width, 2, inner), bf16),
            pltpu.VMEM((depth, 2 * STATE), bf16),
            pltpu.VMEM((depth, mixed + LANES), bf16),
            pltpu.VMEM((depth, inner), bf16),
            pltpu.VMEM((inner, depth), bf16),
            pltpu.VMEM((inner, depth), bf16),
            pltpu.VMEM((ROWS + 8, mixed), f32),
            pltpu.VMEM((length, inner), f32),
            pltpu.VMEM((length, inner), bf16),
            pltpu.VMEM((length, inner), bf16),
            pltpu.VMEM((length, STATE), bf16),
            pltpu.VMEM((length, STATE), bf16),
            pltpu.VMEM((length, LANES), f32),
            pltpu.VMEM((length, LANES), f32),
            pltpu.VMEM((blocks, STATE, inner), f32),
            pltpu.VMEM((blocks, 8, inner), f32),
            pltpu.VMEM((STATE, inner), f32),
            pltpu.VMEM((8, LANES), f32),
            pltpu.VMEM((2, HALVES, count, half_rows, inner), bf16),
            pltpu.VMEM((2, 1, LANES), f32),
            pltpu.VMEM((2, HALVES, count, half_rows, inner), bf16),
            pltpu.VMEM((2, count, 1, LANES), f32),
            pltpu.VMEM((2, HALVES, count, half_rows, inner), bf16),
            pltpu.VMEM((2, HALVES, count, half_rows, inner), bf16),
            pltpu.VMEM((STATE, inner), f32),
            pltpu.VMEM((length, depth), bf16),
            pltpu.VMEM((2, length, width), bf16),
            pltpu.VMEM((length, width), bf16),
            pltpu.VMEM((length, width), bf16),
            pltpu.VMEM((length, inner), bf16),
            pltpu.VMEM((length, length), bf16),
            pltpu.VMEM((length, length), bf16),
            pltpu.VMEM((pieces, length, COLUMNS), bf16),
            pltpu.VMEM((pieces, length, COLUMNS), bf16),
            pltpu.VMEM((length, COLUMNS), bf16),
            pltpu.VMEM((length, mixed + LANES), f32),
            pltpu.VMEM((length, inner), f32),
            pltpu.VMEM((length, width), bf16),
            dma((3,)), dma((2,)), dma,
            dma((2, 3)), dma((3, fines + chunks + pieces - 2)),
            dma((2,)), dma((2, members)), dma, dma,
            dma((2, HALVES)), dma((2, HALVES)), dma((2,)), dma((2,)),
            dma((2, HALVES)), dma((2, HALVES)),
            dma((2, 2)), dma((2, 2, chunks + pieces - 1)),
            dma((2,)), dma((2, chunks + pieces - 1)),
            dma, dma((pieces,)), dma((chunks,)), dma((SMALLS,)),
        ],
        compiler_params=pltpu.CompilerParams(
            collective_id=0, has_side_effects=True, vmem_limit_bytes=63 * 1024 * 1024
        ),
        name="mixer_layers",
    )(
        tokens, w_in, w_bc, w_out, *smalls,
    )


def solution(mesh):
    placed = (
        P("seq", "tp"),
        P("seq"),
        P(),
        P(None, None, None, "tp"),
        P(),
        P(None, None, "tp"),
        P(None, None, "tp"),
        P(),
        P(None, "tp"),
        P(None, "tp"),
        P(None, "tp"),
        P(None, "tp"),
        P(None, "tp", None),
    )
    return jax.shard_map(
        body, mesh=mesh, in_specs=placed, out_specs=P("seq", "tp"), check_vma=False
    )
```
